32 devices in a mesh: dp: 16 (over z, x, core), seq: 2 (over y).
Axes of the slice: x: 2, y: 2, z: 4, core: 2. Of those that a mesh axis runs over, the one named last changes fastest.
Arguments:
- tokens: bfloat16 [64, 1024, 768], P(('dp', 'seq')), may hold values from -6 to 6
- segments: int32 [64, 1024], P(('dp', 'seq')), may hold values from 0 to 3, never falling along the last dimension, each value on 1 to 512 neighbouring positions
- cotangent: bfloat16 [64, 1024, 768], P(('dp', 'seq')), may hold values from -6 to 6
- norm_gain: float32 [768], replicated, may hold values from 0.5 to 1.5
- weight_in: bfloat16 [768, 3352], P('dp'), may hold values from -0.21875 to 0.21875
- conv_weight: float32 [4, 1792], replicated, may hold values from -3 to 3
- conv_bias: float32 [1792], replicated, may hold values from -3 to 3
- dt_bias: float32 [24], replicated, may hold values from -6 to -2
- a_log: float32 [24], replicated, may hold values from -1 to 2.5
- skip_d: float32 [24], replicated, may hold values from 0.5 to 1.5
- gate_gain: float32 [1536], replicated, may hold values from 0.5 to 1.5
- weight_out: bfloat16 [1536, 768], P('dp'), may hold values from -0.15625 to 0.15625
Outputs:
- mixed_out: bfloat16 [64, 1024, 768], P(('dp', 'seq'))
- grad_tokens: bfloat16 [64, 1024, 768], P(('dp', 'seq'))
- grad_norm_gain: float32 [768], replicated
- grad_weight_in: float32 [768, 3352], P('dp')
- grad_conv_weight: float32 [4, 1792], replicated
- grad_conv_bias: float32 [1792], replicated
- grad_dt_bias: float32 [24], replicated
- grad_a_log: float32 [24], replicated
- grad_skip_d: float32 [24], replicated
- grad_gate_gain: float32 [1536], replicated
- grad_weight_out: float32 [1536, 768], P('dp')
The draws below stay inside these ranges and needn't reach their ends.
Inputs may be any that keep to these rules, and one draw needn't show every extreme that they name: `segments`: in each sequence the numbers never fall, all of 0 to 3 occur, each document holds 1 to 512 tokens and one holds exactly 512.
All inputs are finite; a program needn't handle non-finite values.
Results may differ from the reference program's by a relative error of at most 0.0082.
Values may be sent and summed in bfloat16 or wider, within the bound.
A program may use at most 448 MiB of HBM per device.

```python
import math
import jax
import jax.numpy as jnp
import numpy as np
from jax import lax

D = 768
HEADS = 24
CONV = 4
BLOCK = 256
LEN = 1024
SEQ_DEV = 2
DI = 1536
CHANNELS = 1792
PROJ = 3352
SEQUENCES = 64


def levels(own_key, dims, shards, smallest, high):
    gain = 1.0
    for axis_at, parts in shards:
        heights = jax.random.uniform(jax.random.fold_in(jax.random.fold_in(own_key, 6), axis_at), (parts,), jnp.float32, smallest / len(shards), high / len(shards))
        gain = gain * jnp.repeat(jnp.exp(heights), dims[axis_at] // parts).reshape((-1,) + (1,) * (len(dims) - 1 - axis_at))
    return gain


def length_profile(number_of, total, bound, slope):
    loads = [(1 << 20) // math.isqrt(standing ** slope) + 1 for standing in range(2, number_of + 1)]
    rest, counts = total - bound - (number_of - 1), [1] * (number_of - 1)
    while rest > 0:
        candidates = [i for i in range(number_of - 1) if counts[i] < bound]
        mass, remaining = sum([loads[i] for i in candidates]), rest
        for i in candidates:
            addition = min(bound - counts[i], max(1, remaining * loads[i] // mass), rest)
            counts[i] = counts[i] + addition
            rest = rest - addition
    return np.array([bound] + counts)


def uneven(key, count, total, limit, lean):
    if count == 2:
        one = jax.random.randint(key, (), max(1, total - limit), min(limit, total - 1) + 1)
        return jnp.stack([one, total - one])
    lengths = jnp.asarray(length_profile(count, total, limit, lean), jnp.int32)
    twos = (count - 1) // 2
    giver, sink = lengths[1:1 + 2 * twos:2], lengths[2:2 + 2 * twos:2]
    room = jnp.minimum(giver - 1, limit - sink)
    passed = jax.random.randint(jax.random.fold_in(key, 1), (twos,), 0, 1 << 20) % (room + 1)
    lengths = lengths.at[1:1 + 2 * twos:2].set(giver - passed).at[2:2 + 2 * twos:2].set(sink + passed)
    return lengths[jax.random.permutation(jax.random.fold_in(key, 2), count)]


def noise(key, shape, deviation, limit, shards=(), dtype=jnp.bfloat16):
    array = jax.random.normal(key, shape, jnp.float32) * deviation
    if len(shards) > 0:
        array = levels(key, shape, shards, -0.22, 0.18) * array
    return jnp.clip(array, min=-limit, max=limit).astype(dtype)


def setup_inputs(seed: int = 0) -> dict:
    key_of = jax.random.split(jax.random.key(seed), 13)
    return {
        "tokens": noise(key_of[0], (SEQUENCES, LEN, D), 1.0, 6.0, ((0, 32),)),
        "segments": jax.vmap(lambda own: jnp.searchsorted(jnp.cumsum(uneven(own, 4, LEN, LEN // 2, 0)), jnp.arange(LEN), side="right"))(jax.random.split(key_of[1], SEQUENCES)).reshape((SEQUENCES, LEN)).astype(jnp.int32),
        "cotangent": noise(key_of[2], (SEQUENCES, LEN, D), 1.0, 6.0, ((0, 32),)),
        "norm_gain": jnp.clip(1.0 + 0.1 * jax.random.normal(key_of[3], (D,), jnp.float32), 0.5, 1.5),
        "weight_in": noise(key_of[4], (D, PROJ), D ** -0.5, 0.21875, ((0, 16),)),
        "conv_weight": noise(key_of[5], (CONV, CHANNELS), CONV ** -0.5, 3.0, (), jnp.float32),
        "conv_bias": noise(key_of[6], (CHANNELS,), 0.5, 3.0, (), jnp.float32),
        "dt_bias": jnp.clip(jax.random.uniform(key_of[7], (HEADS,), jnp.float32, -6.0, -2.0), -6.0, -2.0),
        "a_log": jnp.clip(jax.random.uniform(key_of[8], (HEADS,), jnp.float32, -1.0, 2.5), -1.0, 2.5),
        "skip_d": jnp.clip(jax.random.uniform(key_of[9], (HEADS,), jnp.float32, 0.5, 1.5), 0.5, 1.5),
        "gate_gain": jnp.clip(1.0 + 0.1 * jax.random.normal(key_of[10], (DI,), jnp.float32), 0.5, 1.5),
        "weight_out": noise(key_of[11], (DI, D), DI ** -0.5, 0.15625, ((0, 16),)),
    }


eps_norm = 1e-05
highest = lax.Precision.HIGHEST

@jax.custom_vjp
def low(v):
    return lax.optimization_barrier(v.astype(jnp.bfloat16)).astype(jnp.float32)

@jax.custom_vjp
def low_back(v):
    return v

def low_keep(v):
    return (low(v), None)

def low_pass(kept, grad):
    return (grad,)

def back_keep(v):
    return (v, None)

def back_low(kept, grad):
    return (low(grad),)
low.defvjp(low_keep, low_pass)
low_back.defvjp(back_keep, back_low)

def rms_scale(values, scale_gain):
    return values * lax.rsqrt(lax.optimization_barrier(jnp.mean(values * values, axis=-1, keepdims=True)) + eps_norm) * scale_gain

def causal_conv(padded, seg_pad, conv_weight, conv_bias):
    tap_count = conv_weight.shape[0]
    row_count = padded.shape[1] - tap_count + 1
    summed = jnp.zeros_like(padded[:, tap_count - 1:, :]) + conv_bias
    for offset in range(tap_count):
        window = padded[:, offset:offset + row_count, :]
        same_seg = (seg_pad[:, offset:offset + row_count] == seg_pad[:, tap_count - 1:]).astype(jnp.float32)
        summed = summed + conv_weight[offset] * window * same_seg[..., None]
    return jax.nn.silu(summed)

def state_space(values_x, b_proj, c_proj, time_step, log_decay, seg_float, skip_d, block_len):
    seq_count, row_count, head_count, head_dim = values_x.shape
    block_count = row_count // block_len
    state_dim = b_proj.shape[-1]
    x_blocks = values_x.reshape(seq_count, block_count, block_len, head_count, head_dim)
    b_blocks = b_proj.reshape(seq_count, block_count, block_len, state_dim)
    c_blocks = c_proj.reshape(seq_count, block_count, block_len, state_dim)
    step_blocks = time_step.reshape(seq_count, block_count, block_len, head_count)
    cumulative = jnp.cumsum(log_decay.reshape(seq_count, block_count, block_len, head_count), axis=2)
    seg_blocks = seg_float.reshape(seq_count, block_count, block_len)
    positions = jnp.arange(block_len)
    causal = positions[:, None] >= positions[None, :]
    same_seg = (seg_blocks[:, :, :, None] == seg_blocks[:, :, None, :]) & causal
    in_segment = same_seg[:, :, None, :, :]
    cum_heads = jnp.moveaxis(cumulative, 3, 2)
    log_gap = cum_heads[..., :, None] - cum_heads[..., None, :]
    decay_mat = jnp.exp(jnp.where(in_segment, log_gap, 0.0)) * in_segment.astype(jnp.float32)
    scores = jnp.einsum('skin,skjn->skij', c_blocks, b_blocks, precision=highest)
    x_scaled = x_blocks * step_blocks[..., None]
    within = jnp.einsum('skhij,skjhp->skihp', decay_mat * scores[:, :, None], x_scaled, precision=highest)
    last_seg = seg_blocks[:, :, -1]
    to_end = (seg_blocks == last_seg[..., None]).astype(jnp.float32)[..., None] * jnp.exp(cumulative[:, :, -1:, :] - cumulative)
    own_state = jnp.einsum('skjhp,skjn->skhpn', x_scaled * to_end[..., None], b_blocks, precision=highest)
    block_decay = jnp.exp(cumulative[:, :, -1, :])
    prev_seg = jnp.concatenate([jnp.full((seq_count, 1), -1.0, jnp.float32), last_seg[:, :-1]], axis=1)
    keep_flag = (last_seg == prev_seg).astype(jnp.float32)
    carried = jnp.zeros((seq_count, head_count, head_dim, state_dim), jnp.float32)
    entering = []
    for block_idx in range(block_count):
        entering.append(carried)
        carried = own_state[:, block_idx] + (keep_flag[:, block_idx, None] * block_decay[:, block_idx])[..., None, None] * carried
    entering = jnp.stack(entering, axis=1)
    from_prev = (seg_blocks == prev_seg[..., None]).astype(jnp.float32)[..., None] * jnp.exp(cumulative)
    state_part = jnp.einsum('skin,skhpn->skihp', c_blocks, entering, precision=highest) * from_prev[..., None]
    result = within + state_part + skip_d[:, None] * x_blocks
    return result.reshape(seq_count, row_count, head_count, head_dim)

def mixer_core(conv_in, dt_raw, conv_weight, conv_bias, dt_bias, a_log, skip_d, seg_float, inner, block_len):
    seq_count, row_count, channels = conv_in.shape
    head_count = dt_bias.shape[0]
    rim_width = conv_weight.shape[0] - 1
    padded = jnp.concatenate([jnp.zeros((seq_count, rim_width, channels), jnp.float32), conv_in], axis=1)
    seg_pad = jnp.concatenate([jnp.full((seq_count, rim_width), -1.0, jnp.float32), seg_float], axis=1)
    conv_out = causal_conv(padded, seg_pad, conv_weight, conv_bias)
    state_dim = (channels - inner) // 2
    values_x = conv_out[..., :inner].reshape(seq_count, row_count, head_count, inner // head_count)
    b_proj = conv_out[..., inner:inner + state_dim]
    c_proj = conv_out[..., inner + state_dim:]
    time_step = jax.nn.softplus(dt_raw + dt_bias)
    log_decay = -jnp.exp(a_log) * time_step
    return state_space(values_x, b_proj, c_proj, time_step, log_decay, seg_float, skip_d, block_len)

def gate_norm(mixed, gate_z, gate_gain):
    gated = mixed.reshape(gate_z.shape[0], gate_z.shape[1], -1) * jax.nn.silu(gate_z)
    return rms_scale(gated, gate_gain)

def layer_forward(tok_float, seg_float, norm_gain, weight_in, conv_weight, conv_bias, dt_bias, a_log, skip_d, gate_gain, weight_out):
    inner = gate_gain.shape[0]
    channels = conv_bias.shape[0]
    normed = low(rms_scale(tok_float, norm_gain))
    projected = low_back(jnp.einsum('srd,de->sre', normed, weight_in, precision=highest))
    gate_z = projected[..., :inner]
    conv_in = projected[..., inner:inner + channels]
    dt_raw = projected[..., inner + channels:]
    mixed = mixer_core(conv_in, dt_raw, conv_weight, conv_bias, dt_bias, a_log, skip_d, seg_float, inner, BLOCK)
    gnormed = low(gate_norm(mixed, gate_z, gate_gain))
    return tok_float + jnp.einsum('sri,id->srd', gnormed, weight_out, precision=highest)

def reference(tokens, segments, cotangent, norm_gain, weight_in, conv_weight, conv_bias, dt_bias, a_log, skip_d, gate_gain, weight_out):
    block_total = tokens.shape[0] // SEQ_DEV
    tok_blocks = tokens.astype(jnp.float32).reshape(block_total, SEQ_DEV, LEN, D)
    seg_blocks = segments.astype(jnp.float32).reshape(block_total, SEQ_DEV, LEN)

    def whole(tok_all, norm_gain, weight_in, conv_weight, conv_bias, dt_bias, a_log, skip_d, gate_gain, weight_out):

        def run_block(carry_none, slab):
            return (carry_none, jax.checkpoint(layer_forward)(slab[0], slab[1], norm_gain, weight_in, conv_weight, conv_bias, dt_bias, a_log, skip_d, gate_gain, weight_out))
        _, outputs = lax.scan(run_block, jnp.zeros((), jnp.float32), (tok_all, seg_blocks))
        return outputs
    outputs, pullback = jax.vjp(whole, tok_blocks, norm_gain, weight_in.astype(jnp.float32), conv_weight, conv_bias, dt_bias, a_log, skip_d, gate_gain, weight_out.astype(jnp.float32))
    grads = pullback(cotangent.astype(jnp.float32).reshape(tok_blocks.shape))
    return (outputs.reshape(tokens.shape).astype(jnp.bfloat16), grads[0].reshape(tokens.shape).astype(jnp.bfloat16), grads[1], grads[2], grads[3], grads[4], grads[5], grads[6], grads[7], grads[8], grads[9])
```

```python
import math

import jax
import jax.numpy as jnp
from jax import lax
from jax.experimental import pallas as pl
from jax.experimental.pallas import tpu as pltpu
from jax.sharding import PartitionSpec as P

f32 = jnp.float32
bf16 = jnp.bfloat16
Q = 128
LANES = 128
EPS = 1e-05
LOG2E = math.log2(math.e)
NEG = -1e30

NN = (((1,), (0,)), ((), ()))
NT = (((1,), (1,)), ((), ()))
TN = (((0,), (0,)), ((), ()))


def dot(a, b, dims=NN):
    return lax.dot_general(a, b, dims, preferred_element_type=f32)


def pair_split(v):
    return jnp.concatenate(split(v, 2), axis=1)


def twice(v, axis):
    return jnp.concatenate([v, v], axis=axis)


def dot_split(a, b):
    low = b[1]
    return dot(jnp.concatenate(a, axis=1), twice(b[0], 1), NT) + dot(a[0], low, NT)


def sigmoid(v):
    return 0.5 + 0.5 * jnp.tanh(0.5 * v)


def split(v, parts):
    out = []
    for _ in range(parts):
        low = v.astype(bf16)
        out.append(low)
        v = v - low.astype(f32)
    return out


def fold_rows(v):
    return jnp.sum(v.reshape(v.shape[0] // 8, 8, v.shape[1]), axis=0)


def wide(v, width):
    col = jnp.broadcast_to(v, (v.shape[0], LANES))
    return jnp.concatenate([col] * (width // LANES), axis=1)


def params(limit=None, **more):
    return pltpu.CompilerParams(vmem_limit_bytes=limit, **more)


def proj_kernel(tok_ref, gain_ref, wx_ref, normed_ref, xbc_ref, dt_ref):
    u = tok_ref[...].astype(f32)
    r = lax.rsqrt(jnp.mean(u * u, axis=-1, keepdims=True) + EPS)
    normed = (u * r * gain_ref[...]).astype(bf16)
    normed_ref[...] = normed
    out = dot(normed, wx_ref[...])
    ch = xbc_ref.shape[1]
    xbc_ref[...] = out[:, :ch]
    dt_ref[...] = out[:, ch:]


def project(tok, gain, wx, channels, tile=256):
    rows, width = tok.shape
    cols = wx.shape[1]
    return pl.pallas_call(
        proj_kernel,
        grid=(rows // tile,),
        in_specs=[
            pl.BlockSpec((tile, width), lambda i: (i, 0)),
            pl.BlockSpec((1, width), lambda i: (0, 0)),
            pl.BlockSpec((width, cols), lambda i: (0, 0)),
        ],
        out_specs=[
            pl.BlockSpec((tile, width), lambda i: (i, 0)),
            pl.BlockSpec((tile, channels), lambda i: (i, 0)),
            pl.BlockSpec((tile, cols - channels), lambda i: (i, 0)),
        ],
        out_shape=[
            jax.ShapeDtypeStruct((rows, width), bf16),
            jax.ShapeDtypeStruct((rows, channels), f32),
            jax.ShapeDtypeStruct((rows, cols - channels), f32),
        ],
        compiler_params=params(60 << 20),
        name="project",
    )(tok, gain, wx)


def table_columns(tab_ref):
    tab = tab_ref[...]
    reps = LANES // tab.shape[0]
    return tab, jnp.concatenate([tab] * reps, axis=0).T


def step_terms(dt, dtb, na2, tri, cols):
    raw = dt + dtb
    ts = jnp.maximum(raw, 0.0) + jnp.log1p(jnp.exp(-jnp.abs(raw)))
    cum = dot(jnp.concatenate([tri] * 3, axis=1), jnp.concatenate(split(ts * na2, 3), axis=0))
    start = jnp.exp2(cum) * wide(cols[:, 4:5], LANES)
    end = jnp.exp2(cum[Q - 1 : Q, :] - cum) * wide(cols[:, 5:6], LANES)
    return raw, ts, cum, start, end


def expand_operand(*terms):
    return jnp.concatenate([jnp.concatenate(split(t, 2), axis=1) for t in terms], axis=0)


def by_head(v, left):
    zero = jnp.zeros_like(v)
    return jnp.concatenate([jnp.where(left, v, zero), jnp.where(left, zero, v)], axis=0)


def fwd_kernel(
    tab_ref, xbc_ref, dt_ref, cw_ref, cb_ref, dtb_ref, na2_ref, skip_ref, e_ref, tri_ref,
    y_ref, s_ref, sin_ref, state, ext,
):
    inner = skip_ref.shape[1]
    channels = cb_ref.shape[1]
    b = pl.program_id(1)

    @pl.when(b == 0)
    def _():
        state[...] = jnp.zeros_like(state)
        ext[0:8, :] = jnp.zeros((8, channels), f32)

    @pl.when(b > 0)
    def _():
        ext[0:8, :] = ext[Q : Q + 8, :]

    ext[8 : 8 + Q, :] = xbc_ref[...]
    tab, cols = table_columns(tab_ref)
    m1, m2, m3 = (wide(cols[:, k : k + 1], 256) for k in (1, 2, 3))

    def conv(c):
        at = pl.ds(c, 256)
        s = cb_ref[:, at] + cw_ref[3:4, at] * ext[8 : 8 + Q, at]
        s += m1 * (cw_ref[2:3, at] * ext[7 : 7 + Q, at])
        s += m2 * (cw_ref[1:2, at] * ext[6 : 6 + Q, at])
        s += m3 * (cw_ref[0:1, at] * ext[5 : 5 + Q, at])
        s_ref[:, at] = s
        return s * sigmoid(s)

    bc, bc_rest = split(conv(inner), 2)
    bm, cm = bc[:, :LANES], bc[:, LANES:]
    bt = bm.T
    c_two = jnp.concatenate([cm, bc_rest[:, LANES:]], axis=1)
    _, ts, cum, start, end = step_terms(dt_ref[...], dtb_ref[...], na2_ref[...], tri_ref[...], cols)
    cum_t = cum.T
    grow = expand_operand(start, end, ts)
    row_i = lax.broadcasted_iota(jnp.int32, (Q, Q), 0)
    col_j = lax.broadcasted_iota(jnp.int32, (Q, Q), 1)
    same = wide(cols[:, 0:1], LANES) == tab[0:1, :]
    mask = jnp.where(same & (row_i >= col_j), 0.0, NEG)
    scores = dot_split((cm, bc_rest[:, LANES:]), (bm, bc_rest[:, :LANES]))
    left = col_j < LANES // 2

    for c in range(0, inner, 256):
        at = pl.ds(c, 256)
        x = conv(c)
        big = dot(grow, e_ref[:, at])
        s_e, e_e, t_e = big[:Q], big[Q : 2 * Q], big[2 * Q :]
        xs = x * t_e
        xs_low = xs.astype(bf16)
        st = state[:, at]
        st_low = st.astype(bf16)
        sin_ref[:, at] = st_low
        carried = dot(c_two, twice(st_low, 0))
        parts = []
        for p in range(2):
            mats = []
            for h in range(2):
                head = (c + p * LANES) // 64 + h
                gap = wide(cum[:, head : head + 1], LANES) - cum_t[head : head + 1, :] + mask
                mats.append((jnp.exp2(gap) * scores).astype(bf16))
            xp = xs_low[:, p * LANES : (p + 1) * LANES]
            parts.append(dot(jnp.concatenate(mats, axis=1), by_head(xp, left)))
        y = jnp.concatenate(parts, axis=1) + s_e * carried + skip_ref[:, at] * x
        y_ref[:, at] = y
        state[:, at] = st * s_e[Q - 1 : Q, :] + dot(bt, (xs * e_e).astype(bf16))


def fixed(shape):
    return pl.BlockSpec(shape, lambda *_: (0,) * len(shape))


def state_forward(tab, xbc, dt, cw, cb, dtb, na2, skip, e2, tri, seqs):
    rows, channels = xbc.shape
    inner = skip.shape[1]
    blocks = rows // seqs // Q
    at = lambda s, b: (s * blocks + b, 0)
    at3 = lambda s, b: (s * blocks + b, 0, 0)
    return pl.pallas_call(
        fwd_kernel,
        grid=(seqs, blocks),
        in_specs=[
            pl.BlockSpec((None, 16, LANES), at3),
            pl.BlockSpec((Q, channels), at),
            pl.BlockSpec((Q, LANES), at),
            fixed(cw.shape), fixed(cb.shape), fixed(dtb.shape), fixed(na2.shape), fixed(skip.shape),
            fixed(e2.shape), fixed(tri.shape),
        ],
        out_specs=[
            pl.BlockSpec((Q, inner), at),
            pl.BlockSpec((Q, channels), at),
            pl.BlockSpec((None, LANES, inner), at3),
        ],
        out_shape=[
            jax.ShapeDtypeStruct((rows, inner), f32),
            jax.ShapeDtypeStruct((rows, channels), f32),
            jax.ShapeDtypeStruct((seqs * blocks, LANES, inner), bf16),
        ],
        scratch_shapes=[pltpu.VMEM((LANES, inner), f32), pltpu.VMEM((Q + 8, channels), f32)],
        compiler_params=params(60 << 20),
        name="state_forward",
    )(tab, xbc, dt, cw, cb, dtb, na2, skip, e2, tri)


def gate_kernel(
    tok_ref, normed_ref, y_ref, cot_ref, wz_ref, wo_ref, gain_ref,
    gn_ref, out_ref, gz_ref, gm_ref, ggain_ref,
):
    z = dot(normed_ref[...], wz_ref[...])
    sg = sigmoid(z)
    sz = z * sg
    y = y_ref[...]
    gated = y * sz
    rstd = lax.rsqrt(jnp.mean(gated * gated, axis=-1, keepdims=True) + EPS)
    unit = gated * rstd
    gn = (unit * gain_ref[...]).astype(bf16)
    gn_ref[...] = gn
    out_ref[...] = (tok_ref[...].astype(f32) + dot(gn, wo_ref[...])).astype(bf16)
    g_gn = dot(cot_ref[...], wo_ref[...], NT)

    @pl.when(pl.program_id(0) == 0)
    def _():
        ggain_ref[...] = jnp.zeros_like(ggain_ref)

    ggain_ref[...] += fold_rows(unit * g_gn)
    q = g_gn * gain_ref[...]
    mean = jnp.mean(unit * q, axis=-1, keepdims=True)
    g_gated = rstd * (q - unit * mean)
    gm_ref[...] = g_gated * sz
    gz_ref[...] = (g_gated * y * (sg * (1.0 + z * (1.0 - sg)))).astype(bf16)


def gate(tok, normed, y, cot, wz, wo, gain, tile=256):
    rows, width = tok.shape
    inner = y.shape[1]
    at = lambda i: (i, 0)
    return pl.pallas_call(
        gate_kernel,
        grid=(rows // tile,),
        in_specs=[
            pl.BlockSpec((tile, width), at),
            pl.BlockSpec((tile, width), at),
            pl.BlockSpec((tile, inner), at),
            pl.BlockSpec((tile, width), at),
            fixed(wz.shape), fixed(wo.shape), fixed(gain.shape),
        ],
        out_specs=[
            pl.BlockSpec((tile, inner), at),
            pl.BlockSpec((tile, width), at),
            pl.BlockSpec((tile, inner), at),
            pl.BlockSpec((tile, inner), at),
            fixed((8, inner)),
        ],
        out_shape=[
            jax.ShapeDtypeStruct((rows, inner), bf16),
            jax.ShapeDtypeStruct((rows, width), bf16),
            jax.ShapeDtypeStruct((rows, inner), bf16),
            jax.ShapeDtypeStruct((rows, inner), f32),
            jax.ShapeDtypeStruct((8, inner), f32),
        ],
        compiler_params=params(60 << 20),
        name="gate",
    )(tok, normed, y, cot, wz, wo, gain)


def bwd_kernel(
    tab_ref, xbc_ref, dt_ref, s_ref, sin_ref, gm_ref, cw_ref, dtb_ref, na2_ref, na_ref, skip_ref,
    e_ref, et_ref, tri_ref, tail_ref, pair_ref,
    gx_ref, gcw_ref, gcb_ref, gskip_ref, galog_ref, gdtb_ref,
    adj, gext, da_rows, edge, spread, grad_b, grad_c, link,
):
    inner = skip_ref.shape[1]
    channels = s_ref.shape[1]
    heads = inner // 64
    b = pl.program_id(1)

    @pl.when((b == 0) & (pl.program_id(0) == 0))
    def _():
        for ref in (gcw_ref, gcb_ref, gskip_ref, galog_ref, gdtb_ref, da_rows):
            ref[...] = jnp.zeros_like(ref)

    @pl.when(b == 0)
    def _():
        adj[...] = jnp.zeros_like(adj)
        gext[Q : Q + 8, :] = jnp.zeros((8, channels), f32)

    @pl.when(b > 0)
    def _():
        gext[Q : Q + 8, :] = gext[0:8, :]

    tab, cols = table_columns(tab_ref)
    raw, ts, cum, start, end = step_terms(
        dt_ref[...], dtb_ref[...], na2_ref[...], tri_ref[...], cols
    )
    cum_t = cum.T
    grow = expand_operand(start, end, ts)

    def act(c):
        s = s_ref[:, pl.ds(c, 256)]
        sg = sigmoid(s)
        return s * sg, sg * (1.0 + s * (1.0 - sg))

    bc, slope_bc = act(inner)
    bc, bc_rest = split(bc, 2)
    bm, cm = bc[:, :LANES], bc[:, LANES:]
    ct = cm.T
    b_two = jnp.concatenate([bm, bc_rest[:, :LANES]], axis=1)
    c_two = jnp.concatenate([cm, bc_rest[:, LANES:]], axis=1)
    row_j = lax.broadcasted_iota(jnp.int32, (Q, Q), 0)
    col_i = lax.broadcasted_iota(jnp.int32, (Q, Q), 1)
    same = wide(cols[:, 0:1], LANES) == tab[0:1, :]
    mask = jnp.where(same & (col_i >= row_j), 0.0, NEG)
    before = (row_j < col_i).astype(f32)
    scores = dot_split((bm, bc_rest[:, :LANES]), (cm, bc_rest[:, LANES:]))
    left = col_i < LANES // 2
    grad_scores = jnp.zeros((Q, Q), f32)

    for c in range(0, inner, 256):
        at = pl.ds(c, 256)
        x, slope = act(c)
        big = dot(grow, e_ref[:, at])
        s_e, e_e, t_e = big[:Q], big[Q : 2 * Q], big[2 * Q :]
        xs = x * t_e
        xs_low, xs_rest = split(xs, 2)
        gm = gm_ref[:, at]
        gm_low, gm_rest = split(gm, 2)
        ad = adj[:, at]
        ad_low, ad_rest = split(ad, 2)
        st_low = sin_ref[:, at]
        into = dot(b_two, twice(ad_low, 0)) + dot(bm, ad_rest)
        carried = dot(c_two, twice(st_low, 0))
        parts = []
        for p in range(2):
            lanes = slice(p * LANES, (p + 1) * LANES)
            diag, diag_rest = by_head(gm_low[:, lanes], left), by_head(gm_rest[:, lanes], left)
            gmat = dot_split((xs_low[:, lanes], xs_rest[:, lanes]), (diag, diag_rest))
            mats, links = [], []
            for h in range(2):
                head = (c + p * LANES) // 64 + h
                gap = cum_t[head : head + 1, :] - wide(cum[:, head : head + 1], LANES) + mask
                decay = jnp.exp2(gap)
                mat = decay * scores
                grad = gmat[:, h * LANES : (h + 1) * LANES]
                grad_scores += decay * grad
                mats.append(split(mat, 2))
                links.append((mat * grad).astype(bf16))
            high = jnp.concatenate([mats[0][0], mats[1][0]], axis=1)
            rest = jnp.concatenate([mats[0][1], mats[1][1]], axis=1)
            parts.append(dot(high, diag) + dot(high, diag_rest) + dot(rest, diag))
            reach = dot(jnp.concatenate(links, axis=1), pair_ref[...])
            for h in range(2):
                head = (c + p * LANES) // 64 + h
                da_rows[head : head + 1, :] = jnp.sum(
                    reach[:, h * LANES : (h + 1) * LANES] * before, axis=0, keepdims=True
                )
        g_xs = jnp.concatenate(parts, axis=1) + e_e * into
        gext[0:Q, at] = (t_e * g_xs + skip_ref[:, at] * gm) * slope
        sums = jnp.concatenate(
            [pair_split(carried * gm), pair_split(x * into), pair_split(x * g_xs)], axis=0
        )
        sums = dot(sums, twice(et_ref[at, :], 0))
        s_gm = (s_e * gm).astype(bf16)
        part_c = dot(s_gm, st_low, NT)
        part_b = dot((e_e * xs).astype(bf16), ad_low, NT)
        if c == 0:
            spread[...] = sums
            grad_c[...] = part_c
            grad_b[...] = part_b
        else:
            spread[...] += sums
            grad_c[...] += part_c
            grad_b[...] += part_b
        gskip_ref[:, at] += fold_rows(gm * x)
        link[:, at] = fold_rows(st_low.astype(f32) * ad)
        adj[:, at] = ad * s_e[Q - 1 : Q, :] + dot(ct, s_gm)

    grad_low = grad_scores.astype(bf16)
    g_b = grad_b[...] + dot(grad_low, cm)
    g_c = grad_c[...] + dot(grad_low, bm, TN)
    gext[0:Q, pl.ds(inner, 256)] = jnp.concatenate([g_b, g_c], axis=1) * slope_bc

    phi = start * spread[0:Q]
    psi = end * ts * spread[Q : 2 * Q]
    through = jnp.sum(dot(jnp.concatenate(split(link[...], 2), axis=0), et_ref[...]), axis=0, keepdims=True)
    around = jnp.concatenate(split(phi, 2) + split(psi, 2), axis=0)
    da = da_rows[...].T + dot(tail_ref[...], around) + start[Q - 1 : Q, :] * through
    g_ts = spread[2 * Q :] + na_ref[...] * da
    galog_ref[...] += fold_rows(ts * na_ref[...] * da)
    g_dt = g_ts * sigmoid(raw)
    gdtb_ref[...] += fold_rows(g_dt)

    n1, n2, n3 = (wide(cols[:, k : k + 1], 256) for k in (6, 7, 8))
    for c in range(0, channels, 256):
        at = pl.ds(c, 256)
        x = xbc_ref[:, at]
        g0 = gext[0:Q, at]
        g1 = gext[1 : 1 + Q, at] * n1
        g2 = gext[2 : 2 + Q, at] * n2
        g3 = gext[3 : 3 + Q, at] * n3
        gx = cw_ref[3:4, at] * g0 + cw_ref[2:3, at] * g1 + cw_ref[1:2, at] * g2 + cw_ref[0:1, at] * g3
        gx_ref[:, at] = gx.astype(bf16)
        gcb_ref[:, at] += fold_rows(g0)
        gcw_ref[24:32, at] += fold_rows(g0 * x)
        gcw_ref[16:24, at] += fold_rows(g1 * x)
        gcw_ref[8:16, at] += fold_rows(g2 * x)
        gcw_ref[0:8, at] += fold_rows(g3 * x)
    gx_ref[:, channels:] = g_dt.astype(bf16)


def state_backward(tab, xbc, dt, s, sin, gm, cw, dtb, na2, na, skip, e2, et, tri, tail, pair, seqs):
    rows, channels = xbc.shape
    inner = skip.shape[1]
    blocks = rows // seqs // Q
    at = lambda s, b: (s * blocks + blocks - 1 - b, 0)
    at3 = lambda s, b: (s * blocks + blocks - 1 - b, 0, 0)
    return pl.pallas_call(
        bwd_kernel,
        grid=(seqs, blocks),
        in_specs=[
            pl.BlockSpec((None, 16, LANES), at3),
            pl.BlockSpec((Q, channels), at),
            pl.BlockSpec((Q, LANES), at),
            pl.BlockSpec((Q, channels), at),
            pl.BlockSpec((None, LANES, inner), at3),
            pl.BlockSpec((Q, inner), at),
        ]
        + [fixed(v.shape) for v in (cw, dtb, na2, na, skip, e2, et, tri, tail, pair)],
        out_specs=[
            pl.BlockSpec((Q, channels + LANES), at),
            fixed((32, channels)), fixed((8, channels)), fixed((8, inner)), fixed((8, LANES)), fixed((8, LANES)),
        ],
        out_shape=[
            jax.ShapeDtypeStruct((rows, channels + LANES), bf16),
            jax.ShapeDtypeStruct((32, channels), f32),
            jax.ShapeDtypeStruct((8, channels), f32),
            jax.ShapeDtypeStruct((8, inner), f32),
            jax.ShapeDtypeStruct((8, LANES), f32),
            jax.ShapeDtypeStruct((8, LANES), f32),
        ],
        scratch_shapes=[
            pltpu.VMEM((LANES, inner), f32),
            pltpu.VMEM((Q + 8, channels), f32),
            pltpu.VMEM((LANES, LANES), f32),
            pltpu.VMEM((8, LANES), f32),
            pltpu.VMEM((3 * Q, LANES), f32),
            pltpu.VMEM((Q, LANES), f32),
            pltpu.VMEM((Q, LANES), f32),
            pltpu.VMEM((8, inner), f32),
        ],
        compiler_params=params(60 << 20),
        name="state_backward",
    )(tab, xbc, dt, s, sin, gm, cw, dtb, na2, na, skip, e2, et, tri, tail, pair)


def token_kernel(tok_ref, cot_ref, gz_ref, gx_ref, wz_ref, wx_ref, gain_ref, out_ref, ggain_ref):
    g = dot(gz_ref[...], wz_ref[...], NT) + dot(gx_ref[...], wx_ref[...], NT)
    u = tok_ref[...].astype(f32)
    r = lax.rsqrt(jnp.mean(u * u, axis=-1, keepdims=True) + EPS)
    unit = u * r

    @pl.when(pl.program_id(0) == 0)
    def _():
        ggain_ref[...] = jnp.zeros_like(ggain_ref)

    ggain_ref[...] += fold_rows(unit * g)
    q = g * gain_ref[...]
    mean = jnp.mean(unit * q, axis=-1, keepdims=True)
    out_ref[...] = (cot_ref[...].astype(f32) + r * (q - unit * mean)).astype(bf16)


def token_grad(tok, cot, gz, gx, wz, wx, gain, tile=256):
    rows, width = tok.shape
    at = lambda i: (i, 0)
    return pl.pallas_call(
        token_kernel,
        grid=(rows // tile,),
        in_specs=[
            pl.BlockSpec((tile, width), at),
            pl.BlockSpec((tile, width), at),
            pl.BlockSpec((tile, gz.shape[1]), at),
            pl.BlockSpec((tile, gx.shape[1]), at),
            fixed(wz.shape), fixed(wx.shape), fixed(gain.shape),
        ],
        out_specs=[pl.BlockSpec((tile, width), at), fixed((8, width))],
        out_shape=[jax.ShapeDtypeStruct((rows, width), bf16), jax.ShapeDtypeStruct((8, width), f32)],
        compiler_params=params(60 << 20),
        name="token_grad",
    )(tok, cot, gz, gx, wz, wx, gain)


def segment_table(segments):
    seqs, length = segments.shape
    seg = segments.astype(f32)
    blocks = length // Q

    def earlier(k):
        return jnp.concatenate([jnp.full((seqs, k), -1.0, f32), seg[:, :-k]], axis=1)

    def later(k):
        return jnp.concatenate([seg[:, k:], jnp.full((seqs, k), -1.0, f32)], axis=1)

    by_block = seg.reshape(seqs, blocks, Q)
    last = by_block[:, :, -1]
    prev = jnp.concatenate([jnp.full((seqs, 1), -1.0, f32), last[:, :-1]], axis=1)
    rows = [seg]
    rows += [(earlier(k) == seg).astype(f32) for k in (1, 2, 3)]
    rows += [(by_block == prev[..., None]).astype(f32).reshape(seqs, length)]
    rows += [(by_block == last[..., None]).astype(f32).reshape(seqs, length)]
    rows += [(later(k) == seg).astype(f32) for k in (1, 2, 3)]
    rows += [jnp.zeros_like(seg)] * (16 - len(rows))
    return jnp.stack(rows, axis=0).reshape(16, seqs * blocks, Q).transpose(1, 0, 2)


def per_device(
    tokens, segments, cotangent, norm_gain, weight_in, conv_weight, conv_bias, dt_bias, a_log, skip_d,
    gate_gain, weight_out,
):
    seqs, length, width = tokens.shape
    rows = seqs * length
    inner = gate_gain.shape[0]
    channels = conv_bias.shape[0]
    heads = dt_bias.shape[0]
    tok = tokens.reshape(rows, width)
    cot = cotangent.reshape(rows, width)
    pad = LANES - heads

    local_x = jnp.pad(weight_in[:, inner:], ((0, 0), (0, pad)))
    wx = lax.all_gather(local_x, "dp", axis=0, tiled=True)
    wz = lax.all_gather(weight_in[:, :inner], "dp", axis=0, tiled=True)
    wo = lax.all_gather(weight_out, "dp", axis=0, tiled=True)

    def row(v):
        return jnp.pad(v, (0, pad)).reshape(1, LANES)

    tab = segment_table(segments)
    neg_rate = -jnp.exp(a_log)
    na, na2 = row(neg_rate), row(neg_rate * LOG2E)
    dtb = row(dt_bias)
    head_of = jnp.arange(inner) // (inner // heads)
    skip = skip_d[head_of].reshape(1, inner)
    et = (head_of[:, None] == jnp.arange(LANES)[None, :]).astype(bf16)
    e2 = jnp.concatenate([et.T, et.T], axis=0)
    pos = jnp.arange(Q)
    tri = (pos[:, None] >= pos[None, :]).astype(bf16)
    below = (pos[:, None] > pos[None, :]).astype(bf16)
    tail = jnp.concatenate([tri.T, tri.T, below, below], axis=1)
    pair = jnp.kron(jnp.eye(2, dtype=f32), tri.astype(f32)).astype(bf16)
    cb = conv_bias.reshape(1, channels)
    ngain = norm_gain.reshape(1, width)
    ggain = gate_gain.reshape(1, inner)

    normed, xbc, dt = project(tok, ngain, wx, channels)
    y, s, sin = state_forward(tab, xbc, dt, conv_weight, cb, dtb, na2, skip, e2, tri, seqs)
    gn, out, gz, gm, p_ggain = gate(tok, normed, y, cot, wz, wo, ggain)
    d_out = dot(gn, cot, TN).astype(bf16)
    d_z = dot(normed, gz, TN).astype(bf16)
    d_out = lax.psum_scatter(d_out, "dp", scatter_dimension=0, tiled=True)
    d_z = lax.psum_scatter(d_z, "dp", scatter_dimension=0, tiled=True)
    gx, p_cw, p_cb, p_skip, p_alog, p_dtb = state_backward(
        tab, xbc, dt, s, sin, gm, conv_weight, dtb, na2, na, skip, e2, et, tri, tail, pair, seqs
    )
    d_x = dot(normed, gx, TN).astype(bf16)
    d_x = lax.psum_scatter(d_x, "dp", scatter_dimension=0, tiled=True)
    g_tok, p_ngain = token_grad(tok, cot, gz, gx, wz, wx, ngain)

    d_in = jnp.concatenate([d_z, d_x], axis=1)
    d_in = lax.psum(d_in, "seq").astype(f32)[:, : weight_in.shape[1]]
    d_out = lax.psum(d_out, "seq").astype(f32)
    small = (
        jnp.sum(p_ngain, axis=0),
        jnp.sum(p_cw.reshape(4, 8, channels), axis=1),
        jnp.sum(p_cb, axis=0),
        jnp.sum(p_dtb, axis=0)[:heads],
        jnp.sum(p_alog, axis=0)[:heads],
        jnp.sum(p_skip.reshape(8, heads, inner // heads), axis=(0, 2)),
        jnp.sum(p_ggain, axis=0),
    )
    s_ngain, s_cw, s_cb, s_dtb, s_alog, s_skip, s_ggain = lax.psum(small, ("dp", "seq"))
    return (
        out.reshape(tokens.shape), g_tok.reshape(tokens.shape), s_ngain, d_in, s_cw, s_cb, s_dtb, s_alog,
        s_skip, s_ggain, d_out,
    )


def solution(mesh):
    data = P(("dp", "seq"), None, None)
    owned = P("dp", None)
    placed = (data, P(("dp", "seq"), None), data, P(), owned, P(), P(), P(), P(), P(), P(), owned)
    return jax.shard_map(
        per_device,
        mesh=mesh,
        in_specs=placed,
        out_specs=(data, data, P(), owned, P(), P(), P(), P(), P(), P(), owned),
        check_vma=False,
    )
```

```python
import functools
import math

import jax
import jax.numpy as jnp
from jax import lax
from jax.experimental import pallas as pl
from jax.experimental.pallas import tpu as pltpu
from jax.sharding import PartitionSpec as P

f32 = jnp.float32
bf16 = jnp.bfloat16
HEAD = 64
Q = 128
LANES = 128
EPS = 1e-05
LOG2E = math.log2(math.e)
NEG = -1e30

NN = (((1,), (0,)), ((), ()))
NT = (((1,), (1,)), ((), ()))
TN = (((0,), (0,)), ((), ()))


def dot(a, b, dims=NN):
    return lax.dot_general(a, b, dims, preferred_element_type=f32)


def pair_split(v):
    return jnp.concatenate(split(v, 2), axis=1)


def twice(v, axis):
    return jnp.concatenate([v, v], axis=axis)


def dot_split(a, b):
    low = b[1]
    return dot(jnp.concatenate(a, axis=1), twice(b[0], 1), NT) + dot(a[0], low, NT)


def sigmoid(v):
    return 0.5 + 0.5 * jnp.tanh(0.5 * v)


def split(v, parts):
    out = []
    for _ in range(parts):
        low = v.astype(bf16)
        out.append(low)
        v = v - low.astype(f32)
    return out


def fold_rows(v):
    return jnp.sum(v.reshape(v.shape[0] // 8, 8, v.shape[1]), axis=0)


def wide(v, width):
    col = jnp.broadcast_to(v, (v.shape[0], LANES))
    return jnp.concatenate([col] * (width // LANES), axis=1)


def params(limit=None, **more):
    return pltpu.CompilerParams(vmem_limit_bytes=limit, **more)


def proj_kernel(tok_ref, gain_ref, wx_ref, normed_ref, xbc_ref, dt_ref):
    u = tok_ref[...].astype(f32)
    r = lax.rsqrt(jnp.mean(u * u, axis=-1, keepdims=True) + EPS)
    normed = (u * r * gain_ref[...]).astype(bf16)
    normed_ref[...] = normed
    out = dot(normed, wx_ref[...])
    ch = xbc_ref.shape[1]
    xbc_ref[...] = out[:, :ch]
    dt_ref[...] = out[:, ch:]


def project(tok, gain, wx, channels, tile=256):
    rows, width = tok.shape
    cols = wx.shape[1]
    return pl.pallas_call(
        proj_kernel,
        grid=(rows // tile,),
        in_specs=[
            pl.BlockSpec((tile, width), lambda i: (i, 0)),
            pl.BlockSpec((1, width), lambda i: (0, 0)),
            pl.BlockSpec((width, cols), lambda i: (0, 0)),
        ],
        out_specs=[
            pl.BlockSpec((tile, width), lambda i: (i, 0)),
            pl.BlockSpec((tile, channels), lambda i: (i, 0)),
            pl.BlockSpec((tile, cols - channels), lambda i: (i, 0)),
        ],
        out_shape=[
            jax.ShapeDtypeStruct((rows, width), bf16),
            jax.ShapeDtypeStruct((rows, channels), f32),
            jax.ShapeDtypeStruct((rows, cols - channels), f32),
        ],
        compiler_params=params(60 << 20),
        name="project",
    )(tok, gain, wx)


def segment_rows(seg_ref, block, blocks, at):
    rows = seg_ref.shape[0]
    none = jnp.full((1, LANES), -1.0, f32)
    seg = seg_ref[pl.ds(at, 1), :]
    prev = jnp.where(block > 0, seg_ref[pl.ds(jnp.maximum(at - 1, 0), 1), :], none)
    after = jnp.where(block < blocks - 1, seg_ref[pl.ds(jnp.minimum(at + 1, rows - 1), 1), :], none)
    lane = lax.broadcasted_iota(jnp.int32, (1, LANES), 1)

    def same(other):
        return (other == seg).astype(f32)

    out = [seg]
    for k in (1, 2, 3):
        out.append(same(jnp.where(lane < k, pltpu.roll(prev, k, 1), pltpu.roll(seg, k, 1))))
    out.append(same(jnp.broadcast_to(prev[:, LANES - 1 :], (1, LANES))))
    out.append(same(jnp.broadcast_to(seg[:, LANES - 1 :], (1, LANES))))
    for k in (1, 2, 3):
        turn = LANES - k
        out.append(same(jnp.where(lane >= turn, pltpu.roll(after, turn, 1), pltpu.roll(seg, turn, 1))))
    tab = jnp.concatenate(out + [none] * (16 - len(out)), axis=0)
    return seg, jnp.concatenate([tab] * (LANES // 16), axis=0).T


def iota(shape, axis):
    return lax.broadcasted_iota(jnp.int32, shape, axis)


def ones_where(cond):
    return jnp.where(cond, 1.0, 0.0).astype(bf16)


def head_columns(heads_wide, inner, width):
    return ones_where(iota((heads_wide, inner), 0) % LANES == iota((heads_wide, inner), 1) // width)


def step_terms(dt, dtb, na2, tri, cols):
    raw = dt + dtb
    ts = jnp.maximum(raw, 0.0) + jnp.log1p(jnp.exp(-jnp.abs(raw)))
    cum = dot(jnp.concatenate([tri] * 3, axis=1), jnp.concatenate(split(ts * na2, 3), axis=0))
    start = jnp.exp2(cum) * wide(cols[:, 4:5], LANES)
    end = jnp.exp2(cum[Q - 1 : Q, :] - cum) * wide(cols[:, 5:6], LANES)
    return raw, ts, cum, start, end


def head_terms(head_ref):
    rate = head_ref[1:2, :]
    return head_ref[0:1, :], rate, rate * LOG2E


def fill_constants(e_ref, tri_ref, skip_ref, head_ref):
    inner = e_ref.shape[1]
    e_ref[...] = head_columns(e_ref.shape[0], inner, HEAD)
    tri_ref[...] = ones_where(iota((Q, Q), 0) >= iota((Q, Q), 1))
    skip = jnp.broadcast_to(head_ref[2:3, :], (8, LANES))
    wide_skip = dot(jnp.concatenate(split(skip, 3), axis=1), head_columns(3 * LANES, inner, HEAD))
    skip_ref[...] = wide_skip[0:1]


def expand_operand(*terms):
    return jnp.concatenate([jnp.concatenate(split(t, 2), axis=1) for t in terms], axis=0)


def by_head(v, left):
    zero = jnp.zeros_like(v)
    return jnp.concatenate([jnp.where(left, v, zero), jnp.where(left, zero, v)], axis=0)


def fwd_kernel(
    seg_ref, xbc_ref, dt_ref, cw_ref, cb_ref, head_ref,
    y_ref, s_ref, sin_ref, state, ext, e_ref, tri_ref, skip_ref,
):
    inner = y_ref.shape[1]
    channels = cb_ref.shape[1]
    b, blocks = pl.program_id(1), pl.num_programs(1)
    dtb, _, na2 = head_terms(head_ref)

    @pl.when((b == 0) & (pl.program_id(0) == 0))
    def _():
        fill_constants(e_ref, tri_ref, skip_ref, head_ref)

    @pl.when(b == 0)
    def _():
        state[...] = jnp.zeros_like(state)
        ext[0:8, :] = jnp.zeros((8, channels), f32)

    @pl.when(b > 0)
    def _():
        ext[0:8, :] = ext[Q : Q + 8, :]

    ext[8 : 8 + Q, :] = xbc_ref[...]
    seg, cols = segment_rows(seg_ref, b, blocks, pl.program_id(0) * blocks + b)
    m1, m2, m3 = (wide(cols[:, k : k + 1], 256) for k in (1, 2, 3))

    def conv(c):
        at = pl.ds(c, 256)
        s = cb_ref[:, at] + cw_ref[3:4, at] * ext[8 : 8 + Q, at]
        s += m1 * (cw_ref[2:3, at] * ext[7 : 7 + Q, at])
        s += m2 * (cw_ref[1:2, at] * ext[6 : 6 + Q, at])
        s += m3 * (cw_ref[0:1, at] * ext[5 : 5 + Q, at])
        s_ref[:, at] = s
        return s * sigmoid(s)

    bc, bc_rest = split(conv(inner), 2)
    bm, cm = bc[:, :LANES], bc[:, LANES:]
    bt = bm.T
    c_two = jnp.concatenate([cm, bc_rest[:, LANES:]], axis=1)
    _, ts, cum, start, end = step_terms(dt_ref[...], dtb, na2, tri_ref[...], cols)
    cum_t = cum.T
    grow = expand_operand(start, end, ts)
    row_i = lax.broadcasted_iota(jnp.int32, (Q, Q), 0)
    col_j = lax.broadcasted_iota(jnp.int32, (Q, Q), 1)
    same = wide(cols[:, 0:1], LANES) == seg
    mask = jnp.where(same & (row_i >= col_j), 0.0, NEG)
    scores = dot_split((cm, bc_rest[:, LANES:]), (bm, bc_rest[:, :LANES]))
    left = col_j < HEAD

    for c in range(0, inner, 256):
        at = pl.ds(c, 256)
        x = conv(c)
        big = dot(grow, e_ref[:, at])
        s_e, e_e, t_e = big[:Q], big[Q : 2 * Q], big[2 * Q :]
        xs = x * t_e
        xs_low = xs.astype(bf16)
        st = state[:, at]
        st_low = st.astype(bf16)
        sin_ref[:, at] = st_low
        carried = dot(c_two, twice(st_low, 0))
        parts = []
        for p in range(2):
            mats = []
            for h in range(2):
                head = (c + p * LANES) // HEAD + h
                gap = wide(cum[:, head : head + 1], LANES) - cum_t[head : head + 1, :] + mask
                mats.append((jnp.exp2(gap) * scores).astype(bf16))
            xp = xs_low[:, p * LANES : (p + 1) * LANES]
            parts.append(dot(jnp.concatenate(mats, axis=1), by_head(xp, left)))
        y = jnp.concatenate(parts, axis=1) + s_e * carried + skip_ref[:, at] * x
        y_ref[:, at] = y
        state[:, at] = st * s_e[Q - 1 : Q, :] + dot(bt, (xs * e_e).astype(bf16))


def fixed(shape):
    return pl.BlockSpec(shape, lambda *_: (0,) * len(shape))


def state_forward(seg, xbc, dt, cw, cb, head, inner, seqs):
    rows, channels = xbc.shape
    blocks = rows // seqs // Q
    at = lambda s, b: (s * blocks + b, 0)
    at3 = lambda s, b: (s * blocks + b, 0, 0)
    return pl.pallas_call(
        fwd_kernel,
        grid=(seqs, blocks),
        in_specs=[
            fixed(seg.shape),
            pl.BlockSpec((Q, channels), at),
            pl.BlockSpec((Q, LANES), at),
            fixed(cw.shape), fixed(cb.shape), fixed(head.shape),
        ],
        out_specs=[
            pl.BlockSpec((Q, inner), at),
            pl.BlockSpec((Q, channels), at),
            pl.BlockSpec((None, LANES, inner), at3),
        ],
        out_shape=[
            jax.ShapeDtypeStruct((rows, inner), f32),
            jax.ShapeDtypeStruct((rows, channels), f32),
            jax.ShapeDtypeStruct((seqs * blocks, LANES, inner), bf16),
        ],
        scratch_shapes=[
            pltpu.VMEM((LANES, inner), f32),
            pltpu.VMEM((Q + 8, channels), f32),
            pltpu.VMEM((2 * LANES, inner), bf16),
            pltpu.VMEM((Q, Q), bf16),
            pltpu.VMEM((1, inner), f32),
        ],
        compiler_params=params(60 << 20),
        name="state_forward",
    )(seg, xbc, dt, cw, cb, head)


def flat(ref):
    v = ref[...]
    return v.reshape(v.shape[0] * v.shape[1], v.shape[2])


def slab_views(slab, own):
    owners, _, width = slab.shape
    if own % 16 == 0:
        first = lambda *_: (0, 0, 0)
        second = lambda *_: (0, 1, 0)
        sizes = ((own, first), (own, second), (2 * own, second))
        return [(slab, pl.BlockSpec((owners, n, width), index)) for n, index in sizes]
    parts = [
        v.reshape(1, -1, width) for v in (slab[:, :own], slab[:, own : 2 * own], slab[:, 2 * own :])
    ]
    return [(v, fixed(v.shape)) for v in parts]


def gate_kernel(
    tok_ref, normed_ref, y_ref, cot_ref, wa_ref, wb_ref, wo_ref, gain_ref,
    gn_ref, out_ref, gz_ref, gm_ref, ggain_ref,
):
    normed, wo = normed_ref[...], flat(wo_ref)
    z = jnp.concatenate([dot(normed, flat(wa_ref)), dot(normed, flat(wb_ref))], axis=1)
    sg = sigmoid(z)
    sz = z * sg
    y = y_ref[...]
    gated = y * sz
    rstd = lax.rsqrt(jnp.mean(gated * gated, axis=-1, keepdims=True) + EPS)
    unit = gated * rstd
    gn = (unit * gain_ref[...]).astype(bf16)
    gn_ref[...] = gn
    out_ref[...] = (tok_ref[...].astype(f32) + dot(gn, wo)).astype(bf16)
    g_gn = dot(cot_ref[...], wo, NT)

    @pl.when(pl.program_id(0) == 0)
    def _():
        ggain_ref[...] = jnp.zeros_like(ggain_ref)

    ggain_ref[...] += fold_rows(unit * g_gn)
    q = g_gn * gain_ref[...]
    mean = jnp.mean(unit * q, axis=-1, keepdims=True)
    g_gated = rstd * (q - unit * mean)
    gm_ref[...] = g_gated * sz
    gz_ref[...] = (g_gated * y * (sg * (1.0 + z * (1.0 - sg)))).astype(bf16)


def gate(tok, normed, y, cot, weights, gain, tile=256):
    rows, width = tok.shape
    inner = y.shape[1]
    at = lambda i: (i, 0)
    return pl.pallas_call(
        gate_kernel,
        grid=(rows // tile,),
        in_specs=[
            pl.BlockSpec((tile, width), at),
            pl.BlockSpec((tile, width), at),
            pl.BlockSpec((tile, inner), at),
            pl.BlockSpec((tile, width), at),
            *[spec for _, spec in weights], fixed(gain.shape),
        ],
        out_specs=[
            pl.BlockSpec((tile, inner), at),
            pl.BlockSpec((tile, width), at),
            pl.BlockSpec((tile, inner), at),
            pl.BlockSpec((tile, inner), at),
            fixed((8, inner)),
        ],
        out_shape=[
            jax.ShapeDtypeStruct((rows, inner), bf16),
            jax.ShapeDtypeStruct((rows, width), bf16),
            jax.ShapeDtypeStruct((rows, inner), bf16),
            jax.ShapeDtypeStruct((rows, inner), f32),
            jax.ShapeDtypeStruct((8, inner), f32),
        ],
        compiler_params=params(60 << 20),
        name="gate",
    )(tok, normed, y, cot, *[v for v, _ in weights], gain)


def bwd_kernel(
    seg_ref, xbc_ref, dt_ref, s_ref, sin_ref, gm_ref, cw_ref, head_ref,
    gx_ref, gcw_ref, gcb_ref, gskip_ref, galog_ref, gdtb_ref,
    adj, gext, da_rows, spread, grad_b, grad_c, link, e_ref, tri_ref, skip_ref, et_ref, tail_ref, pair_ref,
):
    inner = gm_ref.shape[1]
    channels = s_ref.shape[1]
    b, blocks = pl.program_id(1), pl.num_programs(1)
    dtb, rate, na2 = head_terms(head_ref)

    @pl.when((b == 0) & (pl.program_id(0) == 0))
    def _():
        for ref in (gcw_ref, gcb_ref, gskip_ref, galog_ref, gdtb_ref, da_rows):
            ref[...] = jnp.zeros_like(ref)
        fill_constants(e_ref, tri_ref, skip_ref, head_ref)
        et_ref[...] = ones_where(iota((inner, LANES), 0) // HEAD == iota((inner, LANES), 1))
        turned = ones_where(iota((Q, Q), 0) <= iota((Q, Q), 1))
        below = ones_where(iota((Q, Q), 0) > iota((Q, Q), 1))
        tail_ref[...] = jnp.concatenate([turned, turned, below, below], axis=1)
        row, col = iota((2 * Q, 2 * Q), 0), iota((2 * Q, 2 * Q), 1)
        pair_ref[...] = ones_where((row // Q == col // Q) & (row >= col))

    @pl.when(b == 0)
    def _():
        adj[...] = jnp.zeros_like(adj)
        gext[Q : Q + 8, :] = jnp.zeros((8, channels), f32)

    @pl.when(b > 0)
    def _():
        gext[Q : Q + 8, :] = gext[0:8, :]

    turn = blocks - 1 - b
    seg, cols = segment_rows(seg_ref, turn, blocks, pl.program_id(0) * blocks + turn)
    raw, ts, cum, start, end = step_terms(dt_ref[...], dtb, na2, tri_ref[...], cols)
    cum_t = cum.T
    grow = expand_operand(start, end, ts)

    def act(c):
        s = s_ref[:, pl.ds(c, 256)]
        sg = sigmoid(s)
        return s * sg, sg * (1.0 + s * (1.0 - sg))

    bc, slope_bc = act(inner)
    bc, bc_rest = split(bc, 2)
    bm, cm = bc[:, :LANES], bc[:, LANES:]
    ct = cm.T
    b_two = jnp.concatenate([bm, bc_rest[:, :LANES]], axis=1)
    c_two = jnp.concatenate([cm, bc_rest[:, LANES:]], axis=1)
    row_j = lax.broadcasted_iota(jnp.int32, (Q, Q), 0)
    col_i = lax.broadcasted_iota(jnp.int32, (Q, Q), 1)
    same = wide(cols[:, 0:1], LANES) == seg
    mask = jnp.where(same & (col_i >= row_j), 0.0, NEG)
    before = (row_j < col_i).astype(f32)
    scores = dot_split((bm, bc_rest[:, :LANES]), (cm, bc_rest[:, LANES:]))
    left = col_i < HEAD
    grad_scores = jnp.zeros((Q, Q), f32)

    for c in range(0, inner, 256):
        at = pl.ds(c, 256)
        x, slope = act(c)
        big = dot(grow, e_ref[:, at])
        s_e, e_e, t_e = big[:Q], big[Q : 2 * Q], big[2 * Q :]
        xs = x * t_e
        xs_low, xs_rest = split(xs, 2)
        gm = gm_ref[:, at]
        gm_low, gm_rest = split(gm, 2)
        ad = adj[:, at]
        ad_low, ad_rest = split(ad, 2)
        st_low = sin_ref[:, at]
        into = dot(b_two, twice(ad_low, 0)) + dot(bm, ad_rest)
        carried = dot(c_two, twice(st_low, 0))
        parts = []
        for p in range(2):
            lanes = slice(p * LANES, (p + 1) * LANES)
            diag, diag_rest = by_head(gm_low[:, lanes], left), by_head(gm_rest[:, lanes], left)
            gmat = dot_split((xs_low[:, lanes], xs_rest[:, lanes]), (diag, diag_rest))
            mats, links = [], []
            for h in range(2):
                head = (c + p * LANES) // HEAD + h
                gap = cum_t[head : head + 1, :] - wide(cum[:, head : head + 1], LANES) + mask
                decay = jnp.exp2(gap)
                mat = decay * scores
                grad = gmat[:, h * LANES : (h + 1) * LANES]
                grad_scores += decay * grad
                mats.append(split(mat, 2))
                links.append((mat * grad).astype(bf16))
            high = jnp.concatenate([mats[0][0], mats[1][0]], axis=1)
            rest = jnp.concatenate([mats[0][1], mats[1][1]], axis=1)
            parts.append(dot(high, diag) + dot(high, diag_rest) + dot(rest, diag))
            reach = dot(jnp.concatenate(links, axis=1), pair_ref[...])
            for h in range(2):
                head = (c + p * LANES) // HEAD + h
                da_rows[head : head + 1, :] = jnp.sum(
                    reach[:, h * LANES : (h + 1) * LANES] * before, axis=0, keepdims=True
                )
        g_xs = jnp.concatenate(parts, axis=1) + e_e * into
        gext[0:Q, at] = (t_e * g_xs + skip_ref[:, at] * gm) * slope
        sums = jnp.concatenate(
            [pair_split(carried * gm), pair_split(x * into), pair_split(x * g_xs)], axis=0
        )
        sums = dot(sums, twice(et_ref[at, :], 0))
        s_gm = (s_e * gm).astype(bf16)
        part_c = dot(s_gm, st_low, NT)
        part_b = dot((e_e * xs).astype(bf16), ad_low, NT)
        if c == 0:
            spread[...] = sums
            grad_c[...] = part_c
            grad_b[...] = part_b
        else:
            spread[...] += sums
            grad_c[...] += part_c
            grad_b[...] += part_b
        gskip_ref[:, at] += fold_rows(gm * x)
        link[:, at] = fold_rows(st_low.astype(f32) * ad)
        adj[:, at] = ad * s_e[Q - 1 : Q, :] + dot(ct, s_gm)

    grad_low = grad_scores.astype(bf16)
    g_b = grad_b[...] + dot(grad_low, cm)
    g_c = grad_c[...] + dot(grad_low, bm, TN)
    gext[0:Q, pl.ds(inner, 256)] = jnp.concatenate([g_b, g_c], axis=1) * slope_bc

    phi = start * spread[0:Q]
    psi = end * ts * spread[Q : 2 * Q]
    through = jnp.sum(dot(jnp.concatenate(split(link[...], 2), axis=0), et_ref[...]), axis=0, keepdims=True)
    around = jnp.concatenate(split(phi, 2) + split(psi, 2), axis=0)
    da = da_rows[...].T + dot(tail_ref[...], around) + start[Q - 1 : Q, :] * through
    g_ts = spread[2 * Q :] + rate * da
    galog_ref[...] += fold_rows(ts * rate * da)
    g_dt = g_ts * sigmoid(raw)
    gdtb_ref[...] += fold_rows(g_dt)

    n1, n2, n3 = (wide(cols[:, k : k + 1], 256) for k in (6, 7, 8))
    for c in range(0, channels, 256):
        at = pl.ds(c, 256)
        x = xbc_ref[:, at]
        g0 = gext[0:Q, at]
        g1 = gext[1 : 1 + Q, at] * n1
        g2 = gext[2 : 2 + Q, at] * n2
        g3 = gext[3 : 3 + Q, at] * n3
        gx = cw_ref[3:4, at] * g0 + cw_ref[2:3, at] * g1 + cw_ref[1:2, at] * g2 + cw_ref[0:1, at] * g3
        gx_ref[:, at] = gx.astype(bf16)
        gcb_ref[:, at] += fold_rows(g0)
        gcw_ref[24:32, at] += fold_rows(g0 * x)
        gcw_ref[16:24, at] += fold_rows(g1 * x)
        gcw_ref[8:16, at] += fold_rows(g2 * x)
        gcw_ref[0:8, at] += fold_rows(g3 * x)
    gx_ref[:, channels:] = g_dt.astype(bf16)


def state_backward(seg, xbc, dt, s, sin, gm, cw, head, seqs):
    rows, channels = xbc.shape
    inner = gm.shape[1]
    blocks = rows // seqs // Q
    at = lambda s, b: (s * blocks + blocks - 1 - b, 0)
    at3 = lambda s, b: (s * blocks + blocks - 1 - b, 0, 0)
    return pl.pallas_call(
        bwd_kernel,
        grid=(seqs, blocks),
        in_specs=[
            fixed(seg.shape),
            pl.BlockSpec((Q, channels), at),
            pl.BlockSpec((Q, LANES), at),
            pl.BlockSpec((Q, channels), at),
            pl.BlockSpec((None, LANES, inner), at3),
            pl.BlockSpec((Q, inner), at),
        ]
        + [fixed(v.shape) for v in (cw, head)],
        out_specs=[
            pl.BlockSpec((Q, channels + LANES), at),
            fixed((32, channels)), fixed((8, channels)), fixed((8, inner)), fixed((8, LANES)), fixed((8, LANES)),
        ],
        out_shape=[
            jax.ShapeDtypeStruct((rows, channels + LANES), bf16),
            jax.ShapeDtypeStruct((32, channels), f32),
            jax.ShapeDtypeStruct((8, channels), f32),
            jax.ShapeDtypeStruct((8, inner), f32),
            jax.ShapeDtypeStruct((8, LANES), f32),
            jax.ShapeDtypeStruct((8, LANES), f32),
        ],
        scratch_shapes=[
            pltpu.VMEM((LANES, inner), f32),
            pltpu.VMEM((Q + 8, channels), f32),
            pltpu.VMEM((LANES, LANES), f32),
            pltpu.VMEM((3 * Q, LANES), f32),
            pltpu.VMEM((Q, LANES), f32),
            pltpu.VMEM((Q, LANES), f32),
            pltpu.VMEM((8, inner), f32),
            pltpu.VMEM((2 * LANES, inner), bf16),
            pltpu.VMEM((Q, Q), bf16),
            pltpu.VMEM((1, inner), f32),
            pltpu.VMEM((inner, LANES), bf16),
            pltpu.VMEM((Q, 4 * Q), bf16),
            pltpu.VMEM((2 * Q, 2 * Q), bf16),
        ],
        compiler_params=params(60 << 20),
        name="state_backward",
    )(seg, xbc, dt, s, sin, gm, cw, head)


def token_kernel(tok_ref, cot_ref, gz_ref, gx_ref, wa_ref, wb_ref, wx_ref, gain_ref, out_ref, ggain_ref):
    half = gz_ref.shape[1] // 2
    g = dot(gz_ref[:, :half], flat(wa_ref), NT) + dot(gz_ref[:, half:], flat(wb_ref), NT)
    g += dot(gx_ref[...], wx_ref[...], NT)
    u = tok_ref[...].astype(f32)
    r = lax.rsqrt(jnp.mean(u * u, axis=-1, keepdims=True) + EPS)
    unit = u * r

    @pl.when(pl.program_id(0) == 0)
    def _():
        ggain_ref[...] = jnp.zeros_like(ggain_ref)

    ggain_ref[...] += fold_rows(unit * g)
    q = g * gain_ref[...]
    mean = jnp.mean(unit * q, axis=-1, keepdims=True)
    out_ref[...] = (cot_ref[...].astype(f32) + r * (q - unit * mean)).astype(bf16)


def token_grad(tok, cot, gz, gx, weights, wx, gain, tile=256):
    rows, width = tok.shape
    at = lambda i: (i, 0)
    return pl.pallas_call(
        token_kernel,
        grid=(rows // tile,),
        in_specs=[
            pl.BlockSpec((tile, width), at),
            pl.BlockSpec((tile, width), at),
            pl.BlockSpec((tile, gz.shape[1]), at),
            pl.BlockSpec((tile, gx.shape[1]), at),
            *[spec for _, spec in weights], fixed(wx.shape), fixed(gain.shape),
        ],
        out_specs=[pl.BlockSpec((tile, width), at), fixed((8, width))],
        out_shape=[jax.ShapeDtypeStruct((rows, width), bf16), jax.ShapeDtypeStruct((8, width), f32)],
        compiler_params=params(60 << 20),
        name="token_grad",
    )(tok, cot, gz, gx, *[v for v, _ in weights], wx, gain)


def partner(axis, bit):
    me = lax.axis_index(axis)
    return {axis: me + bit - 2 * bit * ((me // bit) % 2)}


def finish_kernel(
    steps, heads, cw_ref, cb_ref, ggain_ref, skip_ref, ngain_ref, alog_ref, dtb_ref, zo_ref, x_ref,
    small_ref, din_ref, dout_ref, acc, got, zo_got, x_got, send, recv, big_send, big_recv,
):
    barrier = pltpu.get_barrier_semaphore()
    for axis, bit in steps:
        pl.semaphore_signal(barrier, inc=1, device_id=partner(axis, bit), device_id_type=pl.DeviceIdType.MESH)
    pl.semaphore_wait(barrier, len(steps))

    def exchange(src, dst, ssem, rsem, axis, bit):
        copy = pltpu.make_async_remote_copy(
            src_ref=src, dst_ref=dst, send_sem=ssem, recv_sem=rsem,
            device_id=partner(axis, bit), device_id_type=pl.DeviceIdType.MESH,
        )
        copy.start()
        return copy

    axis, bit = steps[-1]
    big = [
        exchange(zo_ref, zo_got, big_send.at[0], big_recv.at[0], axis, bit),
        exchange(x_ref, x_got, big_send.at[1], big_recv.at[1], axis, bit),
    ]

    inner, width = ggain_ref.shape[1], ngain_ref.shape[1]
    channels = cb_ref.shape[1]
    total = lambda v: jnp.sum(v, axis=0, keepdims=True)
    acc[0] = jnp.zeros((8, channels), f32)
    for k in range(4):
        acc[0, k : k + 1, :] = total(cw_ref[8 * k : 8 * k + 8, :])
    acc[0, 4:5, :] = total(cb_ref[...])
    acc[0, 5:6, :inner] = total(ggain_ref[...])
    acc[0, 6:7, :width] = total(ngain_ref[...])
    acc[0, 6:7, width : width + LANES] = total(alog_ref[...])
    acc[0, 6:7, width + LANES : width + 2 * LANES] = total(dtb_ref[...])
    skip = jnp.concatenate(split(skip_ref[...], 3), axis=0)
    by_head = ones_where(iota((inner, LANES), 0) // HEAD == iota((inner, LANES), 1))
    acc[0, 6:7, width + 2 * LANES : width + 3 * LANES] = total(dot(skip, by_head))

    for k, (axis, bit) in enumerate(steps):
        exchange(acc.at[k], got.at[k], send.at[k], recv.at[k], axis, bit).wait()
        acc[k + 1] = acc[k] + got[k]
    small_ref[...] = acc[len(steps)]

    for copy in big:
        copy.wait()
    own = din_ref.shape[0]
    zo = zo_ref[...].astype(f32) + zo_got[...].astype(f32)
    half = zo.shape[1]
    din_ref[:, :half] = zo[:own]
    din_ref[:, half : 2 * half] = zo[own : 2 * own]
    dout_ref[...] = zo[2 * own :]
    left = din_ref.shape[1] - 2 * half
    din_ref[:, 2 * half :] = (x_ref[...].astype(f32) + x_got[...].astype(f32))[:, :left]


def finish(p_cw, p_cb, p_ggain, p_skip, p_ngain, p_alog, p_dtb, d_zo, d_x, sizes, heads, proj):
    steps = [(axis, 1 << i) for axis, n in sizes for i in range(n.bit_length() - 1)]
    own, half = d_x.shape[0], d_zo.shape[1]
    channels = p_cb.shape[1]
    vmem = pl.BlockSpec(memory_space=pltpu.VMEM)
    return pl.pallas_call(
        functools.partial(finish_kernel, steps, heads),
        in_specs=[vmem] * 9,
        out_specs=[vmem] * 3,
        out_shape=[
            jax.ShapeDtypeStruct((8, channels), f32),
            jax.ShapeDtypeStruct((own, proj), f32),
            jax.ShapeDtypeStruct((2 * own, half), f32),
        ],
        scratch_shapes=[
            pltpu.VMEM((len(steps) + 1, 8, channels), f32),
            pltpu.VMEM((len(steps), 8, channels), f32),
            pltpu.VMEM(d_zo.shape, bf16),
            pltpu.VMEM(d_x.shape, bf16),
            pltpu.SemaphoreType.DMA((len(steps),)),
            pltpu.SemaphoreType.DMA((len(steps),)),
            pltpu.SemaphoreType.DMA((2,)),
            pltpu.SemaphoreType.DMA((2,)),
        ],
        compiler_params=params(48 << 20, collective_id=0, has_side_effects=True),
        name="finish",
    )(p_cw, p_cb, p_ggain, p_skip, p_ngain, p_alog, p_dtb, d_zo, d_x)


def per_device(
    sizes, tokens, segments, cotangent, norm_gain, weight_in, conv_weight, conv_bias, dt_bias, a_log, skip_d,
    gate_gain, weight_out,
):
    seqs, length, width = tokens.shape
    rows = seqs * length
    inner = gate_gain.shape[0]
    channels = conv_bias.shape[0]
    heads = dt_bias.shape[0]
    own = weight_in.shape[0]
    owners = width // own
    tok = tokens.reshape(rows, width)
    cot = cotangent.reshape(rows, width)
    pad = LANES - heads

    local_x = jnp.pad(weight_in[:, inner:], ((0, 0), (0, pad)))
    wx = lax.all_gather(local_x, "dp", axis=0, tiled=True)
    local_zo = jnp.concatenate([weight_in[:, :width], weight_in[:, width:inner], weight_out], axis=0)
    slab = lax.all_gather(local_zo, "dp", axis=0, tiled=True).reshape(owners, 4 * own, width)
    weights = slab_views(slab, own)

    head = jnp.pad(jnp.stack([dt_bias, -jnp.exp(a_log), skip_d]), ((0, 5), (0, pad)))
    seg = segments.astype(f32).reshape(rows // Q, Q)
    cb = conv_bias.reshape(1, channels)
    ngain = norm_gain.reshape(1, width)
    ggain = gate_gain.reshape(1, inner)

    normed, xbc, dt = project(tok, ngain, wx, channels)
    y, s, sin = state_forward(seg, xbc, dt, conv_weight, cb, head, inner, seqs)
    gn, out, gz, gm, p_ggain = gate(tok, normed, y, cot, weights, ggain)
    d_z = dot(normed, gz, TN).astype(bf16)
    d_out = dot(gn, cot, TN).astype(bf16)
    d_zo = jnp.concatenate(
        [
            d_z[:, :width].reshape(owners, own, width),
            d_z[:, width:].reshape(owners, own, width),
            d_out.reshape(owners, 2 * own, width),
        ],
        axis=1,
    ).reshape(owners * 4 * own, width)
    d_zo = lax.psum_scatter(d_zo, "dp", scatter_dimension=0, tiled=True)
    gx, p_cw, p_cb, p_skip, p_alog, p_dtb = state_backward(seg, xbc, dt, s, sin, gm, conv_weight, head, seqs)
    d_x = dot(normed, gx, TN).astype(bf16)
    d_x = lax.psum_scatter(d_x, "dp", scatter_dimension=0, tiled=True)
    g_tok, p_ngain = token_grad(tok, cot, gz, gx, weights[:2], wx, ngain)
    small, d_in, d_out = finish(
        p_cw, p_cb, p_ggain, p_skip, p_ngain, p_alog, p_dtb, d_zo, d_x, sizes, heads, weight_in.shape[1]
    )
    return (
        out.reshape(tokens.shape),
        g_tok.reshape(tokens.shape),
        small[6, :width],
        d_in,
        small[:4],
        small[4],
        small[6, width + LANES : width + LANES + heads],
        small[6, width : width + heads],
        small[6, width + 2 * LANES : width + 2 * LANES + heads],
        small[5, :inner],
        d_out,
    )


def solution(mesh):
    data = P(("dp", "seq"), None, None)
    owned = P("dp", None)
    placed = (data, P(("dp", "seq"), None), data, P(), owned, P(), P(), P(), P(), P(), P(), owned)
    return jax.shard_map(
        functools.partial(per_device, [(axis, mesh.shape[axis]) for axis in ("dp", "seq")]),
        mesh=mesh,
        in_specs=placed,
        out_specs=(data, data, P(), owned, P(), P(), P(), P(), P(), P(), owned),
        check_vma=False,
    )
```

```python
import functools
import math

import jax
import jax.numpy as jnp
from jax import lax
from jax.experimental import pallas as pl
from jax.experimental.pallas import tpu as pltpu
from jax.sharding import PartitionSpec as P

f32 = jnp.float32
bf16 = jnp.bfloat16
HEAD = 64
Q = 128
LANES = 128
EPS = 1e-05
LOG2E = math.log2(math.e)
NEG = -1e30

NN = (((1,), (0,)), ((), ()))
NT = (((1,), (1,)), ((), ()))
TN = (((0,), (0,)), ((), ()))


def dot(a, b, dims=NN):
    return lax.dot_general(a, b, dims, preferred_element_type=f32)


def pair_split(v):
    return jnp.concatenate(split(v, 2), axis=1)


def twice(v, axis):
    return jnp.concatenate([v, v], axis=axis)


def dot_split(a, b):
    low = b[1]
    return dot(jnp.concatenate(a, axis=1), twice(b[0], 1), NT) + dot(a[0], low, NT)


def sigmoid(v):
    return 0.5 + 0.5 * jnp.tanh(0.5 * v)


def split(v, parts):
    out = []
    for _ in range(parts):
        low = v.astype(bf16)
        out.append(low)
        v = v - low.astype(f32)
    return out


def fold_rows(v):
    return jnp.sum(v.reshape(v.shape[0] // 8, 8, v.shape[1]), axis=0)


def wide(v, width):
    col = jnp.broadcast_to(v, (v.shape[0], LANES))
    return jnp.concatenate([col] * (width // LANES), axis=1)


def params(limit=None, **more):
    return pltpu.CompilerParams(vmem_limit_bytes=limit, **more)


def proj_kernel(tok_ref, gain_ref, wx_ref, normed_ref, xbc_ref, dt_ref):
    u = tok_ref[...].astype(f32)
    r = lax.rsqrt(jnp.mean(u * u, axis=-1, keepdims=True) + EPS)
    normed = (u * r * gain_ref[...]).astype(bf16)
    normed_ref[...] = normed
    out = dot(normed, wx_ref[...])
    ch = xbc_ref.shape[1]
    xbc_ref[...] = out[:, :ch]
    dt_ref[...] = out[:, ch:]


def project(tok, gain, wx, channels, tile=256):
    rows, width = tok.shape
    cols = wx.shape[1]
    return pl.pallas_call(
        proj_kernel,
        grid=(rows // tile,),
        in_specs=[
            pl.BlockSpec((tile, width), lambda i: (i, 0)),
            pl.BlockSpec((1, width), lambda i: (0, 0)),
            pl.BlockSpec((width, cols), lambda i: (0, 0)),
        ],
        out_specs=[
            pl.BlockSpec((tile, width), lambda i: (i, 0)),
            pl.BlockSpec((tile, channels), lambda i: (i, 0)),
            pl.BlockSpec((tile, cols - channels), lambda i: (i, 0)),
        ],
        out_shape=[
            jax.ShapeDtypeStruct((rows, width), bf16),
            jax.ShapeDtypeStruct((rows, channels), f32),
            jax.ShapeDtypeStruct((rows, cols - channels), f32),
        ],
        compiler_params=params(60 << 20),
        name="project",
    )(tok, gain, wx)


def segment_rows(seg_ref, block, blocks, at):
    rows = seg_ref.shape[0]
    none = jnp.full((1, LANES), -1.0, f32)
    seg = seg_ref[pl.ds(at, 1), :]
    prev = jnp.where(block > 0, seg_ref[pl.ds(jnp.maximum(at - 1, 0), 1), :], none)
    after = jnp.where(block < blocks - 1, seg_ref[pl.ds(jnp.minimum(at + 1, rows - 1), 1), :], none)
    lane = lax.broadcasted_iota(jnp.int32, (1, LANES), 1)

    def same(other):
        return (other == seg).astype(f32)

    out = [seg]
    for k in (1, 2, 3):
        out.append(same(jnp.where(lane < k, pltpu.roll(prev, k, 1), pltpu.roll(seg, k, 1))))
    out.append(same(jnp.broadcast_to(prev[:, LANES - 1 :], (1, LANES))))
    out.append(same(jnp.broadcast_to(seg[:, LANES - 1 :], (1, LANES))))
    for k in (1, 2, 3):
        turn = LANES - k
        out.append(same(jnp.where(lane >= turn, pltpu.roll(after, turn, 1), pltpu.roll(seg, turn, 1))))
    tab = jnp.concatenate(out + [none] * (16 - len(out)), axis=0)
    return seg, jnp.concatenate([tab] * (LANES // 16), axis=0).T


def iota(shape, axis):
    return lax.broadcasted_iota(jnp.int32, shape, axis)


def ones_where(cond):
    return jnp.where(cond, 1.0, 0.0).astype(bf16)


def head_columns(heads_wide, inner, width):
    return ones_where(iota((heads_wide, inner), 0) % LANES == iota((heads_wide, inner), 1) // width)


def step_terms(dt, dtb, na2, tri, cols):
    raw = dt + dtb
    ts = jnp.maximum(raw, 0.0) + jnp.log1p(jnp.exp(-jnp.abs(raw)))
    cum = dot(jnp.concatenate([tri] * 3, axis=1), jnp.concatenate(split(ts * na2, 3), axis=0))
    start = jnp.exp2(cum) * wide(cols[:, 4:5], LANES)
    end = jnp.exp2(cum[Q - 1 : Q, :] - cum) * wide(cols[:, 5:6], LANES)
    return raw, ts, cum, start, end


def head_terms(head_ref):
    rate = head_ref[1:2, :]
    return head_ref[0:1, :], rate, rate * LOG2E


def fill_constants(e_ref, tri_ref, skip_ref, head_ref):
    inner = e_ref.shape[1]
    e_ref[...] = head_columns(e_ref.shape[0], inner, HEAD)
    tri_ref[...] = ones_where(iota((Q, Q), 0) >= iota((Q, Q), 1))
    skip = jnp.broadcast_to(head_ref[2:3, :], (8, LANES))
    wide_skip = dot(jnp.concatenate(split(skip, 3), axis=1), head_columns(3 * LANES, inner, HEAD))
    skip_ref[...] = wide_skip[0:1]


def expand_operand(*terms):
    return jnp.concatenate([jnp.concatenate(split(t, 2), axis=1) for t in terms], axis=0)


def by_head(v, left):
    zero = jnp.zeros_like(v)
    return jnp.concatenate([jnp.where(left, v, zero), jnp.where(left, zero, v)], axis=0)


def later_rows(v, k):
    width = v.shape[1]
    v = pltpu.roll(v.reshape(-1, 8, width), 8 - k, 1)
    here = lax.broadcasted_iota(jnp.int32, (1, 8, width), 1) < 8 - k
    return jnp.where(here, v[:-1], v[1:]).reshape(-1, width)


def fwd_kernel(
    seg_ref, xbc_ref, dt_ref, cw_ref, cb_ref, head_ref,
    y_ref, s_ref, sin_ref, state, ext, e_ref, tri_ref, skip_ref,
):
    inner = y_ref.shape[1]
    channels = cb_ref.shape[1]
    b, blocks = pl.program_id(1), pl.num_programs(1)
    dtb, _, na2 = head_terms(head_ref)

    @pl.when((b == 0) & (pl.program_id(0) == 0))
    def _():
        fill_constants(e_ref, tri_ref, skip_ref, head_ref)

    @pl.when(b == 0)
    def _():
        state[...] = jnp.zeros_like(state)
        ext[0:8, :] = jnp.zeros((8, channels), f32)

    @pl.when(b > 0)
    def _():
        ext[0:8, :] = ext[Q : Q + 8, :]

    ext[8 : 8 + Q, :] = xbc_ref[...]
    seg, cols = segment_rows(seg_ref, b, blocks, pl.program_id(0) * blocks + b)
    m1, m2, m3 = (wide(cols[:, k : k + 1], 256) for k in (1, 2, 3))

    def conv(c):
        at = pl.ds(c, 256)
        x = ext[:, at]
        s = cb_ref[:, at] + cw_ref[3:4, at] * x[8:]
        s += m1 * (cw_ref[2:3, at] * later_rows(x, 7))
        s += m2 * (cw_ref[1:2, at] * later_rows(x, 6))
        s += m3 * (cw_ref[0:1, at] * later_rows(x, 5))
        s_ref[:, at] = s
        return s * sigmoid(s)

    bc, bc_rest = split(conv(inner), 2)
    bm, cm = bc[:, :LANES], bc[:, LANES:]
    bt = bm.T
    c_two = jnp.concatenate([cm, bc_rest[:, LANES:]], axis=1)
    _, ts, cum, start, end = step_terms(dt_ref[...], dtb, na2, tri_ref[...], cols)
    cum_t = cum.T
    grow = expand_operand(start, end, ts)
    row_i = lax.broadcasted_iota(jnp.int32, (Q, Q), 0)
    col_j = lax.broadcasted_iota(jnp.int32, (Q, Q), 1)
    same = wide(cols[:, 0:1], LANES) == seg
    mask = jnp.where(same & (row_i >= col_j), 0.0, NEG)
    scores = dot_split((cm, bc_rest[:, LANES:]), (bm, bc_rest[:, :LANES]))
    left = col_j < HEAD

    for c in range(0, inner, 256):
        at = pl.ds(c, 256)
        x = conv(c)
        big = dot(grow, e_ref[:, at])
        s_e, e_e, t_e = big[:Q], big[Q : 2 * Q], big[2 * Q :]
        xs = x * t_e
        xs_low = xs.astype(bf16)
        st = state[:, at]
        st_low = st.astype(bf16)
        sin_ref[:, at] = st_low
        carried = dot(c_two, twice(st_low, 0))
        parts = []
        for p in range(2):
            mats = []
            for h in range(2):
                head = (c + p * LANES) // HEAD + h
                gap = wide(cum[:, head : head + 1], LANES) - cum_t[head : head + 1, :] + mask
                mats.append((jnp.exp2(gap) * scores).astype(bf16))
            xp = xs_low[:, p * LANES : (p + 1) * LANES]
            parts.append(dot(jnp.concatenate(mats, axis=1), by_head(xp, left)))
        y = jnp.concatenate(parts, axis=1) + s_e * carried + skip_ref[:, at] * x
        y_ref[:, at] = y
        state[:, at] = st * s_e[Q - 1 : Q, :] + dot(bt, (xs * e_e).astype(bf16))


def fixed(shape):
    return pl.BlockSpec(shape, lambda *_: (0,) * len(shape))


def state_forward(seg, xbc, dt, cw, cb, head, inner, seqs):
    rows, channels = xbc.shape
    blocks = rows // seqs // Q
    at = lambda s, b: (s * blocks + b, 0)
    at3 = lambda s, b: (s * blocks + b, 0, 0)
    return pl.pallas_call(
        fwd_kernel,
        grid=(seqs, blocks),
        in_specs=[
            fixed(seg.shape),
            pl.BlockSpec((Q, channels), at),
            pl.BlockSpec((Q, LANES), at),
            fixed(cw.shape), fixed(cb.shape), fixed(head.shape),
        ],
        out_specs=[
            pl.BlockSpec((Q, inner), at),
            pl.BlockSpec((Q, channels), at),
            pl.BlockSpec((None, LANES, inner), at3),
        ],
        out_shape=[
            jax.ShapeDtypeStruct((rows, inner), f32),
            jax.ShapeDtypeStruct((rows, channels), f32),
            jax.ShapeDtypeStruct((seqs * blocks, LANES, inner), bf16),
        ],
        scratch_shapes=[
            pltpu.VMEM((LANES, inner), f32),
            pltpu.VMEM((Q + 8, channels), f32),
            pltpu.VMEM((2 * LANES, inner), bf16),
            pltpu.VMEM((Q, Q), bf16),
            pltpu.VMEM((1, inner), f32),
        ],
        compiler_params=params(60 << 20),
        name="state_forward",
    )(seg, xbc, dt, cw, cb, head)


def flat(ref):
    v = ref[...]
    return v.reshape(v.shape[0] * v.shape[1], v.shape[2])


def slab_views(slab, own):
    owners, _, width = slab.shape
    if own % 16 == 0:
        first = lambda *_: (0, 0, 0)
        second = lambda *_: (0, 1, 0)
        sizes = ((own, first), (own, second), (2 * own, second))
        return [(slab, pl.BlockSpec((owners, n, width), index)) for n, index in sizes]
    parts = [
        v.reshape(1, -1, width) for v in (slab[:, :own], slab[:, own : 2 * own], slab[:, 2 * own :])
    ]
    return [(v, fixed(v.shape)) for v in parts]


def gate_kernel(
    tok_ref, normed_ref, y_ref, cot_ref, wa_ref, wb_ref, wo_ref, gain_ref,
    gn_ref, out_ref, gz_ref, gm_ref, ggain_ref,
):
    normed, wo = normed_ref[...], flat(wo_ref)
    z = jnp.concatenate([dot(normed, flat(wa_ref)), dot(normed, flat(wb_ref))], axis=1)
    sg = sigmoid(z)
    sz = z * sg
    y = y_ref[...]
    gated = y * sz
    rstd = lax.rsqrt(jnp.mean(gated * gated, axis=-1, keepdims=True) + EPS)
    unit = gated * rstd
    gn = (unit * gain_ref[...]).astype(bf16)
    gn_ref[...] = gn
    out_ref[...] = (tok_ref[...].astype(f32) + dot(gn, wo)).astype(bf16)
    g_gn = dot(cot_ref[...], wo, NT)

    @pl.when(pl.program_id(0) == 0)
    def _():
        ggain_ref[...] = jnp.zeros_like(ggain_ref)

    ggain_ref[...] += fold_rows(unit * g_gn)
    q = g_gn * gain_ref[...]
    mean = jnp.mean(unit * q, axis=-1, keepdims=True)
    g_gated = rstd * (q - unit * mean)
    gm_ref[...] = g_gated * sz
    gz_ref[...] = (g_gated * y * (sg * (1.0 + z * (1.0 - sg)))).astype(bf16)


def gate(tok, normed, y, cot, weights, gain, tile=256):
    rows, width = tok.shape
    inner = y.shape[1]
    at = lambda i: (i, 0)
    return pl.pallas_call(
        gate_kernel,
        grid=(rows // tile,),
        in_specs=[
            pl.BlockSpec((tile, width), at),
            pl.BlockSpec((tile, width), at),
            pl.BlockSpec((tile, inner), at),
            pl.BlockSpec((tile, width), at),
            *[spec for _, spec in weights], fixed(gain.shape),
        ],
        out_specs=[
            pl.BlockSpec((tile, inner), at),
            pl.BlockSpec((tile, width), at),
            pl.BlockSpec((tile, inner), at),
            pl.BlockSpec((tile, inner), at),
            fixed((8, inner)),
        ],
        out_shape=[
            jax.ShapeDtypeStruct((rows, inner), bf16),
            jax.ShapeDtypeStruct((rows, width), bf16),
            jax.ShapeDtypeStruct((rows, inner), bf16),
            jax.ShapeDtypeStruct((rows, inner), f32),
            jax.ShapeDtypeStruct((8, inner), f32),
        ],
        compiler_params=params(60 << 20),
        name="gate",
    )(tok, normed, y, cot, *[v for v, _ in weights], gain)


def bwd_kernel(
    seg_ref, xbc_ref, dt_ref, s_ref, sin_ref, gm_ref, cw_ref, head_ref,
    gx_ref, gcw_ref, gcb_ref, gskip_ref, galog_ref, gdtb_ref,
    adj, gext, da_rows, spread, grad_b, grad_c, link, e_ref, tri_ref, skip_ref, et_ref, tail_ref, pair_ref,
):
    inner = gm_ref.shape[1]
    channels = s_ref.shape[1]
    b, blocks = pl.program_id(1), pl.num_programs(1)
    dtb, rate, na2 = head_terms(head_ref)

    @pl.when((b == 0) & (pl.program_id(0) == 0))
    def _():
        for ref in (gcw_ref, gcb_ref, gskip_ref, galog_ref, gdtb_ref, da_rows):
            ref[...] = jnp.zeros_like(ref)
        fill_constants(e_ref, tri_ref, skip_ref, head_ref)
        et_ref[...] = ones_where(iota((inner, LANES), 0) // HEAD == iota((inner, LANES), 1))
        turned = ones_where(iota((Q, Q), 0) <= iota((Q, Q), 1))
        below = ones_where(iota((Q, Q), 0) > iota((Q, Q), 1))
        tail_ref[...] = jnp.concatenate([turned, turned, below, below], axis=1)
        row, col = iota((2 * Q, 2 * Q), 0), iota((2 * Q, 2 * Q), 1)
        pair_ref[...] = ones_where((row // Q == col // Q) & (row >= col))

    @pl.when(b == 0)
    def _():
        adj[...] = jnp.zeros_like(adj)
        gext[Q : Q + 8, :] = jnp.zeros((8, channels), f32)

    @pl.when(b > 0)
    def _():
        gext[Q : Q + 8, :] = gext[0:8, :]

    turn = blocks - 1 - b
    seg, cols = segment_rows(seg_ref, turn, blocks, pl.program_id(0) * blocks + turn)
    raw, ts, cum, start, end = step_terms(dt_ref[...], dtb, na2, tri_ref[...], cols)
    cum_t = cum.T
    grow = expand_operand(start, end, ts)

    def act(c):
        s = s_ref[:, pl.ds(c, 256)]
        sg = sigmoid(s)
        return s * sg, sg * (1.0 + s * (1.0 - sg))

    bc, slope_bc = act(inner)
    bc, bc_rest = split(bc, 2)
    bm, cm = bc[:, :LANES], bc[:, LANES:]
    ct = cm.T
    b_two = jnp.concatenate([bm, bc_rest[:, :LANES]], axis=1)
    c_two = jnp.concatenate([cm, bc_rest[:, LANES:]], axis=1)
    row_j = lax.broadcasted_iota(jnp.int32, (Q, Q), 0)
    col_i = lax.broadcasted_iota(jnp.int32, (Q, Q), 1)
    same = wide(cols[:, 0:1], LANES) == seg
    mask = jnp.where(same & (col_i >= row_j), 0.0, NEG)
    before = (row_j < col_i).astype(f32)
    scores = dot_split((bm, bc_rest[:, :LANES]), (cm, bc_rest[:, LANES:]))
    left = col_i < HEAD
    grad_scores = jnp.zeros((Q, Q), f32)

    for c in range(0, inner, 256):
        at = pl.ds(c, 256)
        x, slope = act(c)
        big = dot(grow, e_ref[:, at])
        s_e, e_e, t_e = big[:Q], big[Q : 2 * Q], big[2 * Q :]
        xs = x * t_e
        xs_low, xs_rest = split(xs, 2)
        gm = gm_ref[:, at]
        gm_low, gm_rest = split(gm, 2)
        ad = adj[:, at]
        ad_low, ad_rest = split(ad, 2)
        st_low = sin_ref[:, at]
        into = dot(b_two, twice(ad_low, 0)) + dot(bm, ad_rest)
        carried = dot(c_two, twice(st_low, 0))
        parts = []
        for p in range(2):
            lanes = slice(p * LANES, (p + 1) * LANES)
            diag, diag_rest = by_head(gm_low[:, lanes], left), by_head(gm_rest[:, lanes], left)
            gmat = dot_split((xs_low[:, lanes], xs_rest[:, lanes]), (diag, diag_rest))
            mats, links = [], []
            for h in range(2):
                head = (c + p * LANES) // HEAD + h
                gap = cum_t[head : head + 1, :] - wide(cum[:, head : head + 1], LANES) + mask
                decay = jnp.exp2(gap)
                mat = decay * scores
                grad = gmat[:, h * LANES : (h + 1) * LANES]
                grad_scores += decay * grad
                mats.append(split(mat, 2))
                links.append((mat * grad).astype(bf16))
            high = jnp.concatenate([mats[0][0], mats[1][0]], axis=1)
            rest = jnp.concatenate([mats[0][1], mats[1][1]], axis=1)
            parts.append(dot(high, diag) + dot(high, diag_rest) + dot(rest, diag))
            reach = dot(jnp.concatenate(links, axis=1), pair_ref[...])
            for h in range(2):
                head = (c + p * LANES) // HEAD + h
                da_rows[head : head + 1, :] = jnp.sum(
                    reach[:, h * LANES : (h + 1) * LANES] * before, axis=0, keepdims=True
                )
        g_xs = jnp.concatenate(parts, axis=1) + e_e * into
        gext[0:Q, at] = (t_e * g_xs + skip_ref[:, at] * gm) * slope
        sums = jnp.concatenate(
            [pair_split(carried * gm), pair_split(x * into), pair_split(x * g_xs)], axis=0
        )
        sums = dot(sums, twice(et_ref[at, :], 0))
        s_gm = (s_e * gm).astype(bf16)
        part_c = dot(s_gm, st_low, NT)
        part_b = dot((e_e * xs).astype(bf16), ad_low, NT)
        if c == 0:
            spread[...] = sums
            grad_c[...] = part_c
            grad_b[...] = part_b
        else:
            spread[...] += sums
            grad_c[...] += part_c
            grad_b[...] += part_b
        gskip_ref[:, at] += fold_rows(gm * x)
        link[:, at] = fold_rows(st_low.astype(f32) * ad)
        adj[:, at] = ad * s_e[Q - 1 : Q, :] + dot(ct, s_gm)

    grad_low = grad_scores.astype(bf16)
    g_b = grad_b[...] + dot(grad_low, cm)
    g_c = grad_c[...] + dot(grad_low, bm, TN)
    gext[0:Q, pl.ds(inner, 256)] = jnp.concatenate([g_b, g_c], axis=1) * slope_bc

    phi = start * spread[0:Q]
    psi = end * ts * spread[Q : 2 * Q]
    through = jnp.sum(dot(jnp.concatenate(split(link[...], 2), axis=0), et_ref[...]), axis=0, keepdims=True)
    around = jnp.concatenate(split(phi, 2) + split(psi, 2), axis=0)
    da = da_rows[...].T + dot(tail_ref[...], around) + start[Q - 1 : Q, :] * through
    g_ts = spread[2 * Q :] + rate * da
    galog_ref[...] += fold_rows(ts * rate * da)
    g_dt = g_ts * sigmoid(raw)
    gdtb_ref[...] += fold_rows(g_dt)

    n1, n2, n3 = (wide(cols[:, k : k + 1], 256) for k in (6, 7, 8))
    for c in range(0, channels, 256):
        at = pl.ds(c, 256)
        x = xbc_ref[:, at]
        g = gext[:, at]
        g0 = g[:Q]
        g1 = later_rows(g, 1) * n1
        g2 = later_rows(g, 2) * n2
        g3 = later_rows(g, 3) * n3
        gx = cw_ref[3:4, at] * g0 + cw_ref[2:3, at] * g1 + cw_ref[1:2, at] * g2 + cw_ref[0:1, at] * g3
        gx_ref[:, at] = gx.astype(bf16)
        gcb_ref[:, at] += fold_rows(g0)
        gcw_ref[24:32, at] += fold_rows(g0 * x)
        gcw_ref[16:24, at] += fold_rows(g1 * x)
        gcw_ref[8:16, at] += fold_rows(g2 * x)
        gcw_ref[0:8, at] += fold_rows(g3 * x)
    gx_ref[:, channels:] = g_dt.astype(bf16)


def state_backward(seg, xbc, dt, s, sin, gm, cw, head, seqs):
    rows, channels = xbc.shape
    inner = gm.shape[1]
    blocks = rows // seqs // Q
    at = lambda s, b: (s * blocks + blocks - 1 - b, 0)
    at3 = lambda s, b: (s * blocks + blocks - 1 - b, 0, 0)
    return pl.pallas_call(
        bwd_kernel,
        grid=(seqs, blocks),
        in_specs=[
            fixed(seg.shape),
            pl.BlockSpec((Q, channels), at),
            pl.BlockSpec((Q, LANES), at),
            pl.BlockSpec((Q, channels), at),
            pl.BlockSpec((None, LANES, inner), at3),
            pl.BlockSpec((Q, inner), at),
        ]
        + [fixed(v.shape) for v in (cw, head)],
        out_specs=[
            pl.BlockSpec((Q, channels + LANES), at),
            fixed((32, channels)), fixed((8, channels)), fixed((8, inner)), fixed((8, LANES)), fixed((8, LANES)),
        ],
        out_shape=[
            jax.ShapeDtypeStruct((rows, channels + LANES), bf16),
            jax.ShapeDtypeStruct((32, channels), f32),
            jax.ShapeDtypeStruct((8, channels), f32),
            jax.ShapeDtypeStruct((8, inner), f32),
            jax.ShapeDtypeStruct((8, LANES), f32),
            jax.ShapeDtypeStruct((8, LANES), f32),
        ],
        scratch_shapes=[
            pltpu.VMEM((LANES, inner), f32),
            pltpu.VMEM((Q + 8, channels), f32),
            pltpu.VMEM((LANES, LANES), f32),
            pltpu.VMEM((3 * Q, LANES), f32),
            pltpu.VMEM((Q, LANES), f32),
            pltpu.VMEM((Q, LANES), f32),
            pltpu.VMEM((8, inner), f32),
            pltpu.VMEM((2 * LANES, inner), bf16),
            pltpu.VMEM((Q, Q), bf16),
            pltpu.VMEM((1, inner), f32),
            pltpu.VMEM((inner, LANES), bf16),
            pltpu.VMEM((Q, 4 * Q), bf16),
            pltpu.VMEM((2 * Q, 2 * Q), bf16),
        ],
        compiler_params=params(60 << 20),
        name="state_backward",
    )(seg, xbc, dt, s, sin, gm, cw, head)


def token_kernel(tok_ref, cot_ref, gz_ref, gx_ref, wa_ref, wb_ref, wx_ref, gain_ref, out_ref, ggain_ref):
    half = gz_ref.shape[1] // 2
    g = dot(gz_ref[:, :half], flat(wa_ref), NT) + dot(gz_ref[:, half:], flat(wb_ref), NT)
    g += dot(gx_ref[...], wx_ref[...], NT)
    u = tok_ref[...].astype(f32)
    r = lax.rsqrt(jnp.mean(u * u, axis=-1, keepdims=True) + EPS)
    unit = u * r

    @pl.when(pl.program_id(0) == 0)
    def _():
        ggain_ref[...] = jnp.zeros_like(ggain_ref)

    ggain_ref[...] += fold_rows(unit * g)
    q = g * gain_ref[...]
    mean = jnp.mean(unit * q, axis=-1, keepdims=True)
    out_ref[...] = (cot_ref[...].astype(f32) + r * (q - unit * mean)).astype(bf16)


def token_grad(tok, cot, gz, gx, weights, wx, gain, tile=256):
    rows, width = tok.shape
    at = lambda i: (i, 0)
    return pl.pallas_call(
        token_kernel,
        grid=(rows // tile,),
        in_specs=[
            pl.BlockSpec((tile, width), at),
            pl.BlockSpec((tile, width), at),
            pl.BlockSpec((tile, gz.shape[1]), at),
            pl.BlockSpec((tile, gx.shape[1]), at),
            *[spec for _, spec in weights], fixed(wx.shape), fixed(gain.shape),
        ],
        out_specs=[pl.BlockSpec((tile, width), at), fixed((8, width))],
        out_shape=[jax.ShapeDtypeStruct((rows, width), bf16), jax.ShapeDtypeStruct((8, width), f32)],
        compiler_params=params(60 << 20),
        name="token_grad",
    )(tok, cot, gz, gx, *[v for v, _ in weights], wx, gain)


def partner(axis, bit):
    me = lax.axis_index(axis)
    return {axis: me + bit - 2 * bit * ((me // bit) % 2)}


def finish_kernel(
    steps, heads, cw_ref, cb_ref, ggain_ref, skip_ref, ngain_ref, alog_ref, dtb_ref, zo_ref, x_ref,
    small_ref, din_ref, dout_ref, acc, got, zo_got, x_got, send, recv, big_send, big_recv,
):
    if steps:
        barrier = pltpu.get_barrier_semaphore()
    for axis, bit in steps:
        pl.semaphore_signal(barrier, inc=1, device_id=partner(axis, bit), device_id_type=pl.DeviceIdType.MESH)
    if steps:
        pl.semaphore_wait(barrier, len(steps))

    def exchange(src, dst, ssem, rsem, axis, bit):
        copy = pltpu.make_async_remote_copy(
            src_ref=src, dst_ref=dst, send_sem=ssem, recv_sem=rsem,
            device_id=partner(axis, bit), device_id_type=pl.DeviceIdType.MESH,
        )
        copy.start()
        return copy

    big = []
    for axis, bit in steps[-1:]:
        big.append(exchange(zo_ref, zo_got, big_send.at[0], big_recv.at[0], axis, bit))
        big.append(exchange(x_ref, x_got, big_send.at[1], big_recv.at[1], axis, bit))

    inner, width = ggain_ref.shape[1], ngain_ref.shape[1]
    channels = cb_ref.shape[1]
    total = lambda v: jnp.sum(v, axis=0, keepdims=True)
    acc[0] = jnp.zeros((8, channels), f32)
    for k in range(4):
        acc[0, k : k + 1, :] = total(cw_ref[8 * k : 8 * k + 8, :])
    acc[0, 4:5, :] = total(cb_ref[...])
    acc[0, 5:6, :inner] = total(ggain_ref[...])
    acc[0, 6:7, :width] = total(ngain_ref[...])
    acc[0, 6:7, width : width + LANES] = total(alog_ref[...])
    acc[0, 6:7, width + LANES : width + 2 * LANES] = total(dtb_ref[...])
    skip = jnp.concatenate(split(skip_ref[...], 3), axis=0)
    by_head = ones_where(iota((inner, LANES), 0) // HEAD == iota((inner, LANES), 1))
    acc[0, 6:7, width + 2 * LANES : width + 3 * LANES] = total(dot(skip, by_head))

    for k, (axis, bit) in enumerate(steps):
        exchange(acc.at[k], got.at[k], send.at[k], recv.at[k], axis, bit).wait()
        acc[k + 1] = acc[k] + got[k]
    small_ref[...] = acc[len(steps)]

    for copy in big:
        copy.wait()
    own = din_ref.shape[0]
    zo = zo_ref[...].astype(f32) + zo_got[...].astype(f32)
    half = zo.shape[1]
    din_ref[:, :half] = zo[:own]
    din_ref[:, half : 2 * half] = zo[own : 2 * own]
    dout_ref[...] = zo[2 * own :]
    left = din_ref.shape[1] - 2 * half
    din_ref[:, 2 * half :] = (x_ref[...].astype(f32) + x_got[...].astype(f32))[:, :left]


def finish(p_cw, p_cb, p_ggain, p_skip, p_ngain, p_alog, p_dtb, d_zo, d_x, sizes, heads, proj):
    steps = [(axis, 1 << i) for axis, n in sizes for i in range(n.bit_length() - 1)]
    own, half = d_x.shape[0], d_zo.shape[1]
    channels = p_cb.shape[1]
    vmem = pl.BlockSpec(memory_space=pltpu.VMEM)
    return pl.pallas_call(
        functools.partial(finish_kernel, steps, heads),
        in_specs=[vmem] * 9,
        out_specs=[vmem] * 3,
        out_shape=[
            jax.ShapeDtypeStruct((8, channels), f32),
            jax.ShapeDtypeStruct((own, proj), f32),
            jax.ShapeDtypeStruct((2 * own, half), f32),
        ],
        scratch_shapes=[
            pltpu.VMEM((len(steps) + 1, 8, channels), f32),
            pltpu.VMEM((max(len(steps), 1), 8, channels), f32),
            pltpu.VMEM(d_zo.shape, bf16),
            pltpu.VMEM(d_x.shape, bf16),
            pltpu.SemaphoreType.DMA((max(len(steps), 1),)),
            pltpu.SemaphoreType.DMA((max(len(steps), 1),)),
            pltpu.SemaphoreType.DMA((2,)),
            pltpu.SemaphoreType.DMA((2,)),
        ],
        compiler_params=params(48 << 20, collective_id=0 if steps else None, has_side_effects=True),
        name="finish",
    )(p_cw, p_cb, p_ggain, p_skip, p_ngain, p_alog, p_dtb, d_zo, d_x)


def per_device(
    sizes, tokens, segments, cotangent, norm_gain, weight_in, conv_weight, conv_bias, dt_bias, a_log, skip_d,
    gate_gain, weight_out,
):
    seqs, length, width = tokens.shape
    rows = seqs * length
    inner = gate_gain.shape[0]
    channels = conv_bias.shape[0]
    heads = dt_bias.shape[0]
    own = weight_in.shape[0]
    owners = width // own
    tok = tokens.reshape(rows, width)
    cot = cotangent.reshape(rows, width)
    pad = LANES - heads

    local_x = jnp.pad(weight_in[:, inner:], ((0, 0), (0, pad)))
    wx = lax.all_gather(local_x, "dp", axis=0, tiled=True)
    local_zo = jnp.concatenate([weight_in[:, :width], weight_in[:, width:inner], weight_out], axis=0)
    slab = lax.all_gather(local_zo, "dp", axis=0, tiled=True).reshape(owners, 4 * own, width)
    weights = slab_views(slab, own)

    head = jnp.pad(jnp.stack([dt_bias, -jnp.exp(a_log), skip_d]), ((0, 5), (0, pad)))
    seg = segments.astype(f32).reshape(rows // Q, Q)
    cb = conv_bias.reshape(1, channels)
    ngain = norm_gain.reshape(1, width)
    ggain = gate_gain.reshape(1, inner)

    normed, xbc, dt = project(tok, ngain, wx, channels)
    y, s, sin = state_forward(seg, xbc, dt, conv_weight, cb, head, inner, seqs)
    gn, out, gz, gm, p_ggain = gate(tok, normed, y, cot, weights, ggain)
    d_z = dot(normed, gz, TN).astype(bf16)
    d_out = dot(gn, cot, TN).astype(bf16)
    d_zo = jnp.concatenate(
        [
            d_z[:, :width].reshape(owners, own, width),
            d_z[:, width:].reshape(owners, own, width),
            d_out.reshape(owners, 2 * own, width),
        ],
        axis=1,
    ).reshape(owners * 4 * own, width)
    d_zo, gm = lax.optimization_barrier((d_zo, gm))
    d_zo = lax.psum_scatter(d_zo, "dp", scatter_dimension=0, tiled=True)
    gx, p_cw, p_cb, p_skip, p_alog, p_dtb = state_backward(seg, xbc, dt, s, sin, gm, conv_weight, head, seqs)
    d_x = dot(normed, gx, TN).astype(bf16)
    d_x = lax.psum_scatter(d_x, "dp", scatter_dimension=0, tiled=True)
    g_tok, p_ngain = token_grad(tok, cot, gz, gx, weights[:2], wx, ngain)
    small, d_in, d_out = finish(
        p_cw, p_cb, p_ggain, p_skip, p_ngain, p_alog, p_dtb, d_zo, d_x, sizes, heads, weight_in.shape[1]
    )
    return (
        out.reshape(tokens.shape),
        g_tok.reshape(tokens.shape),
        small[6, :width],
        d_in,
        small[:4],
        small[4],
        small[6, width + LANES : width + LANES + heads],
        small[6, width : width + heads],
        small[6, width + 2 * LANES : width + 2 * LANES + heads],
        small[5, :inner],
        d_out,
    )


def solution(mesh):
    data = P(("dp", "seq"), None, None)
    owned = P("dp", None)
    placed = (data, P(("dp", "seq"), None), data, P(), owned, P(), P(), P(), P(), P(), P(), owned)
    return jax.shard_map(
        functools.partial(per_device, [(axis, mesh.shape[axis]) for axis in ("dp", "seq")]),
        mesh=mesh,
        in_specs=placed,
        out_specs=(data, data, P(), owned, P(), P(), P(), P(), P(), P(), owned),
        check_vma=False,
    )
```

```python
import functools
import math

import jax
import jax.numpy as jnp
from jax import lax
from jax.experimental import pallas as pl
from jax.experimental.pallas import tpu as pltpu
from jax.sharding import PartitionSpec as P

f32 = jnp.float32
bf16 = jnp.bfloat16
HEAD = 64
Q = 128
LANES = 128
EPS = 1e-05
LOG2E = math.log2(math.e)
NEG = -1e30

NN = (((1,), (0,)), ((), ()))
NT = (((1,), (1,)), ((), ()))
TN = (((0,), (0,)), ((), ()))


def dot(a, b, dims=NN):
    return lax.dot_general(a, b, dims, preferred_element_type=f32)


def pair_split(v):
    return jnp.concatenate(split(v, 2), axis=1)


def twice(v, axis):
    return jnp.concatenate([v, v], axis=axis)


def dot_split(a, b):
    low = b[1]
    return dot(jnp.concatenate(a, axis=1), twice(b[0], 1), NT) + dot(a[0], low, NT)


def sigmoid(v):
    return 0.5 + 0.5 * jnp.tanh(0.5 * v)


def split(v, parts):
    out = []
    for _ in range(parts):
        low = v.astype(bf16)
        out.append(low)
        v = v - low.astype(f32)
    return out


def fold_rows(v):
    return jnp.sum(v.reshape(v.shape[0] // 8, 8, v.shape[1]), axis=0)


def wide(v, width):
    col = jnp.broadcast_to(v, (v.shape[0], LANES))
    return jnp.concatenate([col] * (width // LANES), axis=1)


def params(limit=None, **more):
    return pltpu.CompilerParams(vmem_limit_bytes=limit, **more)


def proj_kernel(tok_ref, gain_ref, wx_ref, normed_ref, xbc_ref, dt_ref):
    u = tok_ref[...].astype(f32)
    r = lax.rsqrt(jnp.mean(u * u, axis=-1, keepdims=True) + EPS)
    normed = (u * r * gain_ref[...]).astype(bf16)
    normed_ref[...] = normed
    out = dot(normed, wx_ref[...])
    ch = xbc_ref.shape[1]
    xbc_ref[...] = out[:, :ch]
    dt_ref[...] = out[:, ch:]


def project(tok, gain, wx, channels, tile=256):
    rows, width = tok.shape
    cols = wx.shape[1]
    return pl.pallas_call(
        proj_kernel,
        grid=(rows // tile,),
        in_specs=[
            pl.BlockSpec((tile, width), lambda i: (i, 0)),
            pl.BlockSpec((1, width), lambda i: (0, 0)),
            pl.BlockSpec((width, cols), lambda i: (0, 0)),
        ],
        out_specs=[
            pl.BlockSpec((tile, width), lambda i: (i, 0)),
            pl.BlockSpec((tile, channels), lambda i: (i, 0)),
            pl.BlockSpec((tile, cols - channels), lambda i: (i, 0)),
        ],
        out_shape=[
            jax.ShapeDtypeStruct((rows, width), bf16),
            jax.ShapeDtypeStruct((rows, channels), f32),
            jax.ShapeDtypeStruct((rows, cols - channels), f32),
        ],
        compiler_params=params(60 << 20),
        name="project",
    )(tok, gain, wx)


def segment_rows(seg_ref, block, blocks, at):
    rows = seg_ref.shape[0]
    none = jnp.full((1, LANES), -1.0, f32)
    seg = seg_ref[pl.ds(at, 1), :]
    prev = jnp.where(block > 0, seg_ref[pl.ds(jnp.maximum(at - 1, 0), 1), :], none)
    after = jnp.where(block < blocks - 1, seg_ref[pl.ds(jnp.minimum(at + 1, rows - 1), 1), :], none)
    lane = lax.broadcasted_iota(jnp.int32, (1, LANES), 1)

    def same(other):
        return (other == seg).astype(f32)

    out = [seg]
    for k in (1, 2, 3):
        out.append(same(jnp.where(lane < k, pltpu.roll(prev, k, 1), pltpu.roll(seg, k, 1))))
    out.append(same(jnp.broadcast_to(prev[:, LANES - 1 :], (1, LANES))))
    out.append(same(jnp.broadcast_to(seg[:, LANES - 1 :], (1, LANES))))
    for k in (1, 2, 3):
        turn = LANES - k
        out.append(same(jnp.where(lane >= turn, pltpu.roll(after, turn, 1), pltpu.roll(seg, turn, 1))))
    tab = jnp.concatenate(out + [none] * (16 - len(out)), axis=0)
    return seg, jnp.concatenate([tab] * (LANES // 16), axis=0).T


def iota(shape, axis):
    return lax.broadcasted_iota(jnp.int32, shape, axis)


def ones_where(cond):
    return jnp.where(cond, 1.0, 0.0).astype(bf16)


def head_columns(heads_wide, inner, width):
    return ones_where(iota((heads_wide, inner), 0) % LANES == iota((heads_wide, inner), 1) // width)


def step_terms(dt, dtb, na2, tri, cols):
    raw = dt + dtb
    ts = jnp.maximum(raw, 0.0) + jnp.log1p(jnp.exp(-jnp.abs(raw)))
    cum = dot(jnp.concatenate([tri] * 3, axis=1), jnp.concatenate(split(ts * na2, 3), axis=0))
    start = jnp.exp2(cum) * wide(cols[:, 4:5], LANES)
    end = jnp.exp2(cum[Q - 1 : Q, :] - cum) * wide(cols[:, 5:6], LANES)
    return raw, ts, cum, start, end


def head_terms(head_ref):
    rate = head_ref[1:2, :]
    return head_ref[0:1, :], rate, rate * LOG2E


def fill_constants(e_ref, tri_ref, skip_ref, head_ref):
    inner = e_ref.shape[1]
    e_ref[...] = head_columns(e_ref.shape[0], inner, HEAD)
    tri_ref[...] = ones_where(iota((Q, Q), 0) >= iota((Q, Q), 1))
    skip = jnp.broadcast_to(head_ref[2:3, :], (8, LANES))
    wide_skip = dot(jnp.concatenate(split(skip, 3), axis=1), head_columns(3 * LANES, inner, HEAD))
    skip_ref[...] = wide_skip[0:1]


def expand_operand(*terms):
    return jnp.concatenate([jnp.concatenate(split(t, 2), axis=1) for t in terms], axis=0)


def by_head(v, left):
    zero = jnp.zeros_like(v)
    return jnp.concatenate([jnp.where(left, v, zero), jnp.where(left, zero, v)], axis=0)


def later_rows(v, k):
    width = v.shape[1]
    v = pltpu.roll(v.reshape(-1, 8, width), 8 - k, 1)
    here = lax.broadcasted_iota(jnp.int32, (1, 8, width), 1) < 8 - k
    return jnp.where(here, v[:-1], v[1:]).reshape(-1, width)


def fwd_kernel(
    seg_ref, xbc_ref, dt_ref, cw_ref, cb_ref, head_ref,
    y_ref, s_ref, sin_ref, state, ext, e_ref, tri_ref, skip_ref,
):
    inner = y_ref.shape[1]
    channels = cb_ref.shape[1]
    b, blocks = pl.program_id(1), pl.num_programs(1)
    dtb, _, na2 = head_terms(head_ref)

    @pl.when((b == 0) & (pl.program_id(0) == 0))
    def _():
        fill_constants(e_ref, tri_ref, skip_ref, head_ref)

    @pl.when(b == 0)
    def _():
        state[...] = jnp.zeros_like(state)
        ext[0:8, :] = jnp.zeros((8, channels), f32)

    @pl.when(b > 0)
    def _():
        ext[0:8, :] = ext[Q : Q + 8, :]

    ext[8 : 8 + Q, :] = xbc_ref[...]
    seg, cols = segment_rows(seg_ref, b, blocks, pl.program_id(0) * blocks + b)
    m1, m2, m3 = (wide(cols[:, k : k + 1], 256) for k in (1, 2, 3))

    def conv(c):
        at = pl.ds(c, 256)
        x = ext[:, at]
        s = cb_ref[:, at] + cw_ref[3:4, at] * x[8:]
        s += m1 * (cw_ref[2:3, at] * later_rows(x, 7))
        s += m2 * (cw_ref[1:2, at] * later_rows(x, 6))
        s += m3 * (cw_ref[0:1, at] * later_rows(x, 5))
        s_ref[:, at] = s
        return s * sigmoid(s)

    bc, bc_rest = split(conv(inner), 2)
    bm, cm = bc[:, :LANES], bc[:, LANES:]
    bt = bm.T
    c_two = jnp.concatenate([cm, bc_rest[:, LANES:]], axis=1)
    _, ts, cum, start, end = step_terms(dt_ref[...], dtb, na2, tri_ref[...], cols)
    cum_t = cum.T
    grow = expand_operand(start, end, ts)
    row_i = lax.broadcasted_iota(jnp.int32, (Q, Q), 0)
    col_j = lax.broadcasted_iota(jnp.int32, (Q, Q), 1)
    same = wide(cols[:, 0:1], LANES) == seg
    mask = jnp.where(same & (row_i >= col_j), 0.0, NEG)
    scores = dot_split((cm, bc_rest[:, LANES:]), (bm, bc_rest[:, :LANES]))
    left = col_j < HEAD

    for c in range(0, inner, 256):
        at = pl.ds(c, 256)
        x = conv(c)
        big = dot(grow, e_ref[:, at])
        s_e, e_e, t_e = big[:Q], big[Q : 2 * Q], big[2 * Q :]
        xs = x * t_e
        xs_low = xs.astype(bf16)
        st = state[:, at]
        st_low = st.astype(bf16)
        sin_ref[:, at] = st_low
        carried = dot(c_two, twice(st_low, 0))
        parts = []
        for p in range(2):
            mats = []
            for h in range(2):
                head = (c + p * LANES) // HEAD + h
                gap = wide(cum[:, head : head + 1], LANES) - cum_t[head : head + 1, :] + mask
                mats.append((jnp.exp2(gap) * scores).astype(bf16))
            xp = xs_low[:, p * LANES : (p + 1) * LANES]
            parts.append(dot(jnp.concatenate(mats, axis=1), by_head(xp, left)))
        y = jnp.concatenate(parts, axis=1) + s_e * carried + skip_ref[:, at] * x
        y_ref[:, at] = y
        state[:, at] = st * s_e[Q - 1 : Q, :] + dot(bt, (xs * e_e).astype(bf16))


def fixed(shape):
    return pl.BlockSpec(shape, lambda *_: (0,) * len(shape))


def state_forward(seg, xbc, dt, cw, cb, head, inner, seqs):
    rows, channels = xbc.shape
    blocks = rows // seqs // Q
    at = lambda s, b: (s * blocks + b, 0)
    at3 = lambda s, b: (s * blocks + b, 0, 0)
    return pl.pallas_call(
        fwd_kernel,
        grid=(seqs, blocks),
        in_specs=[
            fixed(seg.shape),
            pl.BlockSpec((Q, channels), at),
            pl.BlockSpec((Q, LANES), at),
            fixed(cw.shape), fixed(cb.shape), fixed(head.shape),
        ],
        out_specs=[
            pl.BlockSpec((Q, inner), at),
            pl.BlockSpec((Q, channels), at),
            pl.BlockSpec((None, LANES, inner), at3),
        ],
        out_shape=[
            jax.ShapeDtypeStruct((rows, inner), f32),
            jax.ShapeDtypeStruct((rows, channels), f32),
            jax.ShapeDtypeStruct((seqs * blocks, LANES, inner), bf16),
        ],
        scratch_shapes=[
            pltpu.VMEM((LANES, inner), f32),
            pltpu.VMEM((Q + 8, channels), f32),
            pltpu.VMEM((2 * LANES, inner), bf16),
            pltpu.VMEM((Q, Q), bf16),
            pltpu.VMEM((1, inner), f32),
        ],
        compiler_params=params(60 << 20),
        name="state_forward",
    )(seg, xbc, dt, cw, cb, head)


def flat(ref):
    v = ref[...]
    return v.reshape(v.shape[0] * v.shape[1], v.shape[2])


def slab_views(slab, own):
    owners, _, width = slab.shape
    if own % 16 == 0:
        first = lambda *_: (0, 0, 0)
        second = lambda *_: (0, 1, 0)
        sizes = ((own, first), (own, second), (2 * own, second))
        return [(slab, pl.BlockSpec((owners, n, width), index)) for n, index in sizes]
    parts = [
        v.reshape(1, -1, width) for v in (slab[:, :own], slab[:, own : 2 * own], slab[:, 2 * own :])
    ]
    return [(v, fixed(v.shape)) for v in parts]


def gate_kernel(
    tok_ref, normed_ref, y_ref, cot_ref, wa_ref, wb_ref, wo_ref, gain_ref,
    gn_ref, out_ref, gz_ref, gm_ref, ggain_ref,
):
    wa, wb, wo = flat(wa_ref), flat(wb_ref), flat(wo_ref)
    gain = gain_ref[...]

    @pl.when(pl.program_id(0) == 0)
    def _():
        ggain_ref[...] = jnp.zeros_like(ggain_ref)

    normed = normed_ref[...]
    z = jnp.concatenate([dot(normed, wa), dot(normed, wb)], axis=1)
    g_gn = dot(cot_ref[...], wo, NT)
    sg = sigmoid(z)
    sz = z * sg
    y = y_ref[...]
    gated = y * sz
    rstd = lax.rsqrt(jnp.mean(gated * gated, axis=-1, keepdims=True) + EPS)
    unit = gated * rstd
    gn = (unit * gain).astype(bf16)
    gn_ref[...] = gn
    out_ref[...] = (tok_ref[...].astype(f32) + dot(gn, wo)).astype(bf16)
    ggain_ref[...] += fold_rows(unit * g_gn)
    q = g_gn * gain
    mean = jnp.mean(unit * q, axis=-1, keepdims=True)
    g_gated = rstd * (q - unit * mean)
    gm_ref[...] = g_gated * sz
    gz_ref[...] = (g_gated * y * (sg * (1.0 + z * (1.0 - sg)))).astype(bf16)


def gate(tok, normed, y, cot, weights, gain, tile=256):
    rows, width = tok.shape
    inner = y.shape[1]
    at = lambda i: (i, 0)
    return pl.pallas_call(
        gate_kernel,
        grid=(rows // tile,),
        in_specs=[
            pl.BlockSpec((tile, width), at),
            pl.BlockSpec((tile, width), at),
            pl.BlockSpec((tile, inner), at),
            pl.BlockSpec((tile, width), at),
            *[spec for _, spec in weights], fixed(gain.shape),
        ],
        out_specs=[
            pl.BlockSpec((tile, inner), at),
            pl.BlockSpec((tile, width), at),
            pl.BlockSpec((tile, inner), at),
            pl.BlockSpec((tile, inner), at),
            fixed((8, inner)),
        ],
        out_shape=[
            jax.ShapeDtypeStruct((rows, inner), bf16),
            jax.ShapeDtypeStruct((rows, width), bf16),
            jax.ShapeDtypeStruct((rows, inner), bf16),
            jax.ShapeDtypeStruct((rows, inner), f32),
            jax.ShapeDtypeStruct((8, inner), f32),
        ],
        compiler_params=params(60 << 20),
        name="gate",
    )(tok, normed, y, cot, *[v for v, _ in weights], gain)


def bwd_kernel(
    seg_ref, xbc_ref, dt_ref, s_ref, sin_ref, gm_ref, cw_ref, head_ref,
    gx_ref, gcw_ref, gcb_ref, gskip_ref, galog_ref, gdtb_ref,
    adj, gext, da_rows, spread, grad_b, grad_c, link, e_ref, tri_ref, skip_ref, et_ref, tail_ref, pair_ref,
):
    inner = gm_ref.shape[1]
    channels = s_ref.shape[1]
    b, blocks = pl.program_id(1), pl.num_programs(1)
    dtb, rate, na2 = head_terms(head_ref)

    @pl.when((b == 0) & (pl.program_id(0) == 0))
    def _():
        for ref in (gcw_ref, gcb_ref, gskip_ref, galog_ref, gdtb_ref, da_rows):
            ref[...] = jnp.zeros_like(ref)
        fill_constants(e_ref, tri_ref, skip_ref, head_ref)
        et_ref[...] = ones_where(iota((inner, LANES), 0) // HEAD == iota((inner, LANES), 1))
        turned = ones_where(iota((Q, Q), 0) <= iota((Q, Q), 1))
        below = ones_where(iota((Q, Q), 0) > iota((Q, Q), 1))
        tail_ref[...] = jnp.concatenate([turned, turned, below, below], axis=1)
        row, col = iota((2 * Q, 2 * Q), 0), iota((2 * Q, 2 * Q), 1)
        pair_ref[...] = ones_where((row // Q == col // Q) & (row >= col))

    @pl.when(b == 0)
    def _():
        adj[...] = jnp.zeros_like(adj)
        gext[Q : Q + 8, :] = jnp.zeros((8, channels), f32)

    @pl.when(b > 0)
    def _():
        gext[Q : Q + 8, :] = gext[0:8, :]

    turn = blocks - 1 - b
    seg, cols = segment_rows(seg_ref, turn, blocks, pl.program_id(0) * blocks + turn)
    raw, ts, cum, start, end = step_terms(dt_ref[...], dtb, na2, tri_ref[...], cols)
    cum_t = cum.T
    grow = expand_operand(start, end, ts)

    def act(c):
        s = s_ref[:, pl.ds(c, 256)]
        sg = sigmoid(s)
        return s * sg, sg * (1.0 + s * (1.0 - sg))

    bc, slope_bc = act(inner)
    bc, bc_rest = split(bc, 2)
    bm, cm = bc[:, :LANES], bc[:, LANES:]
    ct = cm.T
    b_two = jnp.concatenate([bm, bc_rest[:, :LANES]], axis=1)
    c_two = jnp.concatenate([cm, bc_rest[:, LANES:]], axis=1)
    row_j = lax.broadcasted_iota(jnp.int32, (Q, Q), 0)
    col_i = lax.broadcasted_iota(jnp.int32, (Q, Q), 1)
    same = wide(cols[:, 0:1], LANES) == seg
    mask = jnp.where(same & (col_i >= row_j), 0.0, NEG)
    before = (row_j < col_i).astype(f32)
    scores = dot_split((bm, bc_rest[:, :LANES]), (cm, bc_rest[:, LANES:]))
    left = col_i < HEAD
    grad_scores = jnp.zeros((Q, Q), f32)

    for c in range(0, inner, 256):
        at = pl.ds(c, 256)
        x, slope = act(c)
        big = dot(grow, e_ref[:, at])
        s_e, e_e, t_e = big[:Q], big[Q : 2 * Q], big[2 * Q :]
        xs = x * t_e
        xs_low, xs_rest = split(xs, 2)
        gm = gm_ref[:, at]
        gm_low, gm_rest = split(gm, 2)
        ad = adj[:, at]
        ad_low, ad_rest = split(ad, 2)
        st_low = sin_ref[:, at]
        into = dot(b_two, twice(ad_low, 0)) + dot(bm, ad_rest)
        carried = dot(c_two, twice(st_low, 0))
        parts = []
        for p in range(2):
            lanes = slice(p * LANES, (p + 1) * LANES)
            diag, diag_rest = by_head(gm_low[:, lanes], left), by_head(gm_rest[:, lanes], left)
            gmat = dot_split((xs_low[:, lanes], xs_rest[:, lanes]), (diag, diag_rest))
            mats, links = [], []
            for h in range(2):
                head = (c + p * LANES) // HEAD + h
                gap = cum_t[head : head + 1, :] - wide(cum[:, head : head + 1], LANES) + mask
                decay = jnp.exp2(gap)
                mat = decay * scores
                grad = gmat[:, h * LANES : (h + 1) * LANES]
                grad_scores += decay * grad
                mats.append(split(mat, 2))
                links.append((mat * grad).astype(bf16))
            high = jnp.concatenate([mats[0][0], mats[1][0]], axis=1)
            rest = jnp.concatenate([mats[0][1], mats[1][1]], axis=1)
            parts.append(dot(high, diag) + dot(high, diag_rest) + dot(rest, diag))
            reach = dot(jnp.concatenate(links, axis=1), pair_ref[...])
            for h in range(2):
                head = (c + p * LANES) // HEAD + h
                da_rows[head : head + 1, :] = jnp.sum(
                    reach[:, h * LANES : (h + 1) * LANES] * before, axis=0, keepdims=True
                )
        g_xs = jnp.concatenate(parts, axis=1) + e_e * into
        gext[0:Q, at] = (t_e * g_xs + skip_ref[:, at] * gm) * slope
        sums = jnp.concatenate(
            [pair_split(carried * gm), pair_split(x * into), pair_split(x * g_xs)], axis=0
        )
        sums = dot(sums, twice(et_ref[at, :], 0))
        s_gm = (s_e * gm).astype(bf16)
        part_c = dot(s_gm, st_low, NT)
        part_b = dot((e_e * xs).astype(bf16), ad_low, NT)
        if c == 0:
            spread[...] = sums
            grad_c[...] = part_c
            grad_b[...] = part_b
        else:
            spread[...] += sums
            grad_c[...] += part_c
            grad_b[...] += part_b
        gskip_ref[:, at] += fold_rows(gm * x)
        link[:, at] = fold_rows(st_low.astype(f32) * ad)
        adj[:, at] = ad * s_e[Q - 1 : Q, :] + dot(ct, s_gm)

    grad_low = grad_scores.astype(bf16)
    g_b = grad_b[...] + dot(grad_low, cm)
    g_c = grad_c[...] + dot(grad_low, bm, TN)
    gext[0:Q, pl.ds(inner, 256)] = jnp.concatenate([g_b, g_c], axis=1) * slope_bc

    phi = start * spread[0:Q]
    psi = end * ts * spread[Q : 2 * Q]
    through = jnp.sum(dot(jnp.concatenate(split(link[...], 2), axis=0), et_ref[...]), axis=0, keepdims=True)
    around = jnp.concatenate(split(phi, 2) + split(psi, 2), axis=0)
    da = da_rows[...].T + dot(tail_ref[...], around) + start[Q - 1 : Q, :] * through
    g_ts = spread[2 * Q :] + rate * da
    galog_ref[...] += fold_rows(ts * rate * da)
    g_dt = g_ts * sigmoid(raw)
    gdtb_ref[...] += fold_rows(g_dt)

    n1, n2, n3 = (wide(cols[:, k : k + 1], 256) for k in (6, 7, 8))
    for c in range(0, channels, 256):
        at = pl.ds(c, 256)
        x = xbc_ref[:, at]
        g = gext[:, at]
        g0 = g[:Q]
        g1 = later_rows(g, 1) * n1
        g2 = later_rows(g, 2) * n2
        g3 = later_rows(g, 3) * n3
        gx = cw_ref[3:4, at] * g0 + cw_ref[2:3, at] * g1 + cw_ref[1:2, at] * g2 + cw_ref[0:1, at] * g3
        gx_ref[:, at] = gx.astype(bf16)
        gcb_ref[:, at] += fold_rows(g0)
        gcw_ref[24:32, at] += fold_rows(g0 * x)
        gcw_ref[16:24, at] += fold_rows(g1 * x)
        gcw_ref[8:16, at] += fold_rows(g2 * x)
        gcw_ref[0:8, at] += fold_rows(g3 * x)
    gx_ref[:, channels:] = g_dt.astype(bf16)


def state_backward(seg, xbc, dt, s, sin, gm, cw, head, seqs):
    rows, channels = xbc.shape
    inner = gm.shape[1]
    blocks = rows // seqs // Q
    at = lambda s, b: (s * blocks + blocks - 1 - b, 0)
    at3 = lambda s, b: (s * blocks + blocks - 1 - b, 0, 0)
    return pl.pallas_call(
        bwd_kernel,
        grid=(seqs, blocks),
        in_specs=[
            fixed(seg.shape),
            pl.BlockSpec((Q, channels), at),
            pl.BlockSpec((Q, LANES), at),
            pl.BlockSpec((Q, channels), at),
            pl.BlockSpec((None, LANES, inner), at3),
            pl.BlockSpec((Q, inner), at),
        ]
        + [fixed(v.shape) for v in (cw, head)],
        out_specs=[
            pl.BlockSpec((Q, channels + LANES), at),
            fixed((32, channels)), fixed((8, channels)), fixed((8, inner)), fixed((8, LANES)), fixed((8, LANES)),
        ],
        out_shape=[
            jax.ShapeDtypeStruct((rows, channels + LANES), bf16),
            jax.ShapeDtypeStruct((32, channels), f32),
            jax.ShapeDtypeStruct((8, channels), f32),
            jax.ShapeDtypeStruct((8, inner), f32),
            jax.ShapeDtypeStruct((8, LANES), f32),
            jax.ShapeDtypeStruct((8, LANES), f32),
        ],
        scratch_shapes=[
            pltpu.VMEM((LANES, inner), f32),
            pltpu.VMEM((Q + 8, channels), f32),
            pltpu.VMEM((LANES, LANES), f32),
            pltpu.VMEM((3 * Q, LANES), f32),
            pltpu.VMEM((Q, LANES), f32),
            pltpu.VMEM((Q, LANES), f32),
            pltpu.VMEM((8, inner), f32),
            pltpu.VMEM((2 * LANES, inner), bf16),
            pltpu.VMEM((Q, Q), bf16),
            pltpu.VMEM((1, inner), f32),
            pltpu.VMEM((inner, LANES), bf16),
            pltpu.VMEM((Q, 4 * Q), bf16),
            pltpu.VMEM((2 * Q, 2 * Q), bf16),
        ],
        compiler_params=params(60 << 20),
        name="state_backward",
    )(seg, xbc, dt, s, sin, gm, cw, head)


def token_kernel(tok_ref, cot_ref, gz_ref, gx_ref, wa_ref, wb_ref, wx_ref, gain_ref, out_ref, ggain_ref):
    half = gz_ref.shape[1] // 2
    g = dot(gz_ref[:, :half], flat(wa_ref), NT) + dot(gz_ref[:, half:], flat(wb_ref), NT)
    g += dot(gx_ref[...], wx_ref[...], NT)
    u = tok_ref[...].astype(f32)
    r = lax.rsqrt(jnp.mean(u * u, axis=-1, keepdims=True) + EPS)
    unit = u * r

    @pl.when(pl.program_id(0) == 0)
    def _():
        ggain_ref[...] = jnp.zeros_like(ggain_ref)

    ggain_ref[...] += fold_rows(unit * g)
    q = g * gain_ref[...]
    mean = jnp.mean(unit * q, axis=-1, keepdims=True)
    out_ref[...] = (cot_ref[...].astype(f32) + r * (q - unit * mean)).astype(bf16)


def token_grad(tok, cot, gz, gx, weights, wx, gain, tile=256):
    rows, width = tok.shape
    at = lambda i: (i, 0)
    return pl.pallas_call(
        token_kernel,
        grid=(rows // tile,),
        in_specs=[
            pl.BlockSpec((tile, width), at),
            pl.BlockSpec((tile, width), at),
            pl.BlockSpec((tile, gz.shape[1]), at),
            pl.BlockSpec((tile, gx.shape[1]), at),
            *[spec for _, spec in weights], fixed(wx.shape), fixed(gain.shape),
        ],
        out_specs=[pl.BlockSpec((tile, width), at), fixed((8, width))],
        out_shape=[jax.ShapeDtypeStruct((rows, width), bf16), jax.ShapeDtypeStruct((8, width), f32)],
        compiler_params=params(60 << 20),
        name="token_grad",
    )(tok, cot, gz, gx, *[v for v, _ in weights], wx, gain)


def partner(axis, bit):
    me = lax.axis_index(axis)
    return {axis: me + bit - 2 * bit * ((me // bit) % 2)}


def finish_kernel(
    steps, heads, cw_ref, cb_ref, ggain_ref, skip_ref, ngain_ref, alog_ref, dtb_ref, zo_ref, x_ref,
    small_ref, din_ref, dout_ref, acc, got, zo_got, x_got, send, recv, big_send, big_recv,
):
    if steps:
        barrier = pltpu.get_barrier_semaphore()
    for axis, bit in steps:
        pl.semaphore_signal(barrier, inc=1, device_id=partner(axis, bit), device_id_type=pl.DeviceIdType.MESH)
    if steps:
        pl.semaphore_wait(barrier, len(steps))

    def exchange(src, dst, ssem, rsem, axis, bit):
        copy = pltpu.make_async_remote_copy(
            src_ref=src, dst_ref=dst, send_sem=ssem, recv_sem=rsem,
            device_id=partner(axis, bit), device_id_type=pl.DeviceIdType.MESH,
        )
        copy.start()
        return copy

    big = []
    for axis, bit in steps[-1:]:
        big.append(exchange(zo_ref, zo_got, big_send.at[0], big_recv.at[0], axis, bit))
        big.append(exchange(x_ref, x_got, big_send.at[1], big_recv.at[1], axis, bit))

    inner, width = ggain_ref.shape[1], ngain_ref.shape[1]
    channels = cb_ref.shape[1]
    total = lambda v: jnp.sum(v, axis=0, keepdims=True)
    acc[0] = jnp.zeros((8, channels), f32)
    for k in range(4):
        acc[0, k : k + 1, :] = total(cw_ref[8 * k : 8 * k + 8, :])
    acc[0, 4:5, :] = total(cb_ref[...])
    acc[0, 5:6, :inner] = total(ggain_ref[...])
    acc[0, 6:7, :width] = total(ngain_ref[...])
    acc[0, 6:7, width : width + LANES] = total(alog_ref[...])
    acc[0, 6:7, width + LANES : width + 2 * LANES] = total(dtb_ref[...])
    skip = jnp.concatenate(split(skip_ref[...], 3), axis=0)
    by_head = ones_where(iota((inner, LANES), 0) // HEAD == iota((inner, LANES), 1))
    acc[0, 6:7, width + 2 * LANES : width + 3 * LANES] = total(dot(skip, by_head))

    for k, (axis, bit) in enumerate(steps):
        exchange(acc.at[k], got.at[k], send.at[k], recv.at[k], axis, bit).wait()
        acc[k + 1] = acc[k] + got[k]
    small_ref[...] = acc[len(steps)]

    for copy in big:
        copy.wait()
    own = din_ref.shape[0]
    zo = zo_ref[...].astype(f32) + zo_got[...].astype(f32)
    half = zo.shape[1]
    din_ref[:, :half] = zo[:own]
    din_ref[:, half : 2 * half] = zo[own : 2 * own]
    dout_ref[...] = zo[2 * own :]
    left = din_ref.shape[1] - 2 * half
    din_ref[:, 2 * half :] = (x_ref[...].astype(f32) + x_got[...].astype(f32))[:, :left]


def finish(p_cw, p_cb, p_ggain, p_skip, p_ngain, p_alog, p_dtb, d_zo, d_x, sizes, heads, proj):
    steps = [(axis, 1 << i) for axis, n in sizes for i in range(n.bit_length() - 1)]
    own, half = d_x.shape[0], d_zo.shape[1]
    channels = p_cb.shape[1]
    vmem = pl.BlockSpec(memory_space=pltpu.VMEM)
    return pl.pallas_call(
        functools.partial(finish_kernel, steps, heads),
        in_specs=[vmem] * 9,
        out_specs=[vmem] * 3,
        out_shape=[
            jax.ShapeDtypeStruct((8, channels), f32),
            jax.ShapeDtypeStruct((own, proj), f32),
            jax.ShapeDtypeStruct((2 * own, half), f32),
        ],
        scratch_shapes=[
            pltpu.VMEM((len(steps) + 1, 8, channels), f32),
            pltpu.VMEM((max(len(steps), 1), 8, channels), f32),
            pltpu.VMEM(d_zo.shape, bf16),
            pltpu.VMEM(d_x.shape, bf16),
            pltpu.SemaphoreType.DMA((max(len(steps), 1),)),
            pltpu.SemaphoreType.DMA((max(len(steps), 1),)),
            pltpu.SemaphoreType.DMA((2,)),
            pltpu.SemaphoreType.DMA((2,)),
        ],
        compiler_params=params(48 << 20, collective_id=0 if steps else None, has_side_effects=True),
        name="finish",
    )(p_cw, p_cb, p_ggain, p_skip, p_ngain, p_alog, p_dtb, d_zo, d_x)


def per_device(
    sizes, tokens, segments, cotangent, norm_gain, weight_in, conv_weight, conv_bias, dt_bias, a_log, skip_d,
    gate_gain, weight_out,
):
    seqs, length, width = tokens.shape
    rows = seqs * length
    inner = gate_gain.shape[0]
    channels = conv_bias.shape[0]
    heads = dt_bias.shape[0]
    own = weight_in.shape[0]
    owners = width // own
    tok = tokens.reshape(rows, width)
    cot = cotangent.reshape(rows, width)
    pad = LANES - heads

    local_x = jnp.pad(weight_in[:, inner:], ((0, 0), (0, pad)))
    wx = lax.all_gather(local_x, "dp", axis=0, tiled=True)
    local_zo = jnp.concatenate([weight_in[:, :width], weight_in[:, width:inner], weight_out], axis=0)
    slab = lax.all_gather(local_zo, "dp", axis=0, tiled=True).reshape(owners, 4 * own, width)
    weights = slab_views(slab, own)

    head = jnp.pad(jnp.stack([dt_bias, -jnp.exp(a_log), skip_d]), ((0, 5), (0, pad)))
    seg = segments.astype(f32).reshape(rows // Q, Q)
    cb = conv_bias.reshape(1, channels)
    ngain = norm_gain.reshape(1, width)
    ggain = gate_gain.reshape(1, inner)

    normed, xbc, dt = project(tok, ngain, wx, channels)
    y, s, sin = state_forward(seg, xbc, dt, conv_weight, cb, head, inner, seqs)
    gn, out, gz, gm, p_ggain = gate(tok, normed, y, cot, weights, ggain)
    d_z = dot(normed, gz, TN).astype(bf16)
    d_out = dot(gn, cot, TN).astype(bf16)
    d_zo = jnp.concatenate(
        [
            d_z[:, :width].reshape(owners, own, width),
            d_z[:, width:].reshape(owners, own, width),
            d_out.reshape(owners, 2 * own, width),
        ],
        axis=1,
    ).reshape(owners * 4 * own, width)
    d_zo, gm = lax.optimization_barrier((d_zo, gm))
    d_zo = lax.psum_scatter(d_zo, "dp", scatter_dimension=0, tiled=True)
    gx, p_cw, p_cb, p_skip, p_alog, p_dtb = state_backward(seg, xbc, dt, s, sin, gm, conv_weight, head, seqs)
    d_x = dot(normed, gx, TN).astype(bf16)
    d_x, d_zo = lax.optimization_barrier((d_x, d_zo))
    d_x = lax.psum_scatter(d_x, "dp", scatter_dimension=0, tiled=True)
    g_tok, p_ngain = token_grad(tok, cot, gz, gx, weights[:2], wx, ngain)
    small, d_in, d_out = finish(
        p_cw, p_cb, p_ggain, p_skip, p_ngain, p_alog, p_dtb, d_zo, d_x, sizes, heads, weight_in.shape[1]
    )
    return (
        out.reshape(tokens.shape),
        g_tok.reshape(tokens.shape),
        small[6, :width],
        d_in,
        small[:4],
        small[4],
        small[6, width + LANES : width + LANES + heads],
        small[6, width : width + heads],
        small[6, width + 2 * LANES : width + 2 * LANES + heads],
        small[5, :inner],
        d_out,
    )


def solution(mesh):
    data = P(("dp", "seq"), None, None)
    owned = P("dp", None)
    placed = (data, P(("dp", "seq"), None), data, P(), owned, P(), P(), P(), P(), P(), P(), owned)
    return jax.shard_map(
        functools.partial(per_device, [(axis, mesh.shape[axis]) for axis in ("dp", "seq")]),
        mesh=mesh,
        in_specs=placed,
        out_specs=(data, data, P(), owned, P(), P(), P(), P(), P(), P(), owned),
        check_vma=False,
    )
```

```python
import functools
import math

import jax
import jax.numpy as jnp
from jax import lax
from jax.experimental import pallas as pl
from jax.experimental.pallas import tpu as pltpu
from jax.sharding import PartitionSpec as P

f32 = jnp.float32
bf16 = jnp.bfloat16
HEAD = 64
Q = 128
LANES = 128
EPS = 1e-05
LOG2E = math.log2(math.e)
NEG = -1e30

NN = (((1,), (0,)), ((), ()))
NT = (((1,), (1,)), ((), ()))
TN = (((0,), (0,)), ((), ()))


def dot(a, b, dims=NN):
    return lax.dot_general(a, b, dims, preferred_element_type=f32)


def pair_split(v):
    return jnp.concatenate(split(v, 2), axis=1)


def twice(v, axis):
    return jnp.concatenate([v, v], axis=axis)


def dot_split(a, b):
    low = b[1]
    return dot(jnp.concatenate(a, axis=1), twice(b[0], 1), NT) + dot(a[0], low, NT)


def sigmoid(v):
    return 0.5 + 0.5 * jnp.tanh(0.5 * v)


def split(v, parts):
    out = []
    for _ in range(parts):
        low = v.astype(bf16)
        out.append(low)
        v = v - low.astype(f32)
    return out


def fold_rows(v):
    return jnp.sum(v.reshape(v.shape[0] // 8, 8, v.shape[1]), axis=0)


def wide(v, width):
    col = jnp.broadcast_to(v, (v.shape[0], LANES))
    return jnp.concatenate([col] * (width // LANES), axis=1)


def params(limit=None, **more):
    return pltpu.CompilerParams(vmem_limit_bytes=limit, **more)


def proj_kernel(tok_ref, gain_ref, wx_ref, normed_ref, xbc_ref, dt_ref):
    u = tok_ref[...].astype(f32)
    r = lax.rsqrt(jnp.mean(u * u, axis=-1, keepdims=True) + EPS)
    normed = (u * r * gain_ref[...]).astype(bf16)
    normed_ref[...] = normed
    out = dot(normed, wx_ref[...])
    ch = xbc_ref.shape[1]
    xbc_ref[...] = out[:, :ch]
    dt_ref[...] = out[:, ch:]


def project(tok, gain, wx, channels, tile=256):
    rows, width = tok.shape
    cols = wx.shape[1]
    return pl.pallas_call(
        proj_kernel,
        grid=(rows // tile,),
        in_specs=[
            pl.BlockSpec((tile, width), lambda i: (i, 0)),
            pl.BlockSpec((1, width), lambda i: (0, 0)),
            pl.BlockSpec((width, cols), lambda i: (0, 0)),
        ],
        out_specs=[
            pl.BlockSpec((tile, width), lambda i: (i, 0)),
            pl.BlockSpec((tile, channels), lambda i: (i, 0)),
            pl.BlockSpec((tile, cols - channels), lambda i: (i, 0)),
        ],
        out_shape=[
            jax.ShapeDtypeStruct((rows, width), bf16),
            jax.ShapeDtypeStruct((rows, channels), f32),
            jax.ShapeDtypeStruct((rows, cols - channels), f32),
        ],
        compiler_params=params(60 << 20),
        name="project",
    )(tok, gain, wx)


def segment_rows(seg_ref, block, blocks, at):
    rows = seg_ref.shape[0]
    none = jnp.full((1, LANES), -1.0, f32)
    seg = seg_ref[pl.ds(at, 1), :]
    prev = jnp.where(block > 0, seg_ref[pl.ds(jnp.maximum(at - 1, 0), 1), :], none)
    after = jnp.where(block < blocks - 1, seg_ref[pl.ds(jnp.minimum(at + 1, rows - 1), 1), :], none)
    lane = lax.broadcasted_iota(jnp.int32, (1, LANES), 1)

    def same(other):
        return (other == seg).astype(f32)

    out = [seg]
    for k in (1, 2, 3):
        out.append(same(jnp.where(lane < k, pltpu.roll(prev, k, 1), pltpu.roll(seg, k, 1))))
    out.append(same(jnp.broadcast_to(prev[:, LANES - 1 :], (1, LANES))))
    out.append(same(jnp.broadcast_to(seg[:, LANES - 1 :], (1, LANES))))
    for k in (1, 2, 3):
        turn = LANES - k
        out.append(same(jnp.where(lane >= turn, pltpu.roll(after, turn, 1), pltpu.roll(seg, turn, 1))))
    tab = jnp.concatenate(out + [none] * (16 - len(out)), axis=0)
    return seg, jnp.concatenate([tab] * (LANES // 16), axis=0).T


def iota(shape, axis):
    return lax.broadcasted_iota(jnp.int32, shape, axis)


def ones_where(cond):
    return jnp.where(cond, 1.0, 0.0).astype(bf16)


def head_columns(heads_wide, inner, width):
    return ones_where(iota((heads_wide, inner), 0) % LANES == iota((heads_wide, inner), 1) // width)


def step_terms(dt, dtb, na2, tri, cols):
    raw = dt + dtb
    ts = jnp.maximum(raw, 0.0) + jnp.log1p(jnp.exp(-jnp.abs(raw)))
    cum = dot(jnp.concatenate([tri] * 3, axis=1), jnp.concatenate(split(ts * na2, 3), axis=0))
    start = jnp.exp2(cum) * wide(cols[:, 4:5], LANES)
    end = jnp.exp2(cum[Q - 1 : Q, :] - cum) * wide(cols[:, 5:6], LANES)
    return raw, ts, cum, start, end


def head_terms(head_ref):
    rate = head_ref[1:2, :]
    return head_ref[0:1, :], rate, rate * LOG2E


def fill_constants(e_ref, tri_ref, skip_ref, head_ref):
    inner = e_ref.shape[1]
    e_ref[...] = head_columns(e_ref.shape[0], inner, HEAD)
    tri_ref[...] = ones_where(iota((Q, Q), 0) >= iota((Q, Q), 1))
    skip = jnp.broadcast_to(head_ref[2:3, :], (8, LANES))
    wide_skip = dot(jnp.concatenate(split(skip, 3), axis=1), head_columns(3 * LANES, inner, HEAD))
    skip_ref[...] = wide_skip[0:1]


def expand_operand(*terms):
    return jnp.concatenate([jnp.concatenate(split(t, 2), axis=1) for t in terms], axis=0)


def by_head(v, left):
    zero = jnp.zeros_like(v)
    return jnp.concatenate([jnp.where(left, v, zero), jnp.where(left, zero, v)], axis=0)


def later_rows(v, k):
    width = v.shape[1]
    v = pltpu.roll(v.reshape(-1, 8, width), 8 - k, 1)
    here = lax.broadcasted_iota(jnp.int32, (1, 8, width), 1) < 8 - k
    return jnp.where(here, v[:-1], v[1:]).reshape(-1, width)


def fwd_kernel(
    seg_ref, xbc_ref, dt_ref, cw_ref, cb_ref, head_ref,
    y_ref, s_ref, sin_ref, state, ext, e_ref, tri_ref, skip_ref,
):
    inner = y_ref.shape[1]
    channels = cb_ref.shape[1]
    b, blocks = pl.program_id(1), pl.num_programs(1)
    dtb, _, na2 = head_terms(head_ref)

    @pl.when((b == 0) & (pl.program_id(0) == 0))
    def _():
        fill_constants(e_ref, tri_ref, skip_ref, head_ref)

    @pl.when(b == 0)
    def _():
        state[...] = jnp.zeros_like(state)
        ext[0:8, :] = jnp.zeros((8, channels), f32)

    @pl.when(b > 0)
    def _():
        ext[0:8, :] = ext[Q : Q + 8, :]

    ext[8 : 8 + Q, :] = xbc_ref[...]
    seg, cols = segment_rows(seg_ref, b, blocks, pl.program_id(0) * blocks + b)
    m1, m2, m3 = (wide(cols[:, k : k + 1], 256) for k in (1, 2, 3))

    def conv(c):
        at = pl.ds(c, 256)
        x = ext[:, at]
        s = cb_ref[:, at] + cw_ref[3:4, at] * x[8:]
        s += m1 * (cw_ref[2:3, at] * later_rows(x, 7))
        s += m2 * (cw_ref[1:2, at] * later_rows(x, 6))
        s += m3 * (cw_ref[0:1, at] * later_rows(x, 5))
        s_ref[:, at] = s
        return s * sigmoid(s)

    bc, bc_rest = split(conv(inner), 2)
    bm, cm = bc[:, :LANES], bc[:, LANES:]
    bt = bm.T
    c_two = jnp.concatenate([cm, bc_rest[:, LANES:]], axis=1)
    _, ts, cum, start, end = step_terms(dt_ref[...], dtb, na2, tri_ref[...], cols)
    cum_t = cum.T
    grow = expand_operand(start, end, ts)
    row_i = lax.broadcasted_iota(jnp.int32, (Q, Q), 0)
    col_j = lax.broadcasted_iota(jnp.int32, (Q, Q), 1)
    same = wide(cols[:, 0:1], LANES) == seg
    mask = jnp.where(same & (row_i >= col_j), 0.0, NEG)
    scores = dot_split((cm, bc_rest[:, LANES:]), (bm, bc_rest[:, :LANES]))
    left = col_j < HEAD

    for c in range(0, inner, 256):
        at = pl.ds(c, 256)
        x = conv(c)
        big = dot(grow, e_ref[:, at])
        s_e, e_e, t_e = big[:Q], big[Q : 2 * Q], big[2 * Q :]
        xs = x * t_e
        xs_low = xs.astype(bf16)
        st = state[:, at]
        st_low = st.astype(bf16)
        sin_ref[:, at] = st_low
        carried = dot(c_two, twice(st_low, 0))
        parts = []
        for p in range(2):
            mats = []
            for h in range(2):
                head = (c + p * LANES) // HEAD + h
                gap = wide(cum[:, head : head + 1], LANES) - cum_t[head : head + 1, :] + mask
                mats.append((jnp.exp2(gap) * scores).astype(bf16))
            xp = xs_low[:, p * LANES : (p + 1) * LANES]
            parts.append(dot(jnp.concatenate(mats, axis=1), by_head(xp, left)))
        y = jnp.concatenate(parts, axis=1) + s_e * carried + skip_ref[:, at] * x
        y_ref[:, at] = y
        state[:, at] = st * s_e[Q - 1 : Q, :] + dot(bt, (xs * e_e).astype(bf16))


def fixed(shape):
    return pl.BlockSpec(shape, lambda *_: (0,) * len(shape))


def state_forward(seg, xbc, dt, cw, cb, head, inner, seqs):
    rows, channels = xbc.shape
    blocks = rows // seqs // Q
    at = lambda s, b: (s * blocks + b, 0)
    at3 = lambda s, b: (s * blocks + b, 0, 0)
    return pl.pallas_call(
        fwd_kernel,
        grid=(seqs, blocks),
        in_specs=[
            fixed(seg.shape),
            pl.BlockSpec((Q, channels), at),
            pl.BlockSpec((Q, LANES), at),
            fixed(cw.shape), fixed(cb.shape), fixed(head.shape),
        ],
        out_specs=[
            pl.BlockSpec((Q, inner), at),
            pl.BlockSpec((Q, channels), at),
            pl.BlockSpec((None, LANES, inner), at3),
        ],
        out_shape=[
            jax.ShapeDtypeStruct((rows, inner), f32),
            jax.ShapeDtypeStruct((rows, channels), f32),
            jax.ShapeDtypeStruct((seqs * blocks, LANES, inner), bf16),
        ],
        scratch_shapes=[
            pltpu.VMEM((LANES, inner), f32),
            pltpu.VMEM((Q + 8, channels), f32),
            pltpu.VMEM((2 * LANES, inner), bf16),
            pltpu.VMEM((Q, Q), bf16),
            pltpu.VMEM((1, inner), f32),
        ],
        compiler_params=params(60 << 20),
        name="state_forward",
    )(seg, xbc, dt, cw, cb, head)


def flat(ref):
    v = ref[...]
    return v.reshape(v.shape[0] * v.shape[1], v.shape[2])


def slab_views(slab, own):
    owners, _, width = slab.shape
    if own % 16 == 0:
        first = lambda *_: (0, 0, 0)
        second = lambda *_: (0, 1, 0)
        sizes = ((own, first), (own, second), (2 * own, second))
        return [(slab, pl.BlockSpec((owners, n, width), index)) for n, index in sizes]
    parts = [
        v.reshape(1, -1, width) for v in (slab[:, :own], slab[:, own : 2 * own], slab[:, 2 * own :])
    ]
    return [(v, fixed(v.shape)) for v in parts]


def gate_kernel(
    tok_ref, normed_ref, y_ref, cot_ref, wa_ref, wb_ref, wo_ref, gain_ref,
    gn_ref, out_ref, gz_ref, gm_ref, ggain_ref,
):
    wa, wb, wo = flat(wa_ref), flat(wb_ref), flat(wo_ref)
    gain = gain_ref[...]

    @pl.when(pl.program_id(0) == 0)
    def _():
        ggain_ref[...] = jnp.zeros_like(ggain_ref)

    normed = normed_ref[...]
    z = jnp.concatenate([dot(normed, wa), dot(normed, wb)], axis=1)
    g_gn = dot(cot_ref[...], wo, NT)
    sg = sigmoid(z)
    sz = z * sg
    y = y_ref[...]
    gated = y * sz
    rstd = lax.rsqrt(jnp.mean(gated * gated, axis=-1, keepdims=True) + EPS)
    unit = gated * rstd
    gn = (unit * gain).astype(bf16)
    gn_ref[...] = gn
    out_ref[...] = (tok_ref[...].astype(f32) + dot(gn, wo)).astype(bf16)
    ggain_ref[...] += fold_rows(unit * g_gn)
    q = g_gn * gain
    mean = jnp.mean(unit * q, axis=-1, keepdims=True)
    g_gated = rstd * (q - unit * mean)
    gm_ref[...] = g_gated * sz
    gz_ref[...] = (g_gated * y * (sg * (1.0 + z * (1.0 - sg)))).astype(bf16)


def gate(tok, normed, y, cot, weights, gain, tile=256):
    rows, width = tok.shape
    inner = y.shape[1]
    at = lambda i: (i, 0)
    return pl.pallas_call(
        gate_kernel,
        grid=(rows // tile,),
        in_specs=[
            pl.BlockSpec((tile, width), at),
            pl.BlockSpec((tile, width), at),
            pl.BlockSpec((tile, inner), at),
            pl.BlockSpec((tile, width), at),
            *[spec for _, spec in weights], fixed(gain.shape),
        ],
        out_specs=[
            pl.BlockSpec((tile, inner), at),
            pl.BlockSpec((tile, width), at),
            pl.BlockSpec((tile, inner), at),
            pl.BlockSpec((tile, inner), at),
            fixed((8, inner)),
        ],
        out_shape=[
            jax.ShapeDtypeStruct((rows, inner), bf16),
            jax.ShapeDtypeStruct((rows, width), bf16),
            jax.ShapeDtypeStruct((rows, inner), bf16),
            jax.ShapeDtypeStruct((rows, inner), f32),
            jax.ShapeDtypeStruct((8, inner), f32),
        ],
        compiler_params=params(60 << 20),
        name="gate",
    )(tok, normed, y, cot, *[v for v, _ in weights], gain)


def bwd_kernel(
    seg_ref, xbc_ref, dt_ref, s_ref, sin_ref, gm_ref, cw_ref, head_ref,
    gx_ref, gcw_ref, gcb_ref, gskip_ref, galog_ref, gdtb_ref,
    adj, gext, da_rows, spread, grad_b, grad_c, link, e_ref, tri_ref, skip_ref, et_ref, tail_ref, pair_ref,
):
    inner = gm_ref.shape[1]
    channels = s_ref.shape[1]
    b, blocks = pl.program_id(1), pl.num_programs(1)
    dtb, rate, na2 = head_terms(head_ref)

    @pl.when((b == 0) & (pl.program_id(0) == 0))
    def _():
        for ref in (gcw_ref, gcb_ref, gskip_ref, galog_ref, gdtb_ref, da_rows):
            ref[...] = jnp.zeros_like(ref)
        fill_constants(e_ref, tri_ref, skip_ref, head_ref)
        et_ref[...] = ones_where(iota((inner, LANES), 0) // HEAD == iota((inner, LANES), 1))
        turned = ones_where(iota((Q, Q), 0) <= iota((Q, Q), 1))
        below = ones_where(iota((Q, Q), 0) > iota((Q, Q), 1))
        tail_ref[...] = jnp.concatenate([turned, turned, below, below], axis=1)
        row, col = iota((2 * Q, 2 * Q), 0), iota((2 * Q, 2 * Q), 1)
        pair_ref[...] = ones_where((row // Q == col // Q) & (row >= col))

    @pl.when(b == 0)
    def _():
        adj[...] = jnp.zeros_like(adj)
        gext[Q : Q + 8, :] = jnp.zeros((8, channels), f32)

    @pl.when(b > 0)
    def _():
        gext[Q : Q + 8, :] = gext[0:8, :]

    turn = blocks - 1 - b
    seg, cols = segment_rows(seg_ref, turn, blocks, pl.program_id(0) * blocks + turn)
    raw, ts, cum, start, end = step_terms(dt_ref[...], dtb, na2, tri_ref[...], cols)
    cum_t = cum.T
    grow = expand_operand(start, end, ts)

    def act(c):
        s = s_ref[:, pl.ds(c, 256)]
        sg = sigmoid(s)
        return s * sg, sg * (1.0 + s * (1.0 - sg))

    bc, slope_bc = act(inner)
    bc, bc_rest = split(bc, 2)
    bm, cm = bc[:, :LANES], bc[:, LANES:]
    ct = cm.T
    b_two = jnp.concatenate([bm, bc_rest[:, :LANES]], axis=1)
    c_two = jnp.concatenate([cm, bc_rest[:, LANES:]], axis=1)
    row_j = lax.broadcasted_iota(jnp.int32, (Q, Q), 0)
    col_i = lax.broadcasted_iota(jnp.int32, (Q, Q), 1)
    same = wide(cols[:, 0:1], LANES) == seg
    mask = jnp.where(same & (col_i >= row_j), 0.0, NEG)
    before = (row_j < col_i).astype(f32)
    scores = dot_split((bm, bc_rest[:, :LANES]), (cm, bc_rest[:, LANES:]))
    left = col_i < HEAD
    grad_scores = jnp.zeros((Q, Q), f32)

    for c in range(0, inner, 256):
        at = pl.ds(c, 256)
        x, slope = act(c)
        big = dot(grow, e_ref[:, at])
        s_e, e_e, t_e = big[:Q], big[Q : 2 * Q], big[2 * Q :]
        xs = x * t_e
        xs_low, xs_rest = split(xs, 2)
        gm = gm_ref[:, at]
        gm_low, gm_rest = split(gm, 2)
        ad = adj[:, at]
        ad_low, ad_rest = split(ad, 2)
        st_low = sin_ref[:, at]
        into = dot(b_two, twice(ad_low, 0)) + dot(bm, ad_rest)
        carried = dot(c_two, twice(st_low, 0))
        parts = []
        for p in range(2):
            lanes = slice(p * LANES, (p + 1) * LANES)
            diag, diag_rest = by_head(gm_low[:, lanes], left), by_head(gm_rest[:, lanes], left)
            gmat = dot_split((xs_low[:, lanes], xs_rest[:, lanes]), (diag, diag_rest))
            mats, links = [], []
            for h in range(2):
                head = (c + p * LANES) // HEAD + h
                gap = cum_t[head : head + 1, :] - wide(cum[:, head : head + 1], LANES) + mask
                decay = jnp.exp2(gap)
                mat = decay * scores
                grad = gmat[:, h * LANES : (h + 1) * LANES]
                grad_scores += decay * grad
                mats.append(split(mat, 2))
                links.append((mat * grad).astype(bf16))
            high = jnp.concatenate([mats[0][0], mats[1][0]], axis=1)
            rest = jnp.concatenate([mats[0][1], mats[1][1]], axis=1)
            parts.append(dot(high, diag) + dot(high, diag_rest) + dot(rest, diag))
            reach = dot(jnp.concatenate(links, axis=1), pair_ref[...])
            for h in range(2):
                head = (c + p * LANES) // HEAD + h
                da_rows[head : head + 1, :] = jnp.sum(
                    reach[:, h * LANES : (h + 1) * LANES] * before, axis=0, keepdims=True
                )
        g_xs = jnp.concatenate(parts, axis=1) + e_e * into
        gext[0:Q, at] = (t_e * g_xs + skip_ref[:, at] * gm) * slope
        sums = jnp.concatenate(
            [pair_split(carried * gm), pair_split(x * into), pair_split(x * g_xs)], axis=0
        )
        sums = dot(sums, twice(et_ref[at, :], 0))
        s_gm = (s_e * gm).astype(bf16)
        part_c = dot(s_gm, st_low, NT)
        part_b = dot((e_e * xs).astype(bf16), ad_low, NT)
        if c == 0:
            spread[...] = sums
            grad_c[...] = part_c
            grad_b[...] = part_b
        else:
            spread[...] += sums
            grad_c[...] += part_c
            grad_b[...] += part_b
        gskip_ref[:, at] += fold_rows(gm * x)
        link[:, at] = fold_rows(st_low.astype(f32) * ad)
        adj[:, at] = ad * s_e[Q - 1 : Q, :] + dot(ct, s_gm)

    grad_low = grad_scores.astype(bf16)
    g_b = grad_b[...] + dot(grad_low, cm)
    g_c = grad_c[...] + dot(grad_low, bm, TN)
    gext[0:Q, pl.ds(inner, 256)] = jnp.concatenate([g_b, g_c], axis=1) * slope_bc

    phi = start * spread[0:Q]
    psi = end * ts * spread[Q : 2 * Q]
    through = jnp.sum(dot(jnp.concatenate(split(link[...], 2), axis=0), et_ref[...]), axis=0, keepdims=True)
    around = jnp.concatenate(split(phi, 2) + split(psi, 2), axis=0)
    da = da_rows[...].T + dot(tail_ref[...], around) + start[Q - 1 : Q, :] * through
    g_ts = spread[2 * Q :] + rate * da
    galog_ref[...] += fold_rows(ts * rate * da)
    g_dt = g_ts * sigmoid(raw)
    gdtb_ref[...] += fold_rows(g_dt)

    n1, n2, n3 = (wide(cols[:, k : k + 1], 256) for k in (6, 7, 8))
    for c in range(0, channels, 256):
        at = pl.ds(c, 256)
        x = xbc_ref[:, at]
        g = gext[:, at]
        g0 = g[:Q]
        g1 = later_rows(g, 1) * n1
        g2 = later_rows(g, 2) * n2
        g3 = later_rows(g, 3) * n3
        gx = cw_ref[3:4, at] * g0 + cw_ref[2:3, at] * g1 + cw_ref[1:2, at] * g2 + cw_ref[0:1, at] * g3
        gx_ref[:, at] = gx.astype(bf16)
        gcb_ref[:, at] += fold_rows(g0)
        gcw_ref[24:32, at] += fold_rows(g0 * x)
        gcw_ref[16:24, at] += fold_rows(g1 * x)
        gcw_ref[8:16, at] += fold_rows(g2 * x)
        gcw_ref[0:8, at] += fold_rows(g3 * x)
    gx_ref[:, channels:] = g_dt.astype(bf16)


def state_backward(seg, xbc, dt, s, sin, gm, cw, head, seqs):
    rows, channels = xbc.shape
    inner = gm.shape[1]
    blocks = rows // seqs // Q
    at = lambda s, b: (s * blocks + blocks - 1 - b, 0)
    at3 = lambda s, b: (s * blocks + blocks - 1 - b, 0, 0)
    return pl.pallas_call(
        bwd_kernel,
        grid=(seqs, blocks),
        in_specs=[
            fixed(seg.shape),
            pl.BlockSpec((Q, channels), at),
            pl.BlockSpec((Q, LANES), at),
            pl.BlockSpec((Q, channels), at),
            pl.BlockSpec((None, LANES, inner), at3),
            pl.BlockSpec((Q, inner), at),
        ]
        + [fixed(v.shape) for v in (cw, head)],
        out_specs=[
            pl.BlockSpec((Q, channels + LANES), at),
            fixed((32, channels)), fixed((8, channels)), fixed((8, inner)), fixed((8, LANES)), fixed((8, LANES)),
        ],
        out_shape=[
            jax.ShapeDtypeStruct((rows, channels + LANES), bf16),
            jax.ShapeDtypeStruct((32, channels), f32),
            jax.ShapeDtypeStruct((8, channels), f32),
            jax.ShapeDtypeStruct((8, inner), f32),
            jax.ShapeDtypeStruct((8, LANES), f32),
            jax.ShapeDtypeStruct((8, LANES), f32),
        ],
        scratch_shapes=[
            pltpu.VMEM((LANES, inner), f32),
            pltpu.VMEM((Q + 8, channels), f32),
            pltpu.VMEM((LANES, LANES), f32),
            pltpu.VMEM((3 * Q, LANES), f32),
            pltpu.VMEM((Q, LANES), f32),
            pltpu.VMEM((Q, LANES), f32),
            pltpu.VMEM((8, inner), f32),
            pltpu.VMEM((2 * LANES, inner), bf16),
            pltpu.VMEM((Q, Q), bf16),
            pltpu.VMEM((1, inner), f32),
            pltpu.VMEM((inner, LANES), bf16),
            pltpu.VMEM((Q, 4 * Q), bf16),
            pltpu.VMEM((2 * Q, 2 * Q), bf16),
        ],
        compiler_params=params(60 << 20),
        name="state_backward",
    )(seg, xbc, dt, s, sin, gm, cw, head)


def token_kernel(tok_ref, cot_ref, gz_ref, gx_ref, wa_ref, wb_ref, wx_ref, gain_ref, out_ref, ggain_ref):
    half = gz_ref.shape[1] // 2
    g = dot(gz_ref[:, :half], flat(wa_ref), NT) + dot(gz_ref[:, half:], flat(wb_ref), NT)
    g += dot(gx_ref[...], wx_ref[...], NT)
    u = tok_ref[...].astype(f32)
    r = lax.rsqrt(jnp.mean(u * u, axis=-1, keepdims=True) + EPS)
    unit = u * r

    @pl.when(pl.program_id(0) == 0)
    def _():
        ggain_ref[...] = jnp.zeros_like(ggain_ref)

    ggain_ref[...] += fold_rows(unit * g)
    q = g * gain_ref[...]
    mean = jnp.mean(unit * q, axis=-1, keepdims=True)
    out_ref[...] = (cot_ref[...].astype(f32) + r * (q - unit * mean)).astype(bf16)


def token_grad(tok, cot, gz, gx, weights, wx, gain, tile=256):
    rows, width = tok.shape
    at = lambda i: (i, 0)
    return pl.pallas_call(
        token_kernel,
        grid=(rows // tile,),
        in_specs=[
            pl.BlockSpec((tile, width), at),
            pl.BlockSpec((tile, width), at),
            pl.BlockSpec((tile, gz.shape[1]), at),
            pl.BlockSpec((tile, gx.shape[1]), at),
            *[spec for _, spec in weights], fixed(wx.shape), fixed(gain.shape),
        ],
        out_specs=[pl.BlockSpec((tile, width), at), fixed((8, width))],
        out_shape=[jax.ShapeDtypeStruct((rows, width), bf16), jax.ShapeDtypeStruct((8, width), f32)],
        compiler_params=params(60 << 20),
        name="token_grad",
    )(tok, cot, gz, gx, *[v for v, _ in weights], wx, gain)


MESH = pl.DeviceIdType.MESH


def place(line):
    me = lax.axis_index("dp")
    index = lambda l, x, c: (l * 2 + x) * 2 + c
    return me // 4, (me // 2) % 2, me % 2, index, lax.axis_index("seq")


def meet(devices):
    barrier = pltpu.get_barrier_semaphore()
    for device in devices:
        pl.semaphore_signal(barrier, inc=1, device_id=device, device_id_type=MESH)
    pl.semaphore_wait(barrier, len(devices))


def remote(src, dst, send, recv, device):
    return pltpu.make_async_remote_copy(
        src_ref=src, dst_ref=dst, send_sem=send, recv_sem=recv, device_id=device, device_id_type=MESH
    )


def gather_kernel(line, own_ref, out_ref, line_send, x_send, y_send, core_send, recv, local):
    l, x, c, index, y = place(line)
    others = [{"dp": index((l + k) % line, x, c)} for k in range(1, line)]
    beside, sibling, across = {"dp": index(l, 1 - x, c)}, {"dp": index(l, x, 1 - c)}, {"seq": 1 - y}
    meet(others + [beside, sibling, across])
    started = []

    def send(src, at, sem, device):
        copy = remote(src, out_ref.at[at], sem, recv.at[at], device)
        copy.start()
        started.append(copy)

    def arrived(at):
        remote(out_ref.at[at], out_ref.at[at], local.at[1], recv.at[at], sibling).wait_recv()

    mine = pltpu.make_async_copy(own_ref, out_ref.at[l, x, c], local.at[0])
    mine.start()
    for k in range(1, line):
        send(own_ref.at[y], (l, x, c, y), line_send.at[k], others[k - 1])
    send(own_ref.at[y], (l, x, c, y), x_send.at[0], beside)
    for h in range(2):
        send(own_ref.at[h], (l, x, c, h), core_send.at[0, h], sibling)
    for k in range(1, line):
        at = ((l + k) % line, x, c, y)
        arrived(at)
        send(out_ref.at[at], at, x_send.at[k], beside)
        send(out_ref.at[at], at, y_send.at[k], across)
        send(out_ref.at[at], at, core_send.at[k, 0], sibling)
    for k in range(line):
        at = ((l + k) % line, 1 - x, c, y)
        arrived(at)
        send(out_ref.at[at], at, y_send.at[line + k], across)
        send(out_ref.at[at], at, core_send.at[line + k, 0], sibling)
    for k in range(1, line):
        at = ((l + k) % line, x, c, 1 - y)
        arrived(at)
        send(out_ref.at[at], at, core_send.at[k, 1], sibling)
    for k in range(line):
        at = ((l + k) % line, 1 - x, c, 1 - y)
        arrived(at)
        send(out_ref.at[at], at, core_send.at[line + k, 1], sibling)
    for k in range(line):
        for side in range(2):
            for h in range(2):
                arrived(((l + k) % line, side, 1 - c, h))
    for copy in started:
        copy.wait_send()
    mine.wait()


def gather(local, owners):
    own, columns = local.shape
    line = owners // 4
    vmem = pl.BlockSpec(memory_space=pltpu.VMEM)
    dma = pltpu.SemaphoreType.DMA
    out = pl.pallas_call(
        functools.partial(gather_kernel, line),
        in_specs=[vmem],
        out_specs=vmem,
        out_shape=jax.ShapeDtypeStruct((line, 2, 2, 2, own // 2, columns), local.dtype),
        scratch_shapes=[
            dma((line,)), dma((line,)), dma((2 * line,)), dma((2 * line, 2)), dma((line, 2, 2, 2)), dma((2,)),
        ],
        compiler_params=params(48 << 20, collective_id=1, has_side_effects=True),
        name="gather",
    )(local.reshape(2, own // 2, columns))
    return out.reshape(owners * own, columns)


def pack_small(acc, cw_ref, cb_ref, ggain_ref, skip_ref, ngain_ref, alog_ref, dtb_ref):
    inner, width = ggain_ref.shape[1], ngain_ref.shape[1]
    total = lambda v: jnp.sum(v, axis=0, keepdims=True)
    acc[...] = jnp.zeros(acc.shape, f32)
    for k in range(4):
        acc[k : k + 1, :] = total(cw_ref[8 * k : 8 * k + 8, :])
    acc[4:5, :] = total(cb_ref[...])
    acc[5:6, :inner] = total(ggain_ref[...])
    acc[6:7, :width] = total(ngain_ref[...])
    acc[6:7, width : width + LANES] = total(alog_ref[...])
    acc[6:7, width + LANES : width + 2 * LANES] = total(dtb_ref[...])
    skip = jnp.concatenate(split(skip_ref[...], 3), axis=0)
    by_head = ones_where(iota((inner, LANES), 0) // HEAD == iota((inner, LANES), 1))
    acc[6:7, width + 2 * LANES : width + 3 * LANES] = total(dot(skip, by_head))


def finish_kernel(
    line, bits, cw_ref, cb_ref, ggain_ref, skip_ref, ngain_ref, alog_ref, dtb_ref, zo_ref, zo_got_ref, d_ref,
    small_ref, din_ref, dout_ref,
    acc, got, core_got, one, two_got, two, three_got, three, line_got, last, last_got,
    small_send, small_recv, core_send, core_recv, two_send, two_recv, three_send, three_recv,
    line_send, line_recv, last_sem,
):
    l, x, c, index, y = place(line)
    me = lax.axis_index("dp")
    doubling = [{"dp": me + bit - 2 * bit * ((me // bit) % 2)} for bit in bits]
    others = [{"dp": index((l + k) % line, x, c)} for k in range(1, line)]
    beside, sibling, across = {"dp": index(l, 1 - x, c)}, {"dp": index(l, x, 1 - c)}, {"seq": 1 - y}
    meet(doubling + others + [beside, sibling, across])
    order = list(range(1, line)) + [0]
    at = [(l + k) % line for k in order]

    def plus(a, b):
        return a.astype(f32) + b.astype(f32)

    def launch(*args):
        copy = remote(*args)
        copy.start()
        return copy

    first = []
    for i in range(line):
        first.append(
            launch(d_ref.at[at[i], :, 1 - c], core_got.at[i], core_send.at[i], core_recv.at[i], sibling)
        )
    pack_small(acc.at[0], cw_ref, cb_ref, ggain_ref, skip_ref, ngain_ref, alog_ref, dtb_ref)
    smalls = doubling + [across]
    second, third, fourth = [], [], []

    def small_start(k):
        return launch(acc.at[k], got.at[k], small_send.at[k], small_recv.at[k], smalls[k])

    for t in range(max(line + 2, len(smalls))):
        small = small_start(t) if t < len(smalls) else None
        if t < line:
            i = t
            first[i].wait()
            for a in range(2):
                for h in range(2):
                    one[i, a, h] = plus(d_ref[at[i], a, c, h], core_got[i, a, h]).astype(bf16)
            src, device = (one.at[i, 1 - x], beside) if i % 2 == 0 else (one.at[i, :, 1 - y], across)
            second.append(launch(src, two_got.at[i], two_send.at[i], two_recv.at[i], device))
        if 1 <= t <= line:
            i = t - 1
            second[i].wait()
            for j in range(2):
                kept = one[i, x, j] if i % 2 == 0 else one[i, j, y]
                two[i, j] = plus(kept, two_got[i, j]).astype(bf16)
            src, device = (two.at[i, 1 - y], across) if i % 2 == 0 else (two.at[i, 1 - x], beside)
            third.append(launch(src, three_got.at[i], three_send.at[i], three_recv.at[i], device))
        if 2 <= t <= line + 1:
            i = t - 2
            third[i].wait()
            kept = two[i, y] if i % 2 == 0 else two[i, x]
            three[i] = plus(kept, three_got[i]).astype(bf16)
            if order[i] > 0:
                fourth.append(
                    launch(three.at[i], line_got.at[l], line_send.at[i], line_recv.at[l], others[order[i] - 1])
                )
        if small is not None:
            small.wait()
            acc[t + 1] = acc[t] + got[t]

    small_ref[...] = acc[len(smalls)]
    own, half = din_ref.shape[0], zo_ref.shape[1]
    zo = plus(zo_ref[...], zo_got_ref[...])
    din_ref[:, :half] = zo[:own]
    din_ref[:, half : 2 * half] = zo[own : 2 * own]
    dout_ref[...] = zo[2 * own :]

    total = three[line - 1].astype(f32)
    for k in range(1, line):
        at_k = (l + k) % line
        remote(three.at[0], line_got.at[at_k], last_sem.at[2], line_recv.at[at_k], sibling).wait_recv()
        total += line_got[at_k].astype(f32)
    last[...] = total.astype(bf16)
    final = launch(last, last_got, last_sem.at[0], last_sem.at[1], across)
    for copy in fourth:
        copy.wait_send()
    final.wait()
    left = din_ref.shape[1] - 2 * half
    kept, came = last[...].astype(f32), last_got[...].astype(f32)
    lower = (y == 0).astype(f32)
    din_ref[: own // 2, 2 * half :] = (kept * lower + came * (1.0 - lower))[:, :left]
    din_ref[own // 2 :, 2 * half :] = (came * lower + kept * (1.0 - lower))[:, :left]


def finish(smalls, d_zo, zo_got, d_x, own, proj):
    owners = d_x.shape[0] // own
    line, columns, half = owners // 4, d_x.shape[1], d_zo.shape[1]
    bits = [1 << i for i in range(owners.bit_length() - 1)]
    channels = smalls[1].shape[1]
    vmem = pl.BlockSpec(memory_space=pltpu.VMEM)
    dma = pltpu.SemaphoreType.DMA
    piece = (own // 2, columns)
    steps = len(bits) + 1
    low = lambda *dims: pltpu.VMEM(dims + piece, bf16)
    return pl.pallas_call(
        functools.partial(finish_kernel, line, bits),
        in_specs=[vmem] * 10,
        out_specs=[vmem] * 3,
        out_shape=[
            jax.ShapeDtypeStruct((8, channels), f32),
            jax.ShapeDtypeStruct((own, proj), f32),
            jax.ShapeDtypeStruct((2 * own, half), f32),
        ],
        scratch_shapes=[
            pltpu.VMEM((steps + 1, 8, channels), f32),
            pltpu.VMEM((steps, 8, channels), f32),
            low(line, 2, 2), low(line, 2, 2), low(line, 2), low(line, 2), low(line), low(line), low(line), low(), low(),
            dma((steps,)), dma((steps,)),
        ]
        + [dma((line,))] * 8
        + [dma((3,))],
        compiler_params=params(48 << 20, collective_id=0, has_side_effects=True),
        name="finish",
    )(*smalls, d_zo, zo_got, d_x.reshape(line, 2, 2, 2, own // 2, columns))


def finish_plain(smalls, d_zo, d_x, own, proj):
    cw, cb, ggain, skip, ngain, alog, dtb = (v.reshape(-1, 8, v.shape[1]).sum(1) for v in smalls)
    skip = jnp.pad(skip.reshape(1, -1, HEAD).sum(2), ((0, 0), (0, LANES - skip.shape[1] // HEAD)))
    tail = jnp.concatenate([ngain, alog, dtb, skip], axis=1)
    wide = lambda v: jnp.pad(v, ((0, 0), (0, cb.shape[1] - v.shape[1])))
    small = lax.psum(jnp.concatenate([cw, cb, wide(ggain), wide(tail)], axis=0), ("dp", "seq"))
    d_x = lax.psum_scatter(d_x, "dp", scatter_dimension=0, tiled=True)
    d_zo, d_x = lax.psum((d_zo.astype(f32), d_x.astype(f32)), "seq")
    d_in = jnp.concatenate([d_zo[:own], d_zo[own : 2 * own], d_x], axis=1)[:, :proj]
    return small, d_in, d_zo[2 * own :]


def per_device(
    sizes, tokens, segments, cotangent, norm_gain, weight_in, conv_weight, conv_bias, dt_bias, a_log, skip_d,
    gate_gain, weight_out,
):
    seqs, length, width = tokens.shape
    rows = seqs * length
    inner = gate_gain.shape[0]
    channels = conv_bias.shape[0]
    heads = dt_bias.shape[0]
    own = weight_in.shape[0]
    owners = width // own
    tok = tokens.reshape(rows, width)
    cot = cotangent.reshape(rows, width)
    pad = LANES - heads

    local_x = jnp.pad(weight_in[:, inner:], ((0, 0), (0, pad)))
    owned = sizes["dp"] % 4 == 0 and sizes["seq"] == 2
    wx = gather(local_x, owners) if owned else lax.all_gather(local_x, "dp", axis=0, tiled=True)
    wx, weight_out = lax.optimization_barrier((wx, weight_out))
    local_zo = jnp.concatenate([weight_in[:, :width], weight_in[:, width:inner], weight_out], axis=0)
    slab = lax.all_gather(local_zo, "dp", axis=0, tiled=True).reshape(owners, 4 * own, width)
    weights = slab_views(slab, own)

    head = jnp.pad(jnp.stack([dt_bias, -jnp.exp(a_log), skip_d]), ((0, 5), (0, pad)))
    seg = segments.astype(f32).reshape(rows // Q, Q)
    cb = conv_bias.reshape(1, channels)
    ngain = norm_gain.reshape(1, width)
    ggain = gate_gain.reshape(1, inner)

    normed, xbc, dt = project(tok, ngain, wx, channels)
    y, s, sin = state_forward(seg, xbc, dt, conv_weight, cb, head, inner, seqs)
    gn, out, gz, gm, p_ggain = gate(tok, normed, y, cot, weights, ggain)
    d_z = dot(normed, gz, TN).astype(bf16)
    d_out = dot(gn, cot, TN).astype(bf16)
    d_zo = jnp.concatenate(
        [
            d_z[:, :width].reshape(owners, own, width),
            d_z[:, width:].reshape(owners, own, width),
            d_out.reshape(owners, 2 * own, width),
        ],
        axis=1,
    ).reshape(owners * 4 * own, width)
    d_zo, gm = lax.optimization_barrier((d_zo, gm))
    d_zo = lax.psum_scatter(d_zo, "dp", scatter_dimension=0, tiled=True)
    gx, p_cw, p_cb, p_skip, p_alog, p_dtb = state_backward(seg, xbc, dt, s, sin, gm, conv_weight, head, seqs)
    d_x = dot(normed, gx, TN).astype(bf16)
    g_tok, p_ngain = token_grad(tok, cot, gz, gx, weights[:2], wx, ngain)
    smalls = (p_cw, p_cb, p_ggain, p_skip, p_ngain, p_alog, p_dtb)
    if owned:
        zo_got = lax.ppermute(d_zo, "seq", [(0, 1), (1, 0)])
        small, d_in, d_out = finish(smalls, d_zo, zo_got, d_x, own, weight_in.shape[1])
    else:
        small, d_in, d_out = finish_plain(smalls, d_zo, d_x, own, weight_in.shape[1])
    return (
        out.reshape(tokens.shape),
        g_tok.reshape(tokens.shape),
        small[6, :width],
        d_in,
        small[:4],
        small[4],
        small[6, width + LANES : width + LANES + heads],
        small[6, width : width + heads],
        small[6, width + 2 * LANES : width + 2 * LANES + heads],
        small[5, :inner],
        d_out,
    )


def solution(mesh):
    data = P(("dp", "seq"), None, None)
    owned = P("dp", None)
    placed = (data, P(("dp", "seq"), None), data, P(), owned, P(), P(), P(), P(), P(), P(), owned)
    return jax.shard_map(
        functools.partial(per_device, dict(mesh.shape)),
        mesh=mesh,
        in_specs=placed,
        out_specs=(data, data, P(), owned, P(), P(), P(), P(), P(), P(), owned),
        check_vma=False,
    )
```

```python
import functools
import math

import jax
import jax.numpy as jnp
from jax import lax
from jax.experimental import pallas as pl
from jax.experimental.pallas import tpu as pltpu
from jax.sharding import PartitionSpec as P

f32 = jnp.float32
bf16 = jnp.bfloat16
HEAD = 64
Q = 128
LANES = 128
EPS = 1e-05
LOG2E = math.log2(math.e)
NEG = -1e30

NN = (((1,), (0,)), ((), ()))
NT = (((1,), (1,)), ((), ()))
TN = (((0,), (0,)), ((), ()))


def dot(a, b, dims=NN):
    return lax.dot_general(a, b, dims, preferred_element_type=f32)


def pair_split(v):
    return jnp.concatenate(split(v, 2), axis=1)


def twice(v, axis):
    return jnp.concatenate([v, v], axis=axis)


def dot_split(a, b):
    low = b[1]
    return dot(jnp.concatenate(a, axis=1), twice(b[0], 1), NT) + dot(a[0], low, NT)


def sigmoid(v):
    return 0.5 + 0.5 * jnp.tanh(0.5 * v)


def split(v, parts):
    out = []
    for _ in range(parts):
        low = v.astype(bf16)
        out.append(low)
        v = v - low.astype(f32)
    return out


def fold_rows(v):
    return jnp.sum(v.reshape(v.shape[0] // 8, 8, v.shape[1]), axis=0)


def wide(v, width):
    col = jnp.broadcast_to(v, (v.shape[0], LANES))
    return jnp.concatenate([col] * (width // LANES), axis=1)


def params(limit=None, **more):
    return pltpu.CompilerParams(vmem_limit_bytes=limit, **more)


def proj_kernel(tok_ref, gain_ref, wx_ref, normed_ref, xbc_ref, dt_ref):
    u = tok_ref[...].astype(f32)
    r = lax.rsqrt(jnp.mean(u * u, axis=-1, keepdims=True) + EPS)
    normed = (u * r * gain_ref[...]).astype(bf16)
    normed_ref[...] = normed
    out = dot(normed, wx_ref[...])
    ch = xbc_ref.shape[1]
    xbc_ref[...] = out[:, :ch]
    dt_ref[...] = out[:, ch:]


def project(tok, gain, wx, channels, tile=256):
    rows, width = tok.shape
    cols = wx.shape[1]
    return pl.pallas_call(
        proj_kernel,
        grid=(rows // tile,),
        in_specs=[
            pl.BlockSpec((tile, width), lambda i: (i, 0)),
            pl.BlockSpec((1, width), lambda i: (0, 0)),
            pl.BlockSpec((width, cols), lambda i: (0, 0)),
        ],
        out_specs=[
            pl.BlockSpec((tile, width), lambda i: (i, 0)),
            pl.BlockSpec((tile, channels), lambda i: (i, 0)),
            pl.BlockSpec((tile, cols - channels), lambda i: (i, 0)),
        ],
        out_shape=[
            jax.ShapeDtypeStruct((rows, width), bf16),
            jax.ShapeDtypeStruct((rows, channels), f32),
            jax.ShapeDtypeStruct((rows, cols - channels), f32),
        ],
        compiler_params=params(60 << 20),
        name="project",
    )(tok, gain, wx)


def segment_rows(seg_ref, block, blocks, at):
    rows = seg_ref.shape[0]
    none = jnp.full((1, LANES), -1.0, f32)
    seg = seg_ref[pl.ds(at, 1), :]
    prev = jnp.where(block > 0, seg_ref[pl.ds(jnp.maximum(at - 1, 0), 1), :], none)
    after = jnp.where(block < blocks - 1, seg_ref[pl.ds(jnp.minimum(at + 1, rows - 1), 1), :], none)
    lane = lax.broadcasted_iota(jnp.int32, (1, LANES), 1)

    def same(other):
        return (other == seg).astype(f32)

    out = [seg]
    for k in (1, 2, 3):
        out.append(same(jnp.where(lane < k, pltpu.roll(prev, k, 1), pltpu.roll(seg, k, 1))))
    out.append(same(jnp.broadcast_to(prev[:, LANES - 1 :], (1, LANES))))
    out.append(same(jnp.broadcast_to(seg[:, LANES - 1 :], (1, LANES))))
    for k in (1, 2, 3):
        turn = LANES - k
        out.append(same(jnp.where(lane >= turn, pltpu.roll(after, turn, 1), pltpu.roll(seg, turn, 1))))
    tab = jnp.concatenate(out + [none] * (16 - len(out)), axis=0)
    return seg, jnp.concatenate([tab] * (LANES // 16), axis=0).T


def iota(shape, axis):
    return lax.broadcasted_iota(jnp.int32, shape, axis)


def ones_where(cond):
    return jnp.where(cond, 1.0, 0.0).astype(bf16)


def head_columns(heads_wide, inner, width):
    return ones_where(iota((heads_wide, inner), 0) % LANES == iota((heads_wide, inner), 1) // width)


def step_terms(dt, dtb, na2, tri, cols):
    raw = dt + dtb
    ts = jnp.maximum(raw, 0.0) + jnp.log1p(jnp.exp(-jnp.abs(raw)))
    cum = dot(jnp.concatenate([tri] * 3, axis=1), jnp.concatenate(split(ts * na2, 3), axis=0))
    start = jnp.exp2(cum) * wide(cols[:, 4:5], LANES)
    end = jnp.exp2(cum[Q - 1 : Q, :] - cum) * wide(cols[:, 5:6], LANES)
    return raw, ts, cum, start, end


def head_terms(head_ref):
    rate = head_ref[1:2, :]
    return head_ref[0:1, :], rate, rate * LOG2E


def fill_constants(e_ref, tri_ref, skip_ref, head_ref):
    inner = e_ref.shape[1]
    e_ref[...] = head_columns(e_ref.shape[0], inner, HEAD)
    tri_ref[...] = ones_where(iota((Q, Q), 0) >= iota((Q, Q), 1))
    skip = jnp.broadcast_to(head_ref[2:3, :], (8, LANES))
    wide_skip = dot(jnp.concatenate(split(skip, 3), axis=1), head_columns(3 * LANES, inner, HEAD))
    skip_ref[...] = wide_skip[0:1]


def expand_operand(*terms):
    return jnp.concatenate([jnp.concatenate(split(t, 2), axis=1) for t in terms], axis=0)


def by_head(v, left):
    zero = jnp.zeros_like(v)
    return jnp.concatenate([jnp.where(left, v, zero), jnp.where(left, zero, v)], axis=0)


def later_rows(v, k):
    width = v.shape[1]
    v = pltpu.roll(v.reshape(-1, 8, width), 8 - k, 1)
    here = lax.broadcasted_iota(jnp.int32, (1, 8, width), 1) < 8 - k
    return jnp.where(here, v[:-1], v[1:]).reshape(-1, width)


def fwd_kernel(
    seg_ref, xbc_ref, dt_ref, cw_ref, cb_ref, head_ref,
    y_ref, s_ref, sin_ref, state, ext, e_ref, tri_ref, skip_ref,
):
    inner = y_ref.shape[1]
    channels = cb_ref.shape[1]
    b, blocks = pl.program_id(1), pl.num_programs(1)
    dtb, _, na2 = head_terms(head_ref)

    @pl.when((b == 0) & (pl.program_id(0) == 0))
    def _():
        fill_constants(e_ref, tri_ref, skip_ref, head_ref)

    @pl.when(b == 0)
    def _():
        state[...] = jnp.zeros_like(state)
        ext[0:8, :] = jnp.zeros((8, channels), f32)

    @pl.when(b > 0)
    def _():
        ext[0:8, :] = ext[Q : Q + 8, :]

    ext[8 : 8 + Q, :] = xbc_ref[...]
    seg, cols = segment_rows(seg_ref, b, blocks, pl.program_id(0) * blocks + b)
    m1, m2, m3 = (wide(cols[:, k : k + 1], 256) for k in (1, 2, 3))

    def conv(c):
        at = pl.ds(c, 256)
        x = ext[:, at]
        s = cb_ref[:, at] + cw_ref[3:4, at] * x[8:]
        s += m1 * (cw_ref[2:3, at] * later_rows(x, 7))
        s += m2 * (cw_ref[1:2, at] * later_rows(x, 6))
        s += m3 * (cw_ref[0:1, at] * later_rows(x, 5))
        s_ref[:, at] = s
        return s * sigmoid(s)

    bc, bc_rest = split(conv(inner), 2)
    bm, cm = bc[:, :LANES], bc[:, LANES:]
    bt = bm.T
    c_two = jnp.concatenate([cm, bc_rest[:, LANES:]], axis=1)
    _, ts, cum, start, end = step_terms(dt_ref[...], dtb, na2, tri_ref[...], cols)
    cum_t = cum.T
    grow = expand_operand(start, end, ts)
    row_i = lax.broadcasted_iota(jnp.int32, (Q, Q), 0)
    col_j = lax.broadcasted_iota(jnp.int32, (Q, Q), 1)
    same = wide(cols[:, 0:1], LANES) == seg
    mask = jnp.where(same & (row_i >= col_j), 0.0, NEG)
    scores = dot_split((cm, bc_rest[:, LANES:]), (bm, bc_rest[:, :LANES]))
    left = col_j < HEAD

    for c in range(0, inner, 256):
        at = pl.ds(c, 256)
        x = conv(c)
        big = dot(grow, e_ref[:, at])
        s_e, e_e, t_e = big[:Q], big[Q : 2 * Q], big[2 * Q :]
        xs = x * t_e
        xs_low = xs.astype(bf16)
        st = state[:, at]
        st_low = st.astype(bf16)
        sin_ref[:, at] = st_low
        carried = dot(c_two, twice(st_low, 0))
        parts = []
        for p in range(2):
            mats = []
            for h in range(2):
                head = (c + p * LANES) // HEAD + h
                gap = wide(cum[:, head : head + 1], LANES) - cum_t[head : head + 1, :] + mask
                mats.append((jnp.exp2(gap) * scores).astype(bf16))
            xp = xs_low[:, p * LANES : (p + 1) * LANES]
            parts.append(dot(jnp.concatenate(mats, axis=1), by_head(xp, left)))
        y = jnp.concatenate(parts, axis=1) + s_e * carried + skip_ref[:, at] * x
        y_ref[:, at] = y
        state[:, at] = st * s_e[Q - 1 : Q, :] + dot(bt, (xs * e_e).astype(bf16))


def fixed(shape):
    return pl.BlockSpec(shape, lambda *_: (0,) * len(shape))


def state_forward(seg, xbc, dt, cw, cb, head, inner, seqs):
    rows, channels = xbc.shape
    blocks = rows // seqs // Q
    at = lambda s, b: (s * blocks + b, 0)
    at3 = lambda s, b: (s * blocks + b, 0, 0)
    return pl.pallas_call(
        fwd_kernel,
        grid=(seqs, blocks),
        in_specs=[
            fixed(seg.shape),
            pl.BlockSpec((Q, channels), at),
            pl.BlockSpec((Q, LANES), at),
            fixed(cw.shape), fixed(cb.shape), fixed(head.shape),
        ],
        out_specs=[
            pl.BlockSpec((Q, inner), at),
            pl.BlockSpec((Q, channels), at),
            pl.BlockSpec((None, LANES, inner), at3),
        ],
        out_shape=[
            jax.ShapeDtypeStruct((rows, inner), f32),
            jax.ShapeDtypeStruct((rows, channels), f32),
            jax.ShapeDtypeStruct((seqs * blocks, LANES, inner), bf16),
        ],
        scratch_shapes=[
            pltpu.VMEM((LANES, inner), f32),
            pltpu.VMEM((Q + 8, channels), f32),
            pltpu.VMEM((2 * LANES, inner), bf16),
            pltpu.VMEM((Q, Q), bf16),
            pltpu.VMEM((1, inner), f32),
        ],
        compiler_params=params(60 << 20),
        name="state_forward",
    )(seg, xbc, dt, cw, cb, head)


def flat(ref):
    v = ref[...]
    return v.reshape(v.shape[0] * v.shape[1], v.shape[2])


def slab_views(slab, own):
    owners, _, width = slab.shape
    if own % 16 == 0:
        first = lambda *_: (0, 0, 0)
        second = lambda *_: (0, 1, 0)
        sizes = ((own, first), (own, second), (2 * own, second))
        return [(slab, pl.BlockSpec((owners, n, width), index)) for n, index in sizes]
    parts = [
        v.reshape(1, -1, width) for v in (slab[:, :own], slab[:, own : 2 * own], slab[:, 2 * own :])
    ]
    return [(v, fixed(v.shape)) for v in parts]


def gate_kernel(
    tok_ref, normed_ref, y_ref, cot_ref, wa_ref, wb_ref, wo_ref, gain_ref,
    gn_ref, out_ref, gz_ref, gm_ref, ggain_ref,
):
    wa, wb, wo = flat(wa_ref), flat(wb_ref), flat(wo_ref)
    gain = gain_ref[...]

    @pl.when(pl.program_id(0) == 0)
    def _():
        ggain_ref[...] = jnp.zeros_like(ggain_ref)

    normed = normed_ref[...]
    z = jnp.concatenate([dot(normed, wa), dot(normed, wb)], axis=1)
    g_gn = dot(cot_ref[...], wo, NT)
    sg = sigmoid(z)
    sz = z * sg
    y = y_ref[...]
    gated = y * sz
    rstd = lax.rsqrt(jnp.mean(gated * gated, axis=-1, keepdims=True) + EPS)
    unit = gated * rstd
    gn = (unit * gain).astype(bf16)
    gn_ref[...] = gn
    out_ref[...] = (tok_ref[...].astype(f32) + dot(gn, wo)).astype(bf16)
    ggain_ref[...] += fold_rows(unit * g_gn)
    q = g_gn * gain
    mean = jnp.mean(unit * q, axis=-1, keepdims=True)
    g_gated = rstd * (q - unit * mean)
    gm_ref[...] = g_gated * sz
    gz_ref[...] = (g_gated * y * (sg * (1.0 + z * (1.0 - sg)))).astype(bf16)


def gate(tok, normed, y, cot, weights, gain, tile=256):
    rows, width = tok.shape
    inner = y.shape[1]
    at = lambda i: (i, 0)
    return pl.pallas_call(
        gate_kernel,
        grid=(rows // tile,),
        in_specs=[
            pl.BlockSpec((tile, width), at),
            pl.BlockSpec((tile, width), at),
            pl.BlockSpec((tile, inner), at),
            pl.BlockSpec((tile, width), at),
            *[spec for _, spec in weights], fixed(gain.shape),
        ],
        out_specs=[
            pl.BlockSpec((tile, inner), at),
            pl.BlockSpec((tile, width), at),
            pl.BlockSpec((tile, inner), at),
            pl.BlockSpec((tile, inner), at),
            fixed((8, inner)),
        ],
        out_shape=[
            jax.ShapeDtypeStruct((rows, inner), bf16),
            jax.ShapeDtypeStruct((rows, width), bf16),
            jax.ShapeDtypeStruct((rows, inner), bf16),
            jax.ShapeDtypeStruct((rows, inner), f32),
            jax.ShapeDtypeStruct((8, inner), f32),
        ],
        compiler_params=params(60 << 20),
        name="gate",
    )(tok, normed, y, cot, *[v for v, _ in weights], gain)


def bwd_kernel(
    seg_ref, xbc_ref, dt_ref, s_ref, sin_ref, gm_ref, cw_ref, head_ref,
    gx_ref, gcw_ref, gcb_ref, gskip_ref, galog_ref, gdtb_ref,
    adj, gext, da_rows, spread, grad_b, grad_c, link, e_ref, tri_ref, skip_ref, et_ref, tail_ref, pair_ref,
):
    inner = gm_ref.shape[1]
    channels = s_ref.shape[1]
    b, blocks = pl.program_id(1), pl.num_programs(1)
    dtb, rate, na2 = head_terms(head_ref)

    @pl.when((b == 0) & (pl.program_id(0) == 0))
    def _():
        for ref in (gcw_ref, gcb_ref, gskip_ref, galog_ref, gdtb_ref, da_rows):
            ref[...] = jnp.zeros_like(ref)
        fill_constants(e_ref, tri_ref, skip_ref, head_ref)
        et_ref[...] = ones_where(iota((inner, LANES), 0) // HEAD == iota((inner, LANES), 1))
        turned = ones_where(iota((Q, Q), 0) <= iota((Q, Q), 1))
        below = ones_where(iota((Q, Q), 0) > iota((Q, Q), 1))
        tail_ref[...] = jnp.concatenate([turned, turned, below, below], axis=1)
        row, col = iota((2 * Q, 2 * Q), 0), iota((2 * Q, 2 * Q), 1)
        pair_ref[...] = ones_where((row // Q == col // Q) & (row >= col))

    @pl.when(b == 0)
    def _():
        adj[...] = jnp.zeros_like(adj)
        gext[Q : Q + 8, :] = jnp.zeros((8, channels), f32)

    @pl.when(b > 0)
    def _():
        gext[Q : Q + 8, :] = gext[0:8, :]

    turn = blocks - 1 - b
    seg, cols = segment_rows(seg_ref, turn, blocks, pl.program_id(0) * blocks + turn)
    raw, ts, cum, start, end = step_terms(dt_ref[...], dtb, na2, tri_ref[...], cols)
    cum_t = cum.T
    grow = expand_operand(start, end, ts)

    def act(c):
        s = s_ref[:, pl.ds(c, 256)]
        sg = sigmoid(s)
        return s * sg, sg * (1.0 + s * (1.0 - sg))

    bc, slope_bc = act(inner)
    bc, bc_rest = split(bc, 2)
    bm, cm = bc[:, :LANES], bc[:, LANES:]
    ct = cm.T
    b_two = jnp.concatenate([bm, bc_rest[:, :LANES]], axis=1)
    c_two = jnp.concatenate([cm, bc_rest[:, LANES:]], axis=1)
    row_j = lax.broadcasted_iota(jnp.int32, (Q, Q), 0)
    col_i = lax.broadcasted_iota(jnp.int32, (Q, Q), 1)
    same = wide(cols[:, 0:1], LANES) == seg
    mask = jnp.where(same & (col_i >= row_j), 0.0, NEG)
    before = (row_j < col_i).astype(f32)
    scores = dot_split((bm, bc_rest[:, :LANES]), (cm, bc_rest[:, LANES:]))
    left = col_i < HEAD
    grad_scores = jnp.zeros((Q, Q), f32)

    for c in range(0, inner, 256):
        at = pl.ds(c, 256)
        x, slope = act(c)
        big = dot(grow, e_ref[:, at])
        s_e, e_e, t_e = big[:Q], big[Q : 2 * Q], big[2 * Q :]
        xs = x * t_e
        xs_low, xs_rest = split(xs, 2)
        gm = gm_ref[:, at]
        gm_low, gm_rest = split(gm, 2)
        ad = adj[:, at]
        ad_low, ad_rest = split(ad, 2)
        st_low = sin_ref[:, at]
        into = dot(b_two, twice(ad_low, 0)) + dot(bm, ad_rest)
        carried = dot(c_two, twice(st_low, 0))
        parts = []
        for p in range(2):
            lanes = slice(p * LANES, (p + 1) * LANES)
            diag, diag_rest = by_head(gm_low[:, lanes], left), by_head(gm_rest[:, lanes], left)
            gmat = dot_split((xs_low[:, lanes], xs_rest[:, lanes]), (diag, diag_rest))
            mats, links = [], []
            for h in range(2):
                head = (c + p * LANES) // HEAD + h
                gap = cum_t[head : head + 1, :] - wide(cum[:, head : head + 1], LANES) + mask
                decay = jnp.exp2(gap)
                mat = decay * scores
                grad = gmat[:, h * LANES : (h + 1) * LANES]
                grad_scores += decay * grad
                mats.append(split(mat, 2))
                links.append((mat * grad).astype(bf16))
            high = jnp.concatenate([mats[0][0], mats[1][0]], axis=1)
            rest = jnp.concatenate([mats[0][1], mats[1][1]], axis=1)
            parts.append(dot(high, diag) + dot(high, diag_rest) + dot(rest, diag))
            reach = dot(jnp.concatenate(links, axis=1), pair_ref[...])
            for h in range(2):
                head = (c + p * LANES) // HEAD + h
                da_rows[head : head + 1, :] = jnp.sum(
                    reach[:, h * LANES : (h + 1) * LANES] * before, axis=0, keepdims=True
                )
        g_xs = jnp.concatenate(parts, axis=1) + e_e * into
        gext[0:Q, at] = (t_e * g_xs + skip_ref[:, at] * gm) * slope
        sums = jnp.concatenate(
            [pair_split(carried * gm), pair_split(x * into), pair_split(x * g_xs)], axis=0
        )
        sums = dot(sums, twice(et_ref[at, :], 0))
        s_gm = (s_e * gm).astype(bf16)
        part_c = dot(s_gm, st_low, NT)
        part_b = dot((e_e * xs).astype(bf16), ad_low, NT)
        if c == 0:
            spread[...] = sums
            grad_c[...] = part_c
            grad_b[...] = part_b
        else:
            spread[...] += sums
            grad_c[...] += part_c
            grad_b[...] += part_b
        gskip_ref[:, at] += fold_rows(gm * x)
        link[:, at] = fold_rows(st_low.astype(f32) * ad)
        adj[:, at] = ad * s_e[Q - 1 : Q, :] + dot(ct, s_gm)

    grad_low = grad_scores.astype(bf16)
    g_b = grad_b[...] + dot(grad_low, cm)
    g_c = grad_c[...] + dot(grad_low, bm, TN)
    gext[0:Q, pl.ds(inner, 256)] = jnp.concatenate([g_b, g_c], axis=1) * slope_bc

    phi = start * spread[0:Q]
    psi = end * ts * spread[Q : 2 * Q]
    through = jnp.sum(dot(jnp.concatenate(split(link[...], 2), axis=0), et_ref[...]), axis=0, keepdims=True)
    around = jnp.concatenate(split(phi, 2) + split(psi, 2), axis=0)
    da = da_rows[...].T + dot(tail_ref[...], around) + start[Q - 1 : Q, :] * through
    g_ts = spread[2 * Q :] + rate * da
    galog_ref[...] += fold_rows(ts * rate * da)
    g_dt = g_ts * sigmoid(raw)
    gdtb_ref[...] += fold_rows(g_dt)

    n1, n2, n3 = (wide(cols[:, k : k + 1], 256) for k in (6, 7, 8))
    for c in range(0, channels, 256):
        at = pl.ds(c, 256)
        x = xbc_ref[:, at]
        g = gext[:, at]
        g0 = g[:Q]
        g1 = later_rows(g, 1) * n1
        g2 = later_rows(g, 2) * n2
        g3 = later_rows(g, 3) * n3
        gx = cw_ref[3:4, at] * g0 + cw_ref[2:3, at] * g1 + cw_ref[1:2, at] * g2 + cw_ref[0:1, at] * g3
        gx_ref[:, at] = gx.astype(bf16)
        gcb_ref[:, at] += fold_rows(g0)
        gcw_ref[24:32, at] += fold_rows(g0 * x)
        gcw_ref[16:24, at] += fold_rows(g1 * x)
        gcw_ref[8:16, at] += fold_rows(g2 * x)
        gcw_ref[0:8, at] += fold_rows(g3 * x)
    gx_ref[:, channels:] = g_dt.astype(bf16)


def state_backward(seg, xbc, dt, s, sin, gm, cw, head, seqs):
    rows, channels = xbc.shape
    inner = gm.shape[1]
    blocks = rows // seqs // Q
    at = lambda s, b: (s * blocks + blocks - 1 - b, 0)
    at3 = lambda s, b: (s * blocks + blocks - 1 - b, 0, 0)
    return pl.pallas_call(
        bwd_kernel,
        grid=(seqs, blocks),
        in_specs=[
            fixed(seg.shape),
            pl.BlockSpec((Q, channels), at),
            pl.BlockSpec((Q, LANES), at),
            pl.BlockSpec((Q, channels), at),
            pl.BlockSpec((None, LANES, inner), at3),
            pl.BlockSpec((Q, inner), at),
        ]
        + [fixed(v.shape) for v in (cw, head)],
        out_specs=[
            pl.BlockSpec((Q, channels + LANES), at),
            fixed((32, channels)), fixed((8, channels)), fixed((8, inner)), fixed((8, LANES)), fixed((8, LANES)),
        ],
        out_shape=[
            jax.ShapeDtypeStruct((rows, channels + LANES), bf16),
            jax.ShapeDtypeStruct((32, channels), f32),
            jax.ShapeDtypeStruct((8, channels), f32),
            jax.ShapeDtypeStruct((8, inner), f32),
            jax.ShapeDtypeStruct((8, LANES), f32),
            jax.ShapeDtypeStruct((8, LANES), f32),
        ],
        scratch_shapes=[
            pltpu.VMEM((LANES, inner), f32),
            pltpu.VMEM((Q + 8, channels), f32),
            pltpu.VMEM((LANES, LANES), f32),
            pltpu.VMEM((3 * Q, LANES), f32),
            pltpu.VMEM((Q, LANES), f32),
            pltpu.VMEM((Q, LANES), f32),
            pltpu.VMEM((8, inner), f32),
            pltpu.VMEM((2 * LANES, inner), bf16),
            pltpu.VMEM((Q, Q), bf16),
            pltpu.VMEM((1, inner), f32),
            pltpu.VMEM((inner, LANES), bf16),
            pltpu.VMEM((Q, 4 * Q), bf16),
            pltpu.VMEM((2 * Q, 2 * Q), bf16),
        ],
        compiler_params=params(60 << 20),
        name="state_backward",
    )(seg, xbc, dt, s, sin, gm, cw, head)


def token_kernel(tok_ref, cot_ref, gz_ref, gx_ref, wa_ref, wb_ref, wx_ref, gain_ref, out_ref, ggain_ref):
    half = gz_ref.shape[1] // 2
    g = dot(gz_ref[:, :half], flat(wa_ref), NT) + dot(gz_ref[:, half:], flat(wb_ref), NT)
    g += dot(gx_ref[...], wx_ref[...], NT)
    u = tok_ref[...].astype(f32)
    r = lax.rsqrt(jnp.mean(u * u, axis=-1, keepdims=True) + EPS)
    unit = u * r

    @pl.when(pl.program_id(0) == 0)
    def _():
        ggain_ref[...] = jnp.zeros_like(ggain_ref)

    ggain_ref[...] += fold_rows(unit * g)
    q = g * gain_ref[...]
    mean = jnp.mean(unit * q, axis=-1, keepdims=True)
    out_ref[...] = (cot_ref[...].astype(f32) + r * (q - unit * mean)).astype(bf16)


def token_grad(tok, cot, gz, gx, weights, wx, gain, tile=256):
    rows, width = tok.shape
    at = lambda i: (i, 0)
    return pl.pallas_call(
        token_kernel,
        grid=(rows // tile,),
        in_specs=[
            pl.BlockSpec((tile, width), at),
            pl.BlockSpec((tile, width), at),
            pl.BlockSpec((tile, gz.shape[1]), at),
            pl.BlockSpec((tile, gx.shape[1]), at),
            *[spec for _, spec in weights], fixed(wx.shape), fixed(gain.shape),
        ],
        out_specs=[pl.BlockSpec((tile, width), at), fixed((8, width))],
        out_shape=[jax.ShapeDtypeStruct((rows, width), bf16), jax.ShapeDtypeStruct((8, width), f32)],
        compiler_params=params(60 << 20),
        name="token_grad",
    )(tok, cot, gz, gx, *[v for v, _ in weights], wx, gain)


MESH = pl.DeviceIdType.MESH


def place(line):
    me = lax.axis_index("dp")
    index = lambda l, x, c: (l * 2 + x) * 2 + c
    return me // 4, (me // 2) % 2, me % 2, index, lax.axis_index("seq")


def meet(devices):
    barrier = pltpu.get_barrier_semaphore()
    for device in devices:
        pl.semaphore_signal(barrier, inc=1, device_id=device, device_id_type=MESH)
    pl.semaphore_wait(barrier, len(devices))


def remote(src, dst, send, recv, device):
    return pltpu.make_async_remote_copy(
        src_ref=src, dst_ref=dst, send_sem=send, recv_sem=recv, device_id=device, device_id_type=MESH
    )


def gather_kernel(line, own_ref, out_ref, line_send, x_send, y_send, core_send, recv, local):
    l, x, c, index, y = place(line)
    others = [{"dp": index((l + k) % line, x, c)} for k in range(1, line)]
    beside, sibling, across = {"dp": index(l, 1 - x, c)}, {"dp": index(l, x, 1 - c)}, {"seq": 1 - y}
    meet(others + [beside, sibling, across])
    started = []

    def send(src, at, sem, device):
        copy = remote(src, out_ref.at[at], sem, recv.at[at], device)
        copy.start()
        started.append(copy)

    def arrived(at):
        remote(out_ref.at[at], out_ref.at[at], local.at[1], recv.at[at], sibling).wait_recv()

    mine = pltpu.make_async_copy(own_ref, out_ref.at[l, x, c], local.at[0])
    mine.start()
    for k in range(1, line):
        send(own_ref.at[y], (l, x, c, y), line_send.at[k], others[k - 1])
    send(own_ref.at[y], (l, x, c, y), x_send.at[0], beside)
    for h in range(2):
        send(own_ref.at[h], (l, x, c, h), core_send.at[0, h], sibling)
    for k in range(1, line):
        at = ((l + k) % line, x, c, y)
        arrived(at)
        send(out_ref.at[at], at, x_send.at[k], beside)
        send(out_ref.at[at], at, y_send.at[k], across)
        send(out_ref.at[at], at, core_send.at[k, 0], sibling)
    for k in range(line):
        at = ((l + k) % line, 1 - x, c, y)
        arrived(at)
        send(out_ref.at[at], at, y_send.at[line + k], across)
        send(out_ref.at[at], at, core_send.at[line + k, 0], sibling)
    for k in range(1, line):
        at = ((l + k) % line, x, c, 1 - y)
        arrived(at)
        send(out_ref.at[at], at, core_send.at[k, 1], sibling)
    for k in range(line):
        at = ((l + k) % line, 1 - x, c, 1 - y)
        arrived(at)
        send(out_ref.at[at], at, core_send.at[line + k, 1], sibling)
    for k in range(line):
        for side in range(2):
            for h in range(2):
                arrived(((l + k) % line, side, 1 - c, h))
    for copy in started:
        copy.wait_send()
    mine.wait()


def gather(local, owners):
    own, columns = local.shape
    line = owners // 4
    vmem = pl.BlockSpec(memory_space=pltpu.VMEM)
    dma = pltpu.SemaphoreType.DMA
    out = pl.pallas_call(
        functools.partial(gather_kernel, line),
        in_specs=[vmem],
        out_specs=vmem,
        out_shape=jax.ShapeDtypeStruct((line, 2, 2, 2, own // 2, columns), local.dtype),
        scratch_shapes=[
            dma((line,)), dma((line,)), dma((2 * line,)), dma((2 * line, 2)), dma((line, 2, 2, 2)), dma((2,)),
        ],
        compiler_params=params(48 << 20, collective_id=1, has_side_effects=True),
        name="gather",
    )(local.reshape(2, own // 2, columns))
    return out.reshape(owners * own, columns)


def pack_small(acc, width, cw_ref, cb_ref, ggain_ref, skip_ref, alog_ref, dtb_ref):
    inner = ggain_ref.shape[1]
    total = lambda v: jnp.sum(v, axis=0, keepdims=True)
    acc[...] = jnp.zeros(acc.shape, f32)
    for k in range(4):
        acc[k : k + 1, :] = total(cw_ref[8 * k : 8 * k + 8, :])
    acc[4:5, :] = total(cb_ref[...])
    acc[5:6, :inner] = total(ggain_ref[...])
    acc[6:7, width : width + LANES] = total(alog_ref[...])
    acc[6:7, width + LANES : width + 2 * LANES] = total(dtb_ref[...])
    skip = jnp.concatenate(split(skip_ref[...], 3), axis=0)
    by_head = ones_where(iota((inner, LANES), 0) // HEAD == iota((inner, LANES), 1))
    acc[6:7, width + 2 * LANES : width + 3 * LANES] = total(dot(skip, by_head))


def finish_kernel(
    line, bits, tile, starts, own,
    cw_ref, cb_ref, ggain_ref, skip_ref, alog_ref, dtb_ref, zo_ref, zo_got_ref, d_ref, gain_ref,
    tok_ref, cot_ref, gz_ref, gx_ref, wa_ref, wb_ref, wx_ref,
    small_ref, din_ref, dout_ref, gtok_ref,
    acc, got, gain_acc, gain_got, core_got, one, two_got, two, three_got, three, line_got, last, last_got,
    tok, cot, gz, gx, wa, wb, wx, gtok, gain_rows,
    small_send, small_recv, gain_send, gain_recv, core_send, core_recv, two_send, two_recv,
    three_send, three_recv, line_send, line_recv, last_sem, tile_sem, out_sem, weight_sem,
):
    l, x, c, index, y = place(line)
    me = lax.axis_index("dp")
    doubling = [{"dp": me + bit - 2 * bit * ((me // bit) % 2)} for bit in bits]
    others = [{"dp": index((l + k) % line, x, c)} for k in range(1, line)]
    beside, sibling, across = {"dp": index(l, 1 - x, c)}, {"dp": index(l, x, 1 - c)}, {"seq": 1 - y}
    order = list(range(1, line)) + [0]
    at = [(l + k) % line for k in order]
    tiles = tok.shape[0]
    width = gain_ref.shape[1]

    def fetches(i):
        rows = pl.ds(pl.multiple_of(i * tile, tile), tile)
        pairs = ((tok_ref, tok), (cot_ref, cot), (gz_ref, gz), (gx_ref, gx))
        return [pltpu.make_async_copy(src.at[rows], dst.at[i], tile_sem.at[i, n]) for n, (src, dst) in enumerate(pairs)]

    def stored(i):
        rows = pl.ds(pl.multiple_of(i * tile, tile), tile)
        return pltpu.make_async_copy(gtok.at[i], gtok_ref.at[rows], out_sem.at[i])

    weights = [
        pltpu.make_async_copy(src.at[:, pl.ds(start, dst.shape[1])], dst, weight_sem.at[n])
        for n, (src, dst, start) in enumerate(((wa_ref, wa, starts[0]), (wb_ref, wb, starts[1])))
    ] + [pltpu.make_async_copy(wx_ref, wx, weight_sem.at[2])]
    for copy in weights:
        copy.start()
    for i in range(tiles):
        for copy in fetches(i):
            copy.start()

    meet(doubling + others + [beside, sibling, across])

    def plus(a, b):
        return a.astype(f32) + b.astype(f32)

    smalls = doubling + [across]

    def first(i):
        return remote(d_ref.at[at[i], :, 1 - c], core_got.at[i], core_send.at[i], core_recv.at[i], sibling)

    def second(i):
        src, device = (one.at[i, 1 - x], beside) if i % 2 == 0 else (one.at[i, :, 1 - y], across)
        return remote(src, two_got.at[i], two_send.at[i], two_recv.at[i], device)

    def third(i):
        src, device = (two.at[i, 1 - y], across) if i % 2 == 0 else (two.at[i, 1 - x], beside)
        return remote(src, three_got.at[i], three_send.at[i], three_recv.at[i], device)

    def fourth(i):
        return remote(three.at[i], line_got.at[l], line_send.at[i], line_recv.at[l], others[order[i] - 1])

    def small(k):
        return remote(acc.at[k], got.at[k], small_send.at[k], small_recv.at[k], smalls[k])

    def gains(k):
        return remote(gain_acc.at[k], gain_got.at[k], gain_send.at[k], gain_recv.at[k], smalls[k])

    def after_first(i):
        first(i).wait()
        for a in range(2):
            for h in range(2):
                one[i, a, h] = plus(d_ref[at[i], a, c, h], core_got[i, a, h]).astype(bf16)
        second(i).start()

    def after_second(i):
        second(i).wait()
        for j in range(2):
            kept = one[i, x, j] if i % 2 == 0 else one[i, j, y]
            two[i, j] = plus(kept, two_got[i, j]).astype(bf16)
        third(i).start()

    def after_third(i):
        third(i).wait()
        kept = two[i, y] if i % 2 == 0 else two[i, x]
        three[i] = plus(kept, three_got[i]).astype(bf16)
        if order[i] > 0:
            fourth(i).start()

    def after_small(k):
        small(k).wait()
        acc[k + 1] = acc[k] + got[k]
        if k + 1 < len(smalls):
            small(k + 1).start()

    plan = [[] for _ in range(tiles)]
    for i in range(line):
        plan[min(i * 2 // line, tiles - 1)].append((after_first, i))
    for i in range(line):
        plan[min(2 + i * 3 // line, tiles - 1)].append((after_second, i))
    for i in range(line):
        plan[min(4 + i * 4 // line, tiles - 1)].append((after_third, i))
    for k in range(len(smalls)):
        plan[min(k + 1, tiles - 1)].append((after_small, k))

    for i in range(line):
        first(i).start()
    pack_small(acc.at[0], width, cw_ref, cb_ref, ggain_ref, skip_ref, alog_ref, dtb_ref)
    small(0).start()
    gain_rows[...] = jnp.zeros_like(gain_rows)
    for copy in weights:
        copy.wait()
    half = zo_ref.shape[1]

    @pl.loop(0, tiles)
    def _(i):
        for t, work in enumerate(plan):
            if work:

                @pl.when(i == t)
                def _():
                    for step, n in work:
                        step(n)

        for copy in fetches(i):
            copy.wait()
        g = dot(gz[i, :, :half], flat(wa), NT) + dot(gz[i, :, half:], flat(wb), NT)
        g += dot(gx[i], wx[...], NT)
        u = tok[i].astype(f32)
        r = lax.rsqrt(jnp.mean(u * u, axis=-1, keepdims=True) + EPS)
        unit = u * r
        gain_rows[...] += fold_rows(unit * g)
        q = g * gain_ref[...]
        mean = jnp.mean(unit * q, axis=-1, keepdims=True)
        gtok[i] = (cot[i].astype(f32) + r * (q - unit * mean)).astype(bf16)
        stored(i).start()

    gain_acc[0] = jnp.sum(gain_rows[...], axis=0, keepdims=True)
    gains(0).start()
    total = three[line - 1].astype(f32)
    for k in range(1, line):
        at_k = (l + k) % line
        remote(three.at[0], line_got.at[at_k], last_sem.at[2], line_recv.at[at_k], sibling).wait_recv()
        total += line_got[at_k].astype(f32)
    last[...] = total.astype(bf16)
    final = remote(last, last_got, last_sem.at[0], last_sem.at[1], across)
    final.start()

    zo = plus(zo_ref[...], zo_got_ref[...])
    din_ref[:, :half] = zo[:own]
    din_ref[:, half : 2 * half] = zo[own : 2 * own]
    dout_ref[...] = zo[2 * own :]
    for k in range(len(smalls)):
        gains(k).wait()
        gain_acc[k + 1] = gain_acc[k] + gain_got[k]
        if k + 1 < len(smalls):
            gains(k + 1).start()
    small_ref[...] = acc[len(smalls)]
    small_ref[6:7, :width] = gain_acc[len(smalls)]

    for i in range(line):
        if order[i] > 0:
            fourth(i).wait_send()
    final.wait()
    left = din_ref.shape[1] - 2 * half
    kept, came = last[...].astype(f32), last_got[...].astype(f32)
    lower = (y == 0).astype(f32)
    din_ref[: own // 2, 2 * half :] = (kept * lower + came * (1.0 - lower))[:, :left]
    din_ref[own // 2 :, 2 * half :] = (came * lower + kept * (1.0 - lower))[:, :left]
    for i in range(tiles):
        stored(i).wait()


def finish(smalls, d_zo, zo_got, d_x, own, proj, gain, tok, cot, gz, gx, weights, wx, tile=256):
    owners = d_x.shape[0] // own
    line, columns, half = owners // 4, d_x.shape[1], d_zo.shape[1]
    bits = [1 << i for i in range(owners.bit_length() - 1)]
    channels = smalls[1].shape[1]
    rows, width = tok.shape
    tiles = rows // tile
    vmem = pl.BlockSpec(memory_space=pltpu.VMEM)
    away = pl.BlockSpec(memory_space=pl.ANY)
    dma = pltpu.SemaphoreType.DMA
    piece = (own // 2, columns)
    steps = len(bits) + 1
    low = lambda *dims: pltpu.VMEM(dims + piece, bf16)
    held = lambda *dims: pltpu.VMEM(dims, bf16)
    shared = own % 16 == 0
    arrays = [v for v, _ in weights]
    part = (owners, own, half) if shared else arrays[0].shape
    return pl.pallas_call(
        functools.partial(finish_kernel, line, bits, tile, (0, own) if shared else (0, 0), own),
        in_specs=[vmem] * 10 + [away] * 7,
        out_specs=[vmem] * 3 + [away],
        out_shape=[
            jax.ShapeDtypeStruct((8, channels), f32),
            jax.ShapeDtypeStruct((own, proj), f32),
            jax.ShapeDtypeStruct((2 * own, half), f32),
            jax.ShapeDtypeStruct((rows, width), bf16),
        ],
        scratch_shapes=[
            pltpu.VMEM((steps + 1, 8, channels), f32),
            pltpu.VMEM((steps, 8, channels), f32),
            pltpu.VMEM((steps + 1, 1, width), f32),
            pltpu.VMEM((steps, 1, width), f32),
            low(line, 2, 2), low(line, 2, 2), low(line, 2), low(line, 2), low(line), low(line), low(line), low(), low(),
            held(tiles, tile, width), held(tiles, tile, width), held(tiles, tile, gz.shape[1]),
            held(tiles, tile, columns), held(*part), held(*part), held(*wx.shape), held(tiles, tile, width),
            pltpu.VMEM((8, width), f32),
            dma((steps,)), dma((steps,)), dma((steps,)), dma((steps,)),
        ]
        + [dma((line,))] * 8
        + [dma((3,)), dma((tiles, 4)), dma((tiles,)), dma((3,))],
        compiler_params=params(64000 << 10, collective_id=0, has_side_effects=True),
        name="finish",
    )(
        *smalls, d_zo, zo_got, d_x.reshape(line, 2, 2, 2, own // 2, columns), gain, tok, cot, gz, gx, *arrays, wx
    )


def finish_plain(smalls, d_zo, d_x, own, proj):
    cw, cb, ggain, skip, alog, dtb, ngain = (v.reshape(-1, 8, v.shape[1]).sum(1) for v in smalls)
    skip = jnp.pad(skip.reshape(1, -1, HEAD).sum(2), ((0, 0), (0, LANES - skip.shape[1] // HEAD)))
    tail = jnp.concatenate([ngain, alog, dtb, skip], axis=1)
    wide = lambda v: jnp.pad(v, ((0, 0), (0, cb.shape[1] - v.shape[1])))
    small = lax.psum(jnp.concatenate([cw, cb, wide(ggain), wide(tail)], axis=0), ("dp", "seq"))
    d_x = lax.psum_scatter(d_x, "dp", scatter_dimension=0, tiled=True)
    d_zo, d_x = lax.psum((d_zo.astype(f32), d_x.astype(f32)), "seq")
    d_in = jnp.concatenate([d_zo[:own], d_zo[own : 2 * own], d_x], axis=1)[:, :proj]
    return small, d_in, d_zo[2 * own :]


def per_device(
    sizes, tokens, segments, cotangent, norm_gain, weight_in, conv_weight, conv_bias, dt_bias, a_log, skip_d,
    gate_gain, weight_out,
):
    seqs, length, width = tokens.shape
    rows = seqs * length
    inner = gate_gain.shape[0]
    channels = conv_bias.shape[0]
    heads = dt_bias.shape[0]
    own = weight_in.shape[0]
    owners = width // own
    tok = tokens.reshape(rows, width)
    cot = cotangent.reshape(rows, width)
    pad = LANES - heads

    local_x = jnp.pad(weight_in[:, inner:], ((0, 0), (0, pad)))
    owned = sizes["dp"] % 4 == 0 and sizes["seq"] == 2
    wx = gather(local_x, owners) if owned else lax.all_gather(local_x, "dp", axis=0, tiled=True)
    wx, weight_out = lax.optimization_barrier((wx, weight_out))
    local_zo = jnp.concatenate([weight_in[:, :width], weight_in[:, width:inner], weight_out], axis=0)
    slab = lax.all_gather(local_zo, "dp", axis=0, tiled=True).reshape(owners, 4 * own, width)
    weights = slab_views(slab, own)

    head = jnp.pad(jnp.stack([dt_bias, -jnp.exp(a_log), skip_d]), ((0, 5), (0, pad)))
    seg = segments.astype(f32).reshape(rows // Q, Q)
    cb = conv_bias.reshape(1, channels)
    ngain = norm_gain.reshape(1, width)
    ggain = gate_gain.reshape(1, inner)

    normed, xbc, dt = project(tok, ngain, wx, channels)
    y, s, sin = state_forward(seg, xbc, dt, conv_weight, cb, head, inner, seqs)
    gn, out, gz, gm, p_ggain = gate(tok, normed, y, cot, weights, ggain)
    d_z = dot(normed, gz, TN).astype(bf16)
    d_out = dot(gn, cot, TN).astype(bf16)
    d_zo = jnp.concatenate(
        [
            d_z[:, :width].reshape(owners, own, width),
            d_z[:, width:].reshape(owners, own, width),
            d_out.reshape(owners, 2 * own, width),
        ],
        axis=1,
    ).reshape(owners * 4 * own, width)
    d_zo, gm = lax.optimization_barrier((d_zo, gm))
    d_zo = lax.psum_scatter(d_zo, "dp", scatter_dimension=0, tiled=True)
    gx, p_cw, p_cb, p_skip, p_alog, p_dtb = state_backward(seg, xbc, dt, s, sin, gm, conv_weight, head, seqs)
    d_x = dot(normed, gx, TN).astype(bf16)
    smalls = (p_cw, p_cb, p_ggain, p_skip, p_alog, p_dtb)
    if owned:
        zo_got = lax.ppermute(d_zo, "seq", [(0, 1), (1, 0)])
        small, d_in, d_out, g_tok = finish(
            smalls, d_zo, zo_got, d_x, own, weight_in.shape[1], ngain, tok, cot, gz, gx, weights[:2], wx
        )
    else:
        g_tok, p_ngain = token_grad(tok, cot, gz, gx, weights[:2], wx, ngain)
        small, d_in, d_out = finish_plain(smalls + (p_ngain,), d_zo, d_x, own, weight_in.shape[1])
    return (
        out.reshape(tokens.shape),
        g_tok.reshape(tokens.shape),
        small[6, :width],
        d_in,
        small[:4],
        small[4],
        small[6, width + LANES : width + LANES + heads],
        small[6, width : width + heads],
        small[6, width + 2 * LANES : width + 2 * LANES + heads],
        small[5, :inner],
        d_out,
    )


def solution(mesh):
    data = P(("dp", "seq"), None, None)
    owned = P("dp", None)
    placed = (data, P(("dp", "seq"), None), data, P(), owned, P(), P(), P(), P(), P(), P(), owned)
    return jax.shard_map(
        functools.partial(per_device, dict(mesh.shape)),
        mesh=mesh,
        in_specs=placed,
        out_specs=(data, data, P(), owned, P(), P(), P(), P(), P(), P(), owned),
        check_vma=False,
    )
```

```python
import functools
import math

import jax
import jax.numpy as jnp
from jax import lax
from jax.experimental import pallas as pl
from jax.experimental.pallas import tpu as pltpu
from jax.sharding import PartitionSpec as P

f32 = jnp.float32
bf16 = jnp.bfloat16
HEAD = 64
Q = 128
LANES = 128
EPS = 1e-05
LOG2E = math.log2(math.e)
NEG = -1e30

NN = (((1,), (0,)), ((), ()))
NT = (((1,), (1,)), ((), ()))
TN = (((0,), (0,)), ((), ()))


def dot(a, b, dims=NN):
    return lax.dot_general(a, b, dims, preferred_element_type=f32)


def pair_split(v):
    return jnp.concatenate(split(v, 2), axis=1)


def twice(v, axis):
    return jnp.concatenate([v, v], axis=axis)


def dot_split(a, b):
    low = b[1]
    return dot(jnp.concatenate(a, axis=1), twice(b[0], 1), NT) + dot(a[0], low, NT)


def sigmoid(v):
    return 0.5 + 0.5 * jnp.tanh(0.5 * v)


def split(v, parts):
    out = []
    for _ in range(parts):
        low = v.astype(bf16)
        out.append(low)
        v = v - low.astype(f32)
    return out


def fold_rows(v):
    return jnp.sum(v.reshape(v.shape[0] // 8, 8, v.shape[1]), axis=0)


def wide(v, width):
    col = jnp.broadcast_to(v, (v.shape[0], LANES))
    return jnp.concatenate([col] * (width // LANES), axis=1)


def params(limit=None, **more):
    return pltpu.CompilerParams(vmem_limit_bytes=limit, **more)


def proj_kernel(tok_ref, gain_ref, wx_ref, normed_ref, xbc_ref, dt_ref):
    u = tok_ref[...].astype(f32)
    r = lax.rsqrt(jnp.mean(u * u, axis=-1, keepdims=True) + EPS)
    normed = (u * r * gain_ref[...]).astype(bf16)
    normed_ref[...] = normed
    out = dot(normed, wx_ref[...])
    ch = xbc_ref.shape[1]
    xbc_ref[...] = out[:, :ch]
    dt_ref[...] = out[:, ch:]


def project(tok, gain, wx, channels, tile=256):
    rows, width = tok.shape
    cols = wx.shape[1]
    return pl.pallas_call(
        proj_kernel,
        grid=(rows // tile,),
        in_specs=[
            pl.BlockSpec((tile, width), lambda i: (i, 0)),
            pl.BlockSpec((1, width), lambda i: (0, 0)),
            pl.BlockSpec((width, cols), lambda i: (0, 0)),
        ],
        out_specs=[
            pl.BlockSpec((tile, width), lambda i: (i, 0)),
            pl.BlockSpec((tile, channels), lambda i: (i, 0)),
            pl.BlockSpec((tile, cols - channels), lambda i: (i, 0)),
        ],
        out_shape=[
            jax.ShapeDtypeStruct((rows, width), bf16),
            jax.ShapeDtypeStruct((rows, channels), f32),
            jax.ShapeDtypeStruct((rows, cols - channels), f32),
        ],
        compiler_params=params(60 << 20),
        name="project",
    )(tok, gain, wx)


def segment_rows(seg_ref, block, blocks, at):
    rows = seg_ref.shape[0]
    none = jnp.full((1, LANES), -1.0, f32)
    seg = seg_ref[pl.ds(at, 1), :]
    prev = jnp.where(block > 0, seg_ref[pl.ds(jnp.maximum(at - 1, 0), 1), :], none)
    after = jnp.where(block < blocks - 1, seg_ref[pl.ds(jnp.minimum(at + 1, rows - 1), 1), :], none)
    lane = lax.broadcasted_iota(jnp.int32, (1, LANES), 1)

    def same(other):
        return (other == seg).astype(f32)

    out = [seg]
    for k in (1, 2, 3):
        out.append(same(jnp.where(lane < k, pltpu.roll(prev, k, 1), pltpu.roll(seg, k, 1))))
    out.append(same(jnp.broadcast_to(prev[:, LANES - 1 :], (1, LANES))))
    out.append(same(jnp.broadcast_to(seg[:, LANES - 1 :], (1, LANES))))
    for k in (1, 2, 3):
        turn = LANES - k
        out.append(same(jnp.where(lane >= turn, pltpu.roll(after, turn, 1), pltpu.roll(seg, turn, 1))))
    tab = jnp.concatenate(out + [none] * (16 - len(out)), axis=0)
    return seg, jnp.concatenate([tab] * (LANES // 16), axis=0).T


def iota(shape, axis):
    return lax.broadcasted_iota(jnp.int32, shape, axis)


def ones_where(cond):
    return jnp.where(cond, 1.0, 0.0).astype(bf16)


def head_columns(heads_wide, inner, width):
    return ones_where(iota((heads_wide, inner), 0) % LANES == iota((heads_wide, inner), 1) // width)


def step_terms(dt, dtb, na2, tri, cols):
    raw = dt + dtb
    ts = jnp.maximum(raw, 0.0) + jnp.log1p(jnp.exp(-jnp.abs(raw)))
    cum = dot(jnp.concatenate([tri] * 3, axis=1), jnp.concatenate(split(ts * na2, 3), axis=0))
    start = jnp.exp2(cum) * wide(cols[:, 4:5], LANES)
    end = jnp.exp2(cum[Q - 1 : Q, :] - cum) * wide(cols[:, 5:6], LANES)
    return raw, ts, cum, start, end


def head_terms(head_ref):
    rate = head_ref[1:2, :]
    return head_ref[0:1, :], rate, rate * LOG2E


def fill_constants(e_ref, tri_ref, skip_ref, head_ref):
    inner = e_ref.shape[1]
    e_ref[...] = head_columns(e_ref.shape[0], inner, HEAD)
    tri_ref[...] = ones_where(iota((Q, Q), 0) >= iota((Q, Q), 1))
    skip = jnp.broadcast_to(head_ref[2:3, :], (8, LANES))
    wide_skip = dot(jnp.concatenate(split(skip, 3), axis=1), head_columns(3 * LANES, inner, HEAD))
    skip_ref[...] = wide_skip[0:1]


def expand_operand(*terms):
    return jnp.concatenate([jnp.concatenate(split(t, 2), axis=1) for t in terms], axis=0)


def by_head(v, left):
    zero = jnp.zeros_like(v)
    return jnp.concatenate([jnp.where(left, v, zero), jnp.where(left, zero, v)], axis=0)


def later_rows(v, k):
    width = v.shape[1]
    v = pltpu.roll(v.reshape(-1, 8, width), 8 - k, 1)
    here = lax.broadcasted_iota(jnp.int32, (1, 8, width), 1) < 8 - k
    return jnp.where(here, v[:-1], v[1:]).reshape(-1, width)


def fwd_kernel(
    seg_ref, xbc_ref, dt_ref, cw_ref, cb_ref, head_ref,
    y_ref, s_ref, sin_ref, state, ext, e_ref, tri_ref, skip_ref,
):
    seqs, _, inner = y_ref.shape
    channels = cb_ref.shape[1]
    b = pl.program_id(0)

    @pl.when(b == 0)
    def _():
        fill_constants(e_ref, tri_ref, skip_ref, head_ref)

    @pl.when(b == 0)
    def _():
        state[...] = jnp.zeros_like(state)
        ext[:, 0:8, :] = jnp.zeros((seqs, 8, channels), f32)

    @pl.when(b > 0)
    def _():
        ext[:, 0:8, :] = ext[:, Q : Q + 8, :]

    alternate(
        [
            fwd_block(
                q, seg_ref, xbc_ref.at[q], dt_ref.at[q], cw_ref, cb_ref, head_ref,
                *[r.at[q] for r in (y_ref, s_ref, sin_ref, state, ext)], e_ref, tri_ref, skip_ref,
            )
            for q in range(seqs)
        ],
        2,
    )


def fwd_block(
    q, seg_ref, xbc_ref, dt_ref, cw_ref, cb_ref, head_ref,
    y_ref, s_ref, sin_ref, state, ext, e_ref, tri_ref, skip_ref,
):
    inner = y_ref.shape[1]
    b, blocks = pl.program_id(0), pl.num_programs(0)
    dtb, _, na2 = head_terms(head_ref)
    ext[8 : 8 + Q, :] = xbc_ref[...]
    seg, cols = segment_rows(seg_ref, b, blocks, q * blocks + b)
    m1, m2, m3 = (wide(cols[:, k : k + 1], 256) for k in (1, 2, 3))

    def conv(c):
        at = pl.ds(c, 256)
        x = ext[:, at]
        s = cb_ref[:, at] + cw_ref[3:4, at] * x[8:]
        s += m1 * (cw_ref[2:3, at] * later_rows(x, 7))
        s += m2 * (cw_ref[1:2, at] * later_rows(x, 6))
        s += m3 * (cw_ref[0:1, at] * later_rows(x, 5))
        s_ref[:, at] = s
        return s * sigmoid(s)

    bc, bc_rest = split(conv(inner), 2)
    bm, cm = bc[:, :LANES], bc[:, LANES:]
    bt = bm.T
    c_two = jnp.concatenate([cm, bc_rest[:, LANES:]], axis=1)
    _, ts, cum, start, end = step_terms(dt_ref[...], dtb, na2, tri_ref[...], cols)
    cum_t = cum.T
    grow = expand_operand(start, end, ts)
    row_i = lax.broadcasted_iota(jnp.int32, (Q, Q), 0)
    col_j = lax.broadcasted_iota(jnp.int32, (Q, Q), 1)
    same = wide(cols[:, 0:1], LANES) == seg
    mask = jnp.where(same & (row_i >= col_j), 0.0, NEG)
    scores = dot_split((cm, bc_rest[:, LANES:]), (bm, bc_rest[:, :LANES]))
    left = col_j < HEAD
    yield

    for c in range(0, inner, 256):
        at = pl.ds(c, 256)
        x = conv(c)
        big = dot(grow, e_ref[:, at])
        s_e, e_e, t_e = big[:Q], big[Q : 2 * Q], big[2 * Q :]
        xs = x * t_e
        xs_low = xs.astype(bf16)
        st = state[:, at]
        st_low = st.astype(bf16)
        sin_ref[:, at] = st_low
        carried = dot(c_two, twice(st_low, 0))
        parts = []
        for p in range(2):
            mats = []
            for h in range(2):
                head = (c + p * LANES) // HEAD + h
                gap = wide(cum[:, head : head + 1], LANES) - cum_t[head : head + 1, :] + mask
                mats.append((jnp.exp2(gap) * scores).astype(bf16))
            xp = xs_low[:, p * LANES : (p + 1) * LANES]
            parts.append(dot(jnp.concatenate(mats, axis=1), by_head(xp, left)))
        y = jnp.concatenate(parts, axis=1) + s_e * carried + skip_ref[:, at] * x
        y_ref[:, at] = y
        state[:, at] = st * s_e[Q - 1 : Q, :] + dot(bt, (xs * e_e).astype(bf16))
        yield


def fixed(shape):
    return pl.BlockSpec(shape, lambda *_: (0,) * len(shape))


def state_forward(seg, xbc, dt, cw, cb, head, inner, seqs):
    rows, channels = xbc.shape
    blocks = rows // seqs // Q
    at = lambda b: (0, b, 0)
    tiled = lambda v: v.reshape(seqs, rows // seqs, v.shape[1])
    y, s, sin = pl.pallas_call(
        fwd_kernel,
        grid=(blocks,),
        in_specs=[
            fixed(seg.shape),
            pl.BlockSpec((seqs, Q, channels), at),
            pl.BlockSpec((seqs, Q, LANES), at),
            fixed(cw.shape), fixed(cb.shape), fixed(head.shape),
        ],
        out_specs=[
            pl.BlockSpec((seqs, Q, inner), at),
            pl.BlockSpec((seqs, Q, channels), at),
            pl.BlockSpec((seqs, None, LANES, inner), lambda b: (0, b, 0, 0)),
        ],
        out_shape=[
            jax.ShapeDtypeStruct((seqs, rows // seqs, inner), f32),
            jax.ShapeDtypeStruct((seqs, rows // seqs, channels), f32),
            jax.ShapeDtypeStruct((seqs, blocks, LANES, inner), bf16),
        ],
        scratch_shapes=[
            pltpu.VMEM((seqs, LANES, inner), f32),
            pltpu.VMEM((seqs, Q + 8, channels), f32),
            pltpu.VMEM((2 * LANES, inner), bf16),
            pltpu.VMEM((Q, Q), bf16),
            pltpu.VMEM((1, inner), f32),
        ],
        compiler_params=params(60 << 20),
        name="state_forward",
    )(seg, tiled(xbc), tiled(dt), cw, cb, head)
    return y.reshape(rows, inner), s.reshape(rows, channels), sin


def flat(ref):
    v = ref[...]
    return v.reshape(v.shape[0] * v.shape[1], v.shape[2])


def slab_views(slab, own):
    owners, _, width = slab.shape
    if own % 16 == 0:
        first = lambda *_: (0, 0, 0)
        second = lambda *_: (0, 1, 0)
        sizes = ((own, first), (own, second), (2 * own, second))
        return [(slab, pl.BlockSpec((owners, n, width), index)) for n, index in sizes]
    parts = [
        v.reshape(1, -1, width) for v in (slab[:, :own], slab[:, own : 2 * own], slab[:, 2 * own :])
    ]
    return [(v, fixed(v.shape)) for v in parts]


def gate_kernel(
    tok_ref, normed_ref, y_ref, cot_ref, wa_ref, wb_ref, wo_ref, gain_ref,
    gn_ref, out_ref, gz_ref, gm_ref, ggain_ref,
):
    wa, wb, wo = flat(wa_ref), flat(wb_ref), flat(wo_ref)
    gain = gain_ref[...]

    @pl.when(pl.program_id(0) == 0)
    def _():
        ggain_ref[...] = jnp.zeros_like(ggain_ref)

    normed = normed_ref[...]
    z = jnp.concatenate([dot(normed, wa), dot(normed, wb)], axis=1)
    g_gn = dot(cot_ref[...], wo, NT)
    sg = sigmoid(z)
    sz = z * sg
    y = y_ref[...]
    gated = y * sz
    rstd = lax.rsqrt(jnp.mean(gated * gated, axis=-1, keepdims=True) + EPS)
    unit = gated * rstd
    gn = (unit * gain).astype(bf16)
    gn_ref[...] = gn
    out_ref[...] = (tok_ref[...].astype(f32) + dot(gn, wo)).astype(bf16)
    ggain_ref[...] += fold_rows(unit * g_gn)
    q = g_gn * gain
    mean = jnp.mean(unit * q, axis=-1, keepdims=True)
    g_gated = rstd * (q - unit * mean)
    gm_ref[...] = g_gated * sz
    gz_ref[...] = (g_gated * y * (sg * (1.0 + z * (1.0 - sg)))).astype(bf16)


def gate(tok, normed, y, cot, weights, gain, tile=256):
    rows, width = tok.shape
    inner = y.shape[1]
    at = lambda i: (i, 0)
    return pl.pallas_call(
        gate_kernel,
        grid=(rows // tile,),
        in_specs=[
            pl.BlockSpec((tile, width), at),
            pl.BlockSpec((tile, width), at),
            pl.BlockSpec((tile, inner), at),
            pl.BlockSpec((tile, width), at),
            *[spec for _, spec in weights], fixed(gain.shape),
        ],
        out_specs=[
            pl.BlockSpec((tile, inner), at),
            pl.BlockSpec((tile, width), at),
            pl.BlockSpec((tile, inner), at),
            pl.BlockSpec((tile, inner), at),
            fixed((8, inner)),
        ],
        out_shape=[
            jax.ShapeDtypeStruct((rows, inner), bf16),
            jax.ShapeDtypeStruct((rows, width), bf16),
            jax.ShapeDtypeStruct((rows, inner), bf16),
            jax.ShapeDtypeStruct((rows, inner), f32),
            jax.ShapeDtypeStruct((8, inner), f32),
        ],
        compiler_params=params(60 << 20),
        name="gate",
    )(tok, normed, y, cot, *[v for v, _ in weights], gain)


def bwd_kernel(
    seg_ref, xbc_ref, dt_ref, s_ref, sin_ref, gm_ref, cw_ref, head_ref,
    gx_ref, gcw_ref, gcb_ref, gskip_ref, galog_ref, gdtb_ref,
    adj, gext, da_rows, spread, grad_b, grad_c, link, e_ref, tri_ref, skip_ref, et_ref, tail_ref, pair_ref,
):
    seqs, _, inner = gm_ref.shape
    channels = s_ref.shape[2]
    b = pl.program_id(0)

    @pl.when(b == 0)
    def _():
        for ref in (gcw_ref, gcb_ref, gskip_ref, galog_ref, gdtb_ref, da_rows):
            ref[...] = jnp.zeros_like(ref)
        fill_constants(e_ref, tri_ref, skip_ref, head_ref)
        et_ref[...] = ones_where(iota((inner, LANES), 0) // HEAD == iota((inner, LANES), 1))
        turned = ones_where(iota((Q, Q), 0) <= iota((Q, Q), 1))
        below = ones_where(iota((Q, Q), 0) > iota((Q, Q), 1))
        tail_ref[...] = jnp.concatenate([turned, turned, below, below], axis=1)
        row, col = iota((2 * Q, 2 * Q), 0), iota((2 * Q, 2 * Q), 1)
        pair_ref[...] = ones_where((row // Q == col // Q) & (row >= col))

    @pl.when(b == 0)
    def _():
        adj[...] = jnp.zeros_like(adj)
        gext[:, Q : Q + 8, :] = jnp.zeros((seqs, 8, channels), f32)

    @pl.when(b > 0)
    def _():
        gext[:, Q : Q + 8, :] = gext[:, 0:8, :]

    alternate(
        [
            bwd_block(
                q, seg_ref, *[r.at[q] for r in (xbc_ref, dt_ref, s_ref, sin_ref, gm_ref)], cw_ref, head_ref,
                gx_ref.at[q], gcw_ref, gcb_ref, gskip_ref, galog_ref, gdtb_ref,
                *[r.at[q] for r in (adj, gext, da_rows, spread, grad_b, grad_c, link)],
                e_ref, tri_ref, skip_ref, et_ref, tail_ref, pair_ref,
            )
            for q in range(seqs)
        ],
        26,
    )


def alternate(blocks, lead):
    for _ in range(lead):
        next(blocks[0], None)
    live = list(blocks)
    while live:
        live = [block for block in reversed(live) if next(block, live) is not live][::-1]


def bwd_block(
    q, seg_ref, xbc_ref, dt_ref, s_ref, sin_ref, gm_ref, cw_ref, head_ref,
    gx_ref, gcw_ref, gcb_ref, gskip_ref, galog_ref, gdtb_ref,
    adj, gext, da_rows, spread, grad_b, grad_c, link, e_ref, tri_ref, skip_ref, et_ref, tail_ref, pair_ref,
):
    inner = gm_ref.shape[1]
    channels = s_ref.shape[1]
    b, blocks = pl.program_id(0), pl.num_programs(0)
    dtb, rate, na2 = head_terms(head_ref)
    turn = blocks - 1 - b
    seg, cols = segment_rows(seg_ref, turn, blocks, q * blocks + turn)
    raw, ts, cum, start, end = step_terms(dt_ref[...], dtb, na2, tri_ref[...], cols)
    cum_t = cum.T
    grow = expand_operand(start, end, ts)
    yield

    def act(c):
        s = s_ref[:, pl.ds(c, 256)]
        sg = sigmoid(s)
        return s * sg, sg * (1.0 + s * (1.0 - sg))

    bc, slope_bc = act(inner)
    bc, bc_rest = split(bc, 2)
    bm, cm = bc[:, :LANES], bc[:, LANES:]
    ct = cm.T
    b_two = jnp.concatenate([bm, bc_rest[:, :LANES]], axis=1)
    c_two = jnp.concatenate([cm, bc_rest[:, LANES:]], axis=1)
    row_j = lax.broadcasted_iota(jnp.int32, (Q, Q), 0)
    col_i = lax.broadcasted_iota(jnp.int32, (Q, Q), 1)
    same = wide(cols[:, 0:1], LANES) == seg
    mask = jnp.where(same & (col_i >= row_j), 0.0, NEG)
    before = (row_j < col_i).astype(f32)
    scores = dot_split((bm, bc_rest[:, :LANES]), (cm, bc_rest[:, LANES:]))
    left = col_i < HEAD
    grad_scores = jnp.zeros((Q, Q), f32)
    yield

    def enter(c):
        at = pl.ds(c, 256)
        x, slope = act(c)
        big = dot(grow, e_ref[:, at])
        s_e, e_e, t_e = big[:Q], big[Q : 2 * Q], big[2 * Q :]
        xs = x * t_e
        xs_low, xs_rest = split(xs, 2)
        gm = gm_ref[:, at]
        gm_low, gm_rest = split(gm, 2)
        ad_low, ad_rest = split(adj[:, at], 2)
        st_low = sin_ref[:, at]
        into = dot(b_two, twice(ad_low, 0)) + dot(bm, ad_rest)
        carried = dot(c_two, twice(st_low, 0))
        diags, gmats = [], []
        for p in range(2):
            lanes = slice(p * LANES, (p + 1) * LANES)
            diags.append((by_head(gm_low[:, lanes], left), by_head(gm_rest[:, lanes], left)))
            tall = dot(jnp.concatenate([xs_low[:, lanes], xs_rest[:, lanes]], axis=0), diags[p][0], NT)
            gmats.append(tall[:Q] + tall[Q:] + dot(xs_low[:, lanes], diags[p][1], NT))
        return x, slope, s_e, e_e, t_e, xs, gm, ad_low, st_low, into, carried, diags, gmats

    def within(c, held):
        diags, gmats = held[-2:]
        parts, joined = [], []
        extra = jnp.zeros((Q, Q), f32)
        for p in range(2):
            diag, diag_rest = diags[p]
            mats, links = [], []
            for h in range(2):
                head = (c + p * LANES) // HEAD + h
                gap = cum_t[head : head + 1, :] - wide(cum[:, head : head + 1], LANES) + mask
                decay = jnp.exp2(gap)
                mat = decay * scores
                grad = gmats[p][:, h * LANES : (h + 1) * LANES]
                extra += decay * grad
                mats.append(split(mat, 2))
                links.append((mat * grad).astype(bf16))
            high = jnp.concatenate([mats[0][0], mats[1][0]], axis=1)
            rest = jnp.concatenate([mats[0][1], mats[1][1]], axis=1)
            both = dot(jnp.concatenate([high, rest], axis=0), diag)
            parts.append(both[:Q] + both[Q:] + dot(high, diag_rest))
            joined.append(jnp.concatenate(links, axis=1))
            yield
        reach = dot(jnp.concatenate(joined, axis=0), pair_ref[...])
        for n in range(4):
            p, h = n // 2, n % 2
            head = c // HEAD + n
            da_rows[head : head + 1, :] = jnp.sum(
                reach[p * Q : (p + 1) * Q, h * LANES : (h + 1) * LANES] * before, axis=0, keepdims=True
            )
        return parts, extra

    def leave(c, held, parts):
        at = pl.ds(c, 256)
        x, slope, s_e, e_e, t_e, xs, gm, ad_low, st_low, into, carried = held[:-2]
        ad = adj[:, at]
        g_xs = jnp.concatenate(parts, axis=1) + e_e * into
        gext[0:Q, at] = (t_e * g_xs + skip_ref[:, at] * gm) * slope
        sums = jnp.concatenate(
            [pair_split(carried * gm), pair_split(x * into), pair_split(x * g_xs)], axis=0
        )
        sums = dot(sums, twice(et_ref[at, :], 0))
        s_gm = (s_e * gm).astype(bf16)
        part_c = dot(s_gm, st_low, NT)
        part_b = dot((e_e * xs).astype(bf16), ad_low, NT)
        if c == 0:
            spread[...] = sums
            grad_c[...] = part_c
            grad_b[...] = part_b
        else:
            spread[...] += sums
            grad_c[...] += part_c
            grad_b[...] += part_b
        gskip_ref[:, at] += fold_rows(gm * x)
        link[:, at] = fold_rows(st_low.astype(f32) * ad)
        adj[:, at] = ad * s_e[Q - 1 : Q, :] + dot(ct, s_gm)

    starts = list(range(0, inner, 256))
    held, inside = {}, {}
    for step in range(len(starts) + 1):
        if step < len(starts):
            held[step] = enter(starts[step])
            yield
        if 0 <= step - 1:
            parts, extra = yield from within(starts[step - 1], held[step - 1])
            grad_scores += extra
            leave(starts[step - 1], held.pop(step - 1), parts)
        yield

    grad_low = grad_scores.astype(bf16)
    g_b = grad_b[...] + dot(grad_low, cm)
    g_c = grad_c[...] + dot(grad_low, bm, TN)
    gext[0:Q, pl.ds(inner, 256)] = jnp.concatenate([g_b, g_c], axis=1) * slope_bc

    phi = start * spread[0:Q]
    psi = end * ts * spread[Q : 2 * Q]
    through = jnp.sum(dot(jnp.concatenate(split(link[...], 2), axis=0), et_ref[...]), axis=0, keepdims=True)
    around = jnp.concatenate(split(phi, 2) + split(psi, 2), axis=0)
    da = da_rows[...].T + dot(tail_ref[...], around) + start[Q - 1 : Q, :] * through
    g_ts = spread[2 * Q :] + rate * da
    yield
    galog_ref[...] += fold_rows(ts * rate * da)
    g_dt = g_ts * sigmoid(raw)
    gdtb_ref[...] += fold_rows(g_dt)

    n1, n2, n3 = (wide(cols[:, k : k + 1], 256) for k in (6, 7, 8))
    for c in range(0, channels, 256):
        at = pl.ds(c, 256)
        x = xbc_ref[:, at]
        g = gext[:, at]
        g0 = g[:Q]
        g1 = later_rows(g, 1) * n1
        g2 = later_rows(g, 2) * n2
        g3 = later_rows(g, 3) * n3
        gx = cw_ref[3:4, at] * g0 + cw_ref[2:3, at] * g1 + cw_ref[1:2, at] * g2 + cw_ref[0:1, at] * g3
        gx_ref[:, at] = gx.astype(bf16)
        gcb_ref[:, at] += fold_rows(g0)
        gcw_ref[24:32, at] += fold_rows(g0 * x)
        gcw_ref[16:24, at] += fold_rows(g1 * x)
        gcw_ref[8:16, at] += fold_rows(g2 * x)
        gcw_ref[0:8, at] += fold_rows(g3 * x)
        yield
    gx_ref[:, channels:] = g_dt.astype(bf16)


def state_backward(seg, xbc, dt, s, sin, gm, cw, head, seqs):
    rows, channels = xbc.shape
    inner = gm.shape[1]
    blocks = rows // seqs // Q
    at = lambda b: (0, blocks - 1 - b, 0)
    tiled = lambda v: v.reshape(seqs, rows // seqs, v.shape[1])
    out = pl.pallas_call(
        bwd_kernel,
        grid=(blocks,),
        in_specs=[
            fixed(seg.shape),
            pl.BlockSpec((seqs, Q, channels), at),
            pl.BlockSpec((seqs, Q, LANES), at),
            pl.BlockSpec((seqs, Q, channels), at),
            pl.BlockSpec((seqs, None, LANES, inner), lambda b: (0, blocks - 1 - b, 0, 0)),
            pl.BlockSpec((seqs, Q, inner), at),
        ]
        + [fixed(v.shape) for v in (cw, head)],
        out_specs=[
            pl.BlockSpec((seqs, Q, channels + LANES), at),
            fixed((32, channels)), fixed((8, channels)), fixed((8, inner)), fixed((8, LANES)), fixed((8, LANES)),
        ],
        out_shape=[
            jax.ShapeDtypeStruct((seqs, rows // seqs, channels + LANES), bf16),
            jax.ShapeDtypeStruct((32, channels), f32),
            jax.ShapeDtypeStruct((8, channels), f32),
            jax.ShapeDtypeStruct((8, inner), f32),
            jax.ShapeDtypeStruct((8, LANES), f32),
            jax.ShapeDtypeStruct((8, LANES), f32),
        ],
        scratch_shapes=[
            pltpu.VMEM((seqs, LANES, inner), f32),
            pltpu.VMEM((seqs, Q + 8, channels), f32),
            pltpu.VMEM((seqs, LANES, LANES), f32),
            pltpu.VMEM((seqs, 3 * Q, LANES), f32),
            pltpu.VMEM((seqs, Q, LANES), f32),
            pltpu.VMEM((seqs, Q, LANES), f32),
            pltpu.VMEM((seqs, 8, inner), f32),
            pltpu.VMEM((2 * LANES, inner), bf16),
            pltpu.VMEM((Q, Q), bf16),
            pltpu.VMEM((1, inner), f32),
            pltpu.VMEM((inner, LANES), bf16),
            pltpu.VMEM((Q, 4 * Q), bf16),
            pltpu.VMEM((2 * Q, 2 * Q), bf16),
        ],
        compiler_params=params(60 << 20),
        name="state_backward",
    )(
        seg, tiled(xbc), tiled(dt), tiled(s), sin.reshape(seqs, blocks, LANES, inner), tiled(gm), cw, head
    )
    return out[0].reshape(rows, channels + LANES), *out[1:]


def token_kernel(tok_ref, cot_ref, gz_ref, gx_ref, wa_ref, wb_ref, wx_ref, gain_ref, out_ref, ggain_ref):
    half = gz_ref.shape[1] // 2
    g = dot(gz_ref[:, :half], flat(wa_ref), NT) + dot(gz_ref[:, half:], flat(wb_ref), NT)
    g += dot(gx_ref[...], wx_ref[...], NT)
    u = tok_ref[...].astype(f32)
    r = lax.rsqrt(jnp.mean(u * u, axis=-1, keepdims=True) + EPS)
    unit = u * r

    @pl.when(pl.program_id(0) == 0)
    def _():
        ggain_ref[...] = jnp.zeros_like(ggain_ref)

    ggain_ref[...] += fold_rows(unit * g)
    q = g * gain_ref[...]
    mean = jnp.mean(unit * q, axis=-1, keepdims=True)
    out_ref[...] = (cot_ref[...].astype(f32) + r * (q - unit * mean)).astype(bf16)


def token_grad(tok, cot, gz, gx, weights, wx, gain, tile=256):
    rows, width = tok.shape
    at = lambda i: (i, 0)
    return pl.pallas_call(
        token_kernel,
        grid=(rows // tile,),
        in_specs=[
            pl.BlockSpec((tile, width), at),
            pl.BlockSpec((tile, width), at),
            pl.BlockSpec((tile, gz.shape[1]), at),
            pl.BlockSpec((tile, gx.shape[1]), at),
            *[spec for _, spec in weights], fixed(wx.shape), fixed(gain.shape),
        ],
        out_specs=[pl.BlockSpec((tile, width), at), fixed((8, width))],
        out_shape=[jax.ShapeDtypeStruct((rows, width), bf16), jax.ShapeDtypeStruct((8, width), f32)],
        compiler_params=params(60 << 20),
        name="token_grad",
    )(tok, cot, gz, gx, *[v for v, _ in weights], wx, gain)


MESH = pl.DeviceIdType.MESH


def place(line):
    me = lax.axis_index("dp")
    index = lambda l, x, c: (l * 2 + x) * 2 + c
    return me // 4, (me // 2) % 2, me % 2, index, lax.axis_index("seq")


def meet(devices):
    barrier = pltpu.get_barrier_semaphore()
    for device in devices:
        pl.semaphore_signal(barrier, inc=1, device_id=device, device_id_type=MESH)
    pl.semaphore_wait(barrier, len(devices))


def remote(src, dst, send, recv, device):
    return pltpu.make_async_remote_copy(
        src_ref=src, dst_ref=dst, send_sem=send, recv_sem=recv, device_id=device, device_id_type=MESH
    )


def gather_kernel(line, own_ref, out_ref, line_send, x_send, y_send, core_send, recv, local):
    l, x, c, index, y = place(line)
    others = [{"dp": index((l + k) % line, x, c)} for k in range(1, line)]
    beside, sibling, across = {"dp": index(l, 1 - x, c)}, {"dp": index(l, x, 1 - c)}, {"seq": 1 - y}
    meet(others + [beside, sibling, across])
    started = []

    def send(src, at, sem, device):
        copy = remote(src, out_ref.at[at], sem, recv.at[at], device)
        copy.start()
        started.append(copy)

    def arrived(at):
        remote(out_ref.at[at], out_ref.at[at], local.at[1], recv.at[at], sibling).wait_recv()

    mine = pltpu.make_async_copy(own_ref, out_ref.at[l, x, c], local.at[0])
    mine.start()
    send(own_ref.at[y], (l, x, c, y), x_send.at[0], beside)
    for k in range(1, line):
        send(own_ref.at[y], (l, x, c, y), line_send.at[k, 0], others[k - 1])
    for k in range(1, line):
        send(own_ref.at[1 - y], (l, x, c, 1 - y), line_send.at[k, 1], others[k - 1])
    for h in range(2):
        send(own_ref.at[h], (l, x, c, h), core_send.at[0, h], sibling)
    for k in range(1, line):
        at = ((l + k) % line, x, c, y)
        arrived(at)
        send(out_ref.at[at], at, x_send.at[k], beside)
        send(out_ref.at[at], at, core_send.at[k, 0], sibling)
    for k in range(line):
        at = ((l + k) % line, 1 - x, c, y)
        arrived(at)
        send(out_ref.at[at], at, y_send.at[k], across)
        send(out_ref.at[at], at, core_send.at[line + k, 0], sibling)
    for k in range(1, line):
        at = ((l + k) % line, x, c, 1 - y)
        arrived(at)
        send(out_ref.at[at], at, core_send.at[k, 1], sibling)
    for k in range(line):
        at = ((l + k) % line, 1 - x, c, 1 - y)
        arrived(at)
        send(out_ref.at[at], at, core_send.at[line + k, 1], sibling)
    for k in range(line):
        for side in range(2):
            for h in range(2):
                arrived(((l + k) % line, side, 1 - c, h))
    for copy in started:
        copy.wait_send()
    mine.wait()


def gather(local, owners):
    own, columns = local.shape
    line = owners // 4
    vmem = pl.BlockSpec(memory_space=pltpu.VMEM)
    dma = pltpu.SemaphoreType.DMA
    out = pl.pallas_call(
        functools.partial(gather_kernel, line),
        in_specs=[vmem],
        out_specs=vmem,
        out_shape=jax.ShapeDtypeStruct((line, 2, 2, 2, own // 2, columns), local.dtype),
        scratch_shapes=[
            dma((line, 2)), dma((line,)), dma((line,)), dma((2 * line, 2)), dma((line, 2, 2, 2)), dma((2,)),
        ],
        compiler_params=params(48 << 20, collective_id=1, has_side_effects=True),
        name="gather",
    )(local.reshape(2, own // 2, columns))
    return out.reshape(owners * own, columns)


def pack_small(acc, cw_ref, cb_ref, ggain_ref, skip_ref, ngain_ref, alog_ref, dtb_ref):
    inner, width = ggain_ref.shape[1], ngain_ref.shape[1]
    total = lambda v: jnp.sum(v, axis=0, keepdims=True)
    acc[...] = jnp.zeros(acc.shape, f32)
    for k in range(4):
        acc[k : k + 1, :] = total(cw_ref[8 * k : 8 * k + 8, :])
    acc[4:5, :] = total(cb_ref[...])
    acc[5:6, :inner] = total(ggain_ref[...])
    acc[6:7, :width] = total(ngain_ref[...])
    acc[6:7, width : width + LANES] = total(alog_ref[...])
    acc[6:7, width + LANES : width + 2 * LANES] = total(dtb_ref[...])
    skip = jnp.concatenate(split(skip_ref[...], 3), axis=0)
    by_head = ones_where(iota((inner, LANES), 0) // HEAD == iota((inner, LANES), 1))
    acc[6:7, width + 2 * LANES : width + 3 * LANES] = total(dot(skip, by_head))


def finish_kernel(
    line, bits, cw_ref, cb_ref, ggain_ref, skip_ref, ngain_ref, alog_ref, dtb_ref, zo_ref, zo_got_ref, d_ref,
    small_ref, din_ref, dout_ref,
    acc, got, core_got, one, two_got, two, three_got, three, line_got, last, last_got,
    small_send, small_recv, core_send, core_recv, two_send, two_recv, three_send, three_recv,
    line_send, line_recv, last_sem,
):
    l, x, c, index, y = place(line)
    me = lax.axis_index("dp")
    doubling = [{"dp": me + bit - 2 * bit * ((me // bit) % 2)} for bit in bits]
    others = [{"dp": index((l + k) % line, x, c)} for k in range(1, line)]
    beside, sibling, across = {"dp": index(l, 1 - x, c)}, {"dp": index(l, x, 1 - c)}, {"seq": 1 - y}
    meet(doubling + others + [beside, sibling, across])
    order = list(range(1, line)) + [0]
    at = [(l + k) % line for k in order]

    def plus(a, b):
        return a.astype(f32) + b.astype(f32)

    def launch(*args):
        copy = remote(*args)
        copy.start()
        return copy

    first = []
    for i in range(line):
        first.append(
            launch(d_ref.at[at[i], :, 1 - c], core_got.at[i], core_send.at[i], core_recv.at[i], sibling)
        )
    pack_small(acc.at[0], cw_ref, cb_ref, ggain_ref, skip_ref, ngain_ref, alog_ref, dtb_ref)
    smalls = doubling + [across]
    second, third, fourth = [], [], []

    def small_start(k):
        return launch(acc.at[k], got.at[k], small_send.at[k], small_recv.at[k], smalls[k])

    for t in range(max(line + 2, len(smalls))):
        small = small_start(t) if t < len(smalls) else None
        if t < line:
            i = t
            first[i].wait()
            for a in range(2):
                for h in range(2):
                    one[i, a, h] = plus(d_ref[at[i], a, c, h], core_got[i, a, h]).astype(bf16)
            src, device = (one.at[i, 1 - x], beside) if i % 2 == 0 else (one.at[i, :, 1 - y], across)
            second.append(launch(src, two_got.at[i], two_send.at[i], two_recv.at[i], device))
        if 1 <= t <= line:
            i = t - 1
            second[i].wait()
            for j in range(2):
                kept = one[i, x, j] if i % 2 == 0 else one[i, j, y]
                two[i, j] = plus(kept, two_got[i, j]).astype(bf16)
            src, device = (two.at[i, 1 - y], across) if i % 2 == 0 else (two.at[i, 1 - x], beside)
            third.append(launch(src, three_got.at[i], three_send.at[i], three_recv.at[i], device))
        if 2 <= t <= line + 1:
            i = t - 2
            third[i].wait()
            kept = two[i, y] if i % 2 == 0 else two[i, x]
            three[i] = plus(kept, three_got[i]).astype(bf16)
            if order[i] > 0:
                fourth.append(
                    launch(three.at[i], line_got.at[l], line_send.at[i], line_recv.at[l], others[order[i] - 1])
                )
        if small is not None:
            small.wait()
            acc[t + 1] = acc[t] + got[t]

    small_ref[...] = acc[len(smalls)]
    own, half = din_ref.shape[0], zo_ref.shape[1]
    zo = plus(zo_ref[...], zo_got_ref[...])
    din_ref[:, :half] = zo[:own]
    din_ref[:, half : 2 * half] = zo[own : 2 * own]
    dout_ref[...] = zo[2 * own :]

    total = three[line - 1].astype(f32)
    for k in range(1, line):
        at_k = (l + k) % line
        remote(three.at[0], line_got.at[at_k], last_sem.at[2], line_recv.at[at_k], sibling).wait_recv()
        total += line_got[at_k].astype(f32)
    last[...] = total.astype(bf16)
    final = launch(last, last_got, last_sem.at[0], last_sem.at[1], across)
    for copy in fourth:
        copy.wait_send()
    final.wait()
    left = din_ref.shape[1] - 2 * half
    kept, came = last[...].astype(f32), last_got[...].astype(f32)
    lower = (y == 0).astype(f32)
    din_ref[: own // 2, 2 * half :] = (kept * lower + came * (1.0 - lower))[:, :left]
    din_ref[own // 2 :, 2 * half :] = (came * lower + kept * (1.0 - lower))[:, :left]


def finish(smalls, d_zo, zo_got, d_x, own, proj):
    owners = d_x.shape[0] // own
    line, columns, half = owners // 4, d_x.shape[1], d_zo.shape[1]
    bits = [1 << i for i in range(owners.bit_length() - 1)]
    channels = smalls[1].shape[1]
    vmem = pl.BlockSpec(memory_space=pltpu.VMEM)
    dma = pltpu.SemaphoreType.DMA
    piece = (own // 2, columns)
    steps = len(bits) + 1
    low = lambda *dims: pltpu.VMEM(dims + piece, bf16)
    return pl.pallas_call(
        functools.partial(finish_kernel, line, bits),
        in_specs=[vmem] * 10,
        out_specs=[vmem] * 3,
        out_shape=[
            jax.ShapeDtypeStruct((8, channels), f32),
            jax.ShapeDtypeStruct((own, proj), f32),
            jax.ShapeDtypeStruct((2 * own, half), f32),
        ],
        scratch_shapes=[
            pltpu.VMEM((steps + 1, 8, channels), f32),
            pltpu.VMEM((steps, 8, channels), f32),
            low(line, 2, 2), low(line, 2, 2), low(line, 2), low(line, 2), low(line), low(line), low(line), low(), low(),
            dma((steps,)), dma((steps,)),
        ]
        + [dma((line,))] * 8
        + [dma((3,))],
        compiler_params=params(48 << 20, collective_id=0, has_side_effects=True),
        name="finish",
    )(*smalls, d_zo, zo_got, d_x.reshape(line, 2, 2, 2, own // 2, columns))


def finish_plain(smalls, d_zo, d_x, own, proj):
    cw, cb, ggain, skip, ngain, alog, dtb = (v.reshape(-1, 8, v.shape[1]).sum(1) for v in smalls)
    skip = jnp.pad(skip.reshape(1, -1, HEAD).sum(2), ((0, 0), (0, LANES - skip.shape[1] // HEAD)))
    tail = jnp.concatenate([ngain, alog, dtb, skip], axis=1)
    wide = lambda v: jnp.pad(v, ((0, 0), (0, cb.shape[1] - v.shape[1])))
    small = lax.psum(jnp.concatenate([cw, cb, wide(ggain), wide(tail)], axis=0), ("dp", "seq"))
    d_x = lax.psum_scatter(d_x, "dp", scatter_dimension=0, tiled=True)
    d_zo, d_x = lax.psum((d_zo.astype(f32), d_x.astype(f32)), "seq")
    d_in = jnp.concatenate([d_zo[:own], d_zo[own : 2 * own], d_x], axis=1)[:, :proj]
    return small, d_in, d_zo[2 * own :]


def per_device(
    sizes, tokens, segments, cotangent, norm_gain, weight_in, conv_weight, conv_bias, dt_bias, a_log, skip_d,
    gate_gain, weight_out,
):
    seqs, length, width = tokens.shape
    rows = seqs * length
    inner = gate_gain.shape[0]
    channels = conv_bias.shape[0]
    heads = dt_bias.shape[0]
    own = weight_in.shape[0]
    owners = width // own
    tok = tokens.reshape(rows, width)
    cot = cotangent.reshape(rows, width)
    pad = LANES - heads

    local_x = jnp.pad(weight_in[:, inner:], ((0, 0), (0, pad)))
    owned = sizes["dp"] % 4 == 0 and sizes["seq"] == 2
    wx = gather(local_x, owners) if owned else lax.all_gather(local_x, "dp", axis=0, tiled=True)
    local_zo = jnp.concatenate([weight_in[:, :width], weight_in[:, width:inner], weight_out], axis=0)
    wx, local_zo = lax.optimization_barrier((wx, local_zo))
    slab = lax.all_gather(local_zo, "dp", axis=0, tiled=True).reshape(owners, 4 * own, width)
    weights = slab_views(slab, own)

    head = jnp.pad(jnp.stack([dt_bias, -jnp.exp(a_log), skip_d]), ((0, 5), (0, pad)))
    seg = segments.astype(f32).reshape(rows // Q, Q)
    cb = conv_bias.reshape(1, channels)
    ngain = norm_gain.reshape(1, width)
    ggain = gate_gain.reshape(1, inner)

    normed, xbc, dt = project(tok, ngain, wx, channels)
    y, s, sin = state_forward(seg, xbc, dt, conv_weight, cb, head, inner, seqs)
    gn, out, gz, gm, p_ggain = gate(tok, normed, y, cot, weights, ggain)
    d_z = dot(normed, gz, TN).astype(bf16)
    d_out = dot(gn, cot, TN).astype(bf16)
    d_zo = jnp.concatenate(
        [
            d_z[:, :width].reshape(owners, own, width),
            d_z[:, width:].reshape(owners, own, width),
            d_out.reshape(owners, 2 * own, width),
        ],
        axis=1,
    ).reshape(owners * 4 * own, width)
    d_zo, gm = lax.optimization_barrier((d_zo, gm))
    d_zo = lax.psum_scatter(d_zo, "dp", scatter_dimension=0, tiled=True)
    gx, p_cw, p_cb, p_skip, p_alog, p_dtb = state_backward(seg, xbc, dt, s, sin, gm, conv_weight, head, seqs)
    d_x = dot(normed, gx, TN).astype(bf16)
    g_tok, p_ngain = token_grad(tok, cot, gz, gx, weights[:2], wx, ngain)
    smalls = (p_cw, p_cb, p_ggain, p_skip, p_ngain, p_alog, p_dtb)
    if owned:
        zo_got = lax.ppermute(d_zo, "seq", [(0, 1), (1, 0)])
        small, d_in, d_out = finish(smalls, d_zo, zo_got, d_x, own, weight_in.shape[1])
    else:
        small, d_in, d_out = finish_plain(smalls, d_zo, d_x, own, weight_in.shape[1])
    return (
        out.reshape(tokens.shape),
        g_tok.reshape(tokens.shape),
        small[6, :width],
        d_in,
        small[:4],
        small[4],
        small[6, width + LANES : width + LANES + heads],
        small[6, width : width + heads],
        small[6, width + 2 * LANES : width + 2 * LANES + heads],
        small[5, :inner],
        d_out,
    )


def solution(mesh):
    data = P(("dp", "seq"), None, None)
    owned = P("dp", None)
    placed = (data, P(("dp", "seq"), None), data, P(), owned, P(), P(), P(), P(), P(), P(), owned)
    return jax.shard_map(
        functools.partial(per_device, dict(mesh.shape)),
        mesh=mesh,
        in_specs=placed,
        out_specs=(data, data, P(), owned, P(), P(), P(), P(), P(), P(), owned),
        check_vma=False,
    )
```

```python
import functools
import math

import jax
import jax.numpy as jnp
from jax import lax
from jax.experimental import pallas as pl
from jax.experimental.pallas import tpu as pltpu
from jax.sharding import PartitionSpec as P

f32 = jnp.float32
bf16 = jnp.bfloat16
HEAD = 64
Q = 128
LANES = 128
EPS = 1e-05
LOG2E = math.log2(math.e)
NEG = -1e30

NN = (((1,), (0,)), ((), ()))
NT = (((1,), (1,)), ((), ()))
TN = (((0,), (0,)), ((), ()))


def dot(a, b, dims=NN):
    return lax.dot_general(a, b, dims, preferred_element_type=f32)


def pair_split(v):
    return jnp.concatenate(split(v, 2), axis=1)


def twice(v, axis):
    return jnp.concatenate([v, v], axis=axis)


def dot_split(a, b):
    low = b[1]
    return dot(jnp.concatenate(a, axis=1), twice(b[0], 1), NT) + dot(a[0], low, NT)


def sigmoid(v):
    return 0.5 + 0.5 * jnp.tanh(0.5 * v)


def split(v, parts):
    out = []
    for _ in range(parts):
        low = v.astype(bf16)
        out.append(low)
        v = v - low.astype(f32)
    return out


def fold_rows(v):
    return jnp.sum(v.reshape(v.shape[0] // 8, 8, v.shape[1]), axis=0)


def wide(v, width):
    col = jnp.broadcast_to(v, (v.shape[0], LANES))
    return jnp.concatenate([col] * (width // LANES), axis=1)


def params(limit=None, **more):
    return pltpu.CompilerParams(vmem_limit_bytes=limit, **more)


def proj_kernel(tok_ref, gain_ref, wx_ref, normed_ref, xbc_ref, dt_ref):
    u = tok_ref[...].astype(f32)
    r = lax.rsqrt(jnp.mean(u * u, axis=-1, keepdims=True) + EPS)
    normed = (u * r * gain_ref[...]).astype(bf16)
    normed_ref[...] = normed
    out = dot(normed, wx_ref[...])
    ch = xbc_ref.shape[1]
    xbc_ref[...] = out[:, :ch]
    dt_ref[...] = out[:, ch:]


def project(tok, gain, wx, channels, tile=256):
    rows, width = tok.shape
    cols = wx.shape[1]
    return pl.pallas_call(
        proj_kernel,
        grid=(rows // tile,),
        in_specs=[
            pl.BlockSpec((tile, width), lambda i: (i, 0)),
            pl.BlockSpec((1, width), lambda i: (0, 0)),
            pl.BlockSpec((width, cols), lambda i: (0, 0)),
        ],
        out_specs=[
            pl.BlockSpec((tile, width), lambda i: (i, 0)),
            pl.BlockSpec((tile, channels), lambda i: (i, 0)),
            pl.BlockSpec((tile, cols - channels), lambda i: (i, 0)),
        ],
        out_shape=[
            jax.ShapeDtypeStruct((rows, width), bf16),
            jax.ShapeDtypeStruct((rows, channels), f32),
            jax.ShapeDtypeStruct((rows, cols - channels), f32),
        ],
        compiler_params=params(60 << 20),
        name="project",
    )(tok, gain, wx)


def segment_rows(seg_ref, block, blocks, at):
    rows = seg_ref.shape[0]
    none = jnp.full((1, LANES), -1.0, f32)
    seg = seg_ref[pl.ds(at, 1), :]
    prev = jnp.where(block > 0, seg_ref[pl.ds(jnp.maximum(at - 1, 0), 1), :], none)
    after = jnp.where(block < blocks - 1, seg_ref[pl.ds(jnp.minimum(at + 1, rows - 1), 1), :], none)
    lane = lax.broadcasted_iota(jnp.int32, (1, LANES), 1)

    def same(other):
        return (other == seg).astype(f32)

    out = [seg]
    for k in (1, 2, 3):
        out.append(same(jnp.where(lane < k, pltpu.roll(prev, k, 1), pltpu.roll(seg, k, 1))))
    out.append(same(jnp.broadcast_to(prev[:, LANES - 1 :], (1, LANES))))
    out.append(same(jnp.broadcast_to(seg[:, LANES - 1 :], (1, LANES))))
    for k in (1, 2, 3):
        turn = LANES - k
        out.append(same(jnp.where(lane >= turn, pltpu.roll(after, turn, 1), pltpu.roll(seg, turn, 1))))
    tab = jnp.concatenate(out + [none] * (16 - len(out)), axis=0)
    return seg, jnp.concatenate([tab] * (LANES // 16), axis=0).T


def iota(shape, axis):
    return lax.broadcasted_iota(jnp.int32, shape, axis)


def ones_where(cond):
    return jnp.where(cond, 1.0, 0.0).astype(bf16)


def head_columns(heads_wide, inner, width):
    return ones_where(iota((heads_wide, inner), 0) % LANES == iota((heads_wide, inner), 1) // width)


def step_terms(dt, dtb, na2, tri, cols):
    raw = dt + dtb
    ts = jnp.maximum(raw, 0.0) + jnp.log1p(jnp.exp(-jnp.abs(raw)))
    cum = dot(jnp.concatenate([tri] * 3, axis=1), jnp.concatenate(split(ts * na2, 3), axis=0))
    start = jnp.exp2(cum) * wide(cols[:, 4:5], LANES)
    end = jnp.exp2(cum[Q - 1 : Q, :] - cum) * wide(cols[:, 5:6], LANES)
    return raw, ts, cum, start, end


def head_terms(head_ref):
    rate = head_ref[1:2, :]
    return head_ref[0:1, :], rate, rate * LOG2E


def fill_constants(e_ref, tri_ref, skip_ref, head_ref):
    inner = e_ref.shape[1]
    e_ref[...] = head_columns(e_ref.shape[0], inner, HEAD)
    tri_ref[...] = ones_where(iota((Q, Q), 0) >= iota((Q, Q), 1))
    skip = jnp.broadcast_to(head_ref[2:3, :], (8, LANES))
    wide_skip = dot(jnp.concatenate(split(skip, 3), axis=1), head_columns(3 * LANES, inner, HEAD))
    skip_ref[...] = wide_skip[0:1]


def expand_operand(*terms):
    return jnp.concatenate([jnp.concatenate(split(t, 2), axis=1) for t in terms], axis=0)


def by_head(v, left):
    zero = jnp.zeros_like(v)
    return jnp.concatenate([jnp.where(left, v, zero), jnp.where(left, zero, v)], axis=0)


def later_rows(v, k):
    width = v.shape[1]
    v = pltpu.roll(v.reshape(-1, 8, width), 8 - k, 1)
    here = lax.broadcasted_iota(jnp.int32, (1, 8, width), 1) < 8 - k
    return jnp.where(here, v[:-1], v[1:]).reshape(-1, width)


def fwd_kernel(
    seg_ref, xbc_ref, dt_ref, cw_ref, cb_ref, head_ref,
    y_ref, s_ref, sin_ref, state, ext, e_ref, tri_ref, skip_ref,
):
    seqs, _, inner = y_ref.shape
    channels = cb_ref.shape[1]
    b = pl.program_id(0)

    @pl.when(b == 0)
    def _():
        fill_constants(e_ref, tri_ref, skip_ref, head_ref)

    @pl.when(b == 0)
    def _():
        state[...] = jnp.zeros_like(state)
        ext[:, 0:8, :] = jnp.zeros((seqs, 8, channels), f32)

    @pl.when(b > 0)
    def _():
        ext[:, 0:8, :] = ext[:, Q : Q + 8, :]

    alternate(
        [
            fwd_block(
                q, seg_ref, xbc_ref.at[q], dt_ref.at[q], cw_ref, cb_ref, head_ref,
                *[r.at[q] for r in (y_ref, s_ref, sin_ref, state, ext)], e_ref, tri_ref, skip_ref,
            )
            for q in range(seqs)
        ],
        2,
    )


def fwd_block(
    q, seg_ref, xbc_ref, dt_ref, cw_ref, cb_ref, head_ref,
    y_ref, s_ref, sin_ref, state, ext, e_ref, tri_ref, skip_ref,
):
    inner = y_ref.shape[1]
    b, blocks = pl.program_id(0), pl.num_programs(0)
    dtb, _, na2 = head_terms(head_ref)
    ext[8 : 8 + Q, :] = xbc_ref[...]
    seg, cols = segment_rows(seg_ref, b, blocks, q * blocks + b)
    m1, m2, m3 = (wide(cols[:, k : k + 1], 256) for k in (1, 2, 3))

    def conv(c):
        at = pl.ds(c, 256)
        x = ext[:, at]
        s = cb_ref[:, at] + cw_ref[3:4, at] * x[8:]
        s += m1 * (cw_ref[2:3, at] * later_rows(x, 7))
        s += m2 * (cw_ref[1:2, at] * later_rows(x, 6))
        s += m3 * (cw_ref[0:1, at] * later_rows(x, 5))
        s_ref[:, at] = s
        return s * sigmoid(s)

    bc, bc_rest = split(conv(inner), 2)
    bm, cm = bc[:, :LANES], bc[:, LANES:]
    bt = bm.T
    c_two = jnp.concatenate([cm, bc_rest[:, LANES:]], axis=1)
    _, ts, cum, start, end = step_terms(dt_ref[...], dtb, na2, tri_ref[...], cols)
    cum_t = cum.T
    grow = expand_operand(start, end, ts)
    row_i = lax.broadcasted_iota(jnp.int32, (Q, Q), 0)
    col_j = lax.broadcasted_iota(jnp.int32, (Q, Q), 1)
    same = wide(cols[:, 0:1], LANES) == seg
    mask = jnp.where(same & (row_i >= col_j), 0.0, NEG)
    scores = dot_split((cm, bc_rest[:, LANES:]), (bm, bc_rest[:, :LANES]))
    left = col_j < HEAD
    yield

    for c in range(0, inner, 256):
        at = pl.ds(c, 256)
        x = conv(c)
        big = dot(grow, e_ref[:, at])
        s_e, e_e, t_e = big[:Q], big[Q : 2 * Q], big[2 * Q :]
        xs = x * t_e
        xs_low = xs.astype(bf16)
        st = state[:, at]
        st_low = st.astype(bf16)
        sin_ref[:, at] = st_low
        carried = dot(c_two, twice(st_low, 0))
        parts = []
        for p in range(2):
            mats = []
            for h in range(2):
                head = (c + p * LANES) // HEAD + h
                gap = wide(cum[:, head : head + 1], LANES) - cum_t[head : head + 1, :] + mask
                mats.append((jnp.exp2(gap) * scores).astype(bf16))
            xp = xs_low[:, p * LANES : (p + 1) * LANES]
            parts.append(dot(jnp.concatenate(mats, axis=1), by_head(xp, left)))
        y = jnp.concatenate(parts, axis=1) + s_e * carried + skip_ref[:, at] * x
        y_ref[:, at] = y
        state[:, at] = st * s_e[Q - 1 : Q, :] + dot(bt, (xs * e_e).astype(bf16))
        yield


def fixed(shape):
    return pl.BlockSpec(shape, lambda *_: (0,) * len(shape))


def state_forward(seg, xbc, dt, cw, cb, head, inner, seqs):
    rows, channels = xbc.shape
    blocks = rows // seqs // Q
    at = lambda b: (0, b, 0)
    tiled = lambda v: v.reshape(seqs, rows // seqs, v.shape[1])
    y, s, sin = pl.pallas_call(
        fwd_kernel,
        grid=(blocks,),
        in_specs=[
            fixed(seg.shape),
            pl.BlockSpec((seqs, Q, channels), at),
            pl.BlockSpec((seqs, Q, LANES), at),
            fixed(cw.shape), fixed(cb.shape), fixed(head.shape),
        ],
        out_specs=[
            pl.BlockSpec((seqs, Q, inner), at),
            pl.BlockSpec((seqs, Q, channels), at),
            pl.BlockSpec((seqs, None, LANES, inner), lambda b: (0, b, 0, 0)),
        ],
        out_shape=[
            jax.ShapeDtypeStruct((seqs, rows // seqs, inner), f32),
            jax.ShapeDtypeStruct((seqs, rows // seqs, channels), f32),
            jax.ShapeDtypeStruct((seqs, blocks, LANES, inner), bf16),
        ],
        scratch_shapes=[
            pltpu.VMEM((seqs, LANES, inner), f32),
            pltpu.VMEM((seqs, Q + 8, channels), f32),
            pltpu.VMEM((2 * LANES, inner), bf16),
            pltpu.VMEM((Q, Q), bf16),
            pltpu.VMEM((1, inner), f32),
        ],
        compiler_params=params(60 << 20),
        name="state_forward",
    )(seg, tiled(xbc), tiled(dt), cw, cb, head)
    return y.reshape(rows, inner), s.reshape(rows, channels), sin


def flat(ref):
    v = ref[...]
    return v.reshape(v.shape[0] * v.shape[1], v.shape[2])


def slab_views(slab, own):
    owners, _, width = slab.shape
    if own % 16 == 0:
        first = lambda *_: (0, 0, 0)
        second = lambda *_: (0, 1, 0)
        sizes = ((own, first), (own, second), (2 * own, second))
        return [(slab, pl.BlockSpec((owners, n, width), index)) for n, index in sizes]
    parts = [
        v.reshape(1, -1, width) for v in (slab[:, :own], slab[:, own : 2 * own], slab[:, 2 * own :])
    ]
    return [(v, fixed(v.shape)) for v in parts]


def gate_kernel(
    tok_ref, normed_ref, y_ref, cot_ref, wa_ref, wb_ref, wo_ref, gain_ref,
    gn_ref, out_ref, gz_ref, gm_ref, ggain_ref,
):
    wa, wb, wo = flat(wa_ref), flat(wb_ref), flat(wo_ref)
    gain = gain_ref[...]

    @pl.when(pl.program_id(0) == 0)
    def _():
        ggain_ref[...] = jnp.zeros_like(ggain_ref)

    normed = normed_ref[...]
    z = jnp.concatenate([dot(normed, wa), dot(normed, wb)], axis=1)
    g_gn = dot(cot_ref[...], wo, NT)
    sg = sigmoid(z)
    sz = z * sg
    y = y_ref[...]
    gated = y * sz
    rstd = lax.rsqrt(jnp.mean(gated * gated, axis=-1, keepdims=True) + EPS)
    unit = gated * rstd
    gn = (unit * gain).astype(bf16)
    gn_ref[...] = gn
    out_ref[...] = (tok_ref[...].astype(f32) + dot(gn, wo)).astype(bf16)
    ggain_ref[...] += fold_rows(unit * g_gn)
    q = g_gn * gain
    mean = jnp.mean(unit * q, axis=-1, keepdims=True)
    g_gated = rstd * (q - unit * mean)
    gm_ref[...] = g_gated * sz
    gz_ref[...] = (g_gated * y * (sg * (1.0 + z * (1.0 - sg)))).astype(bf16)


def gate(tok, normed, y, cot, weights, gain, tile=256):
    rows, width = tok.shape
    inner = y.shape[1]
    at = lambda i: (i, 0)
    return pl.pallas_call(
        gate_kernel,
        grid=(rows // tile,),
        in_specs=[
            pl.BlockSpec((tile, width), at),
            pl.BlockSpec((tile, width), at),
            pl.BlockSpec((tile, inner), at),
            pl.BlockSpec((tile, width), at),
            *[spec for _, spec in weights], fixed(gain.shape),
        ],
        out_specs=[
            pl.BlockSpec((tile, inner), at),
            pl.BlockSpec((tile, width), at),
            pl.BlockSpec((tile, inner), at),
            pl.BlockSpec((tile, inner), at),
            fixed((8, inner)),
        ],
        out_shape=[
            jax.ShapeDtypeStruct((rows, inner), bf16),
            jax.ShapeDtypeStruct((rows, width), bf16),
            jax.ShapeDtypeStruct((rows, inner), bf16),
            jax.ShapeDtypeStruct((rows, inner), f32),
            jax.ShapeDtypeStruct((8, inner), f32),
        ],
        compiler_params=params(60 << 20),
        name="gate",
    )(tok, normed, y, cot, *[v for v, _ in weights], gain)


def bwd_kernel(
    seg_ref, xbc_ref, dt_ref, s_ref, sin_ref, gm_ref, cw_ref, head_ref,
    gx_ref, gcw_ref, gcb_ref, gskip_ref, galog_ref, gdtb_ref,
    adj, gext, da_rows, spread, grad_b, grad_c, link, e_ref, tri_ref, skip_ref, et_ref, tail_ref, pair_ref,
):
    seqs, _, inner = gm_ref.shape
    channels = s_ref.shape[2]
    b = pl.program_id(0)

    @pl.when(b == 0)
    def _():
        for ref in (gcw_ref, gcb_ref, gskip_ref, galog_ref, gdtb_ref, da_rows):
            ref[...] = jnp.zeros_like(ref)
        fill_constants(e_ref, tri_ref, skip_ref, head_ref)
        et_ref[...] = ones_where(iota((inner, LANES), 0) // HEAD == iota((inner, LANES), 1))
        turned = ones_where(iota((Q, Q), 0) <= iota((Q, Q), 1))
        below = ones_where(iota((Q, Q), 0) > iota((Q, Q), 1))
        tail_ref[...] = jnp.concatenate([turned, turned, below, below], axis=1)
        row, col = iota((2 * Q, 2 * Q), 0), iota((2 * Q, 2 * Q), 1)
        pair_ref[...] = ones_where((row // Q == col // Q) & (row >= col))

    @pl.when(b == 0)
    def _():
        adj[...] = jnp.zeros_like(adj)
        gext[:, Q : Q + 8, :] = jnp.zeros((seqs, 8, channels), f32)

    @pl.when(b > 0)
    def _():
        gext[:, Q : Q + 8, :] = gext[:, 0:8, :]

    alternate(
        [
            bwd_block(
                q, seg_ref, *[r.at[q] for r in (xbc_ref, dt_ref, s_ref, sin_ref, gm_ref)], cw_ref, head_ref,
                gx_ref.at[q], gcw_ref, gcb_ref, gskip_ref, galog_ref, gdtb_ref,
                *[r.at[q] for r in (adj, gext, da_rows, spread, grad_b, grad_c, link)],
                e_ref, tri_ref, skip_ref, et_ref, tail_ref, pair_ref,
            )
            for q in range(seqs)
        ],
        26,
    )


def alternate(blocks, lead):
    for _ in range(lead):
        next(blocks[0], None)
    live = list(blocks)
    while live:
        live = [block for block in reversed(live) if next(block, live) is not live][::-1]


def bwd_block(
    q, seg_ref, xbc_ref, dt_ref, s_ref, sin_ref, gm_ref, cw_ref, head_ref,
    gx_ref, gcw_ref, gcb_ref, gskip_ref, galog_ref, gdtb_ref,
    adj, gext, da_rows, spread, grad_b, grad_c, link, e_ref, tri_ref, skip_ref, et_ref, tail_ref, pair_ref,
):
    inner = gm_ref.shape[1]
    channels = s_ref.shape[1]
    b, blocks = pl.program_id(0), pl.num_programs(0)
    dtb, rate, na2 = head_terms(head_ref)
    turn = blocks - 1 - b
    seg, cols = segment_rows(seg_ref, turn, blocks, q * blocks + turn)
    raw, ts, cum, start, end = step_terms(dt_ref[...], dtb, na2, tri_ref[...], cols)
    cum_t = cum.T
    grow = expand_operand(start, end, ts)
    yield

    def act(c):
        s = s_ref[:, pl.ds(c, 256)]
        sg = sigmoid(s)
        return s * sg, sg * (1.0 + s * (1.0 - sg))

    bc, slope_bc = act(inner)
    bc, bc_rest = split(bc, 2)
    bm, cm = bc[:, :LANES], bc[:, LANES:]
    ct = cm.T
    b_two = jnp.concatenate([bm, bc_rest[:, :LANES]], axis=1)
    c_two = jnp.concatenate([cm, bc_rest[:, LANES:]], axis=1)
    row_j = lax.broadcasted_iota(jnp.int32, (Q, Q), 0)
    col_i = lax.broadcasted_iota(jnp.int32, (Q, Q), 1)
    same = wide(cols[:, 0:1], LANES) == seg
    mask = jnp.where(same & (col_i >= row_j), 0.0, NEG)
    before = (row_j < col_i).astype(f32)
    scores = dot_split((bm, bc_rest[:, :LANES]), (cm, bc_rest[:, LANES:]))
    left = col_i < HEAD
    grad_scores = jnp.zeros((Q, Q), f32)
    yield

    def enter(c):
        at = pl.ds(c, 256)
        x, slope = act(c)
        big = dot(grow, e_ref[:, at])
        s_e, e_e, t_e = big[:Q], big[Q : 2 * Q], big[2 * Q :]
        xs = x * t_e
        xs_low, xs_rest = split(xs, 2)
        gm = gm_ref[:, at]
        gm_low, gm_rest = split(gm, 2)
        ad_low, ad_rest = split(adj[:, at], 2)
        st_low = sin_ref[:, at]
        into = dot(b_two, twice(ad_low, 0)) + dot(bm, ad_rest)
        carried = dot(c_two, twice(st_low, 0))
        diags, gmats = [], []
        for p in range(2):
            lanes = slice(p * LANES, (p + 1) * LANES)
            diags.append((by_head(gm_low[:, lanes], left), by_head(gm_rest[:, lanes], left)))
            tall = dot(jnp.concatenate([xs_low[:, lanes], xs_rest[:, lanes]], axis=0), diags[p][0], NT)
            gmats.append(tall[:Q] + tall[Q:] + dot(xs_low[:, lanes], diags[p][1], NT))
        return x, slope, s_e, e_e, t_e, xs, gm, ad_low, st_low, into, carried, diags, gmats

    def within(c, held):
        diags, gmats = held[-2:]
        parts, joined = [], []
        extra = jnp.zeros((Q, Q), f32)
        for p in range(2):
            diag, diag_rest = diags[p]
            mats, links = [], []
            for h in range(2):
                head = (c + p * LANES) // HEAD + h
                gap = cum_t[head : head + 1, :] - wide(cum[:, head : head + 1], LANES) + mask
                decay = jnp.exp2(gap)
                mat = decay * scores
                grad = gmats[p][:, h * LANES : (h + 1) * LANES]
                extra += decay * grad
                mats.append(split(mat, 2))
                links.append((mat * grad).astype(bf16))
            high = jnp.concatenate([mats[0][0], mats[1][0]], axis=1)
            rest = jnp.concatenate([mats[0][1], mats[1][1]], axis=1)
            both = dot(jnp.concatenate([high, rest], axis=0), diag)
            parts.append(both[:Q] + both[Q:] + dot(high, diag_rest))
            joined.append(jnp.concatenate(links, axis=1))
            yield
        reach = dot(jnp.concatenate(joined, axis=0), pair_ref[...])
        for n in range(4):
            p, h = n // 2, n % 2
            head = c // HEAD + n
            da_rows[head : head + 1, :] = jnp.sum(
                reach[p * Q : (p + 1) * Q, h * LANES : (h + 1) * LANES] * before, axis=0, keepdims=True
            )
        return parts, extra

    def leave(c, held, parts):
        at = pl.ds(c, 256)
        x, slope, s_e, e_e, t_e, xs, gm, ad_low, st_low, into, carried = held[:-2]
        ad = adj[:, at]
        g_xs = jnp.concatenate(parts, axis=1) + e_e * into
        gext[0:Q, at] = (t_e * g_xs + skip_ref[:, at] * gm) * slope
        sums = jnp.concatenate(
            [pair_split(carried * gm), pair_split(x * into), pair_split(x * g_xs)], axis=0
        )
        sums = dot(sums, twice(et_ref[at, :], 0))
        s_gm = (s_e * gm).astype(bf16)
        part_c = dot(s_gm, st_low, NT)
        part_b = dot((e_e * xs).astype(bf16), ad_low, NT)
        if c == 0:
            spread[...] = sums
            grad_c[...] = part_c
            grad_b[...] = part_b
        else:
            spread[...] += sums
            grad_c[...] += part_c
            grad_b[...] += part_b
        gskip_ref[:, at] += fold_rows(gm * x)
        link[:, at] = fold_rows(st_low.astype(f32) * ad)
        adj[:, at] = ad * s_e[Q - 1 : Q, :] + dot(ct, s_gm)

    starts = list(range(0, inner, 256))
    held, inside = {}, {}
    for step in range(len(starts) + 1):
        if step < len(starts):
            held[step] = enter(starts[step])
            yield
        if 0 <= step - 1:
            parts, extra = yield from within(starts[step - 1], held[step - 1])
            grad_scores += extra
            leave(starts[step - 1], held.pop(step - 1), parts)
        yield

    grad_low = grad_scores.astype(bf16)
    g_b = grad_b[...] + dot(grad_low, cm)
    g_c = grad_c[...] + dot(grad_low, bm, TN)
    gext[0:Q, pl.ds(inner, 256)] = jnp.concatenate([g_b, g_c], axis=1) * slope_bc

    phi = start * spread[0:Q]
    psi = end * ts * spread[Q : 2 * Q]
    through = jnp.sum(dot(jnp.concatenate(split(link[...], 2), axis=0), et_ref[...]), axis=0, keepdims=True)
    around = jnp.concatenate(split(phi, 2) + split(psi, 2), axis=0)
    da = da_rows[...].T + dot(tail_ref[...], around) + start[Q - 1 : Q, :] * through
    g_ts = spread[2 * Q :] + rate * da
    yield
    galog_ref[...] += fold_rows(ts * rate * da)
    g_dt = g_ts * sigmoid(raw)
    gdtb_ref[...] += fold_rows(g_dt)

    n1, n2, n3 = (wide(cols[:, k : k + 1], 256) for k in (6, 7, 8))
    for c in range(0, channels, 256):
        at = pl.ds(c, 256)
        x = xbc_ref[:, at]
        g = gext[:, at]
        g0 = g[:Q]
        g1 = later_rows(g, 1) * n1
        g2 = later_rows(g, 2) * n2
        g3 = later_rows(g, 3) * n3
        gx = cw_ref[3:4, at] * g0 + cw_ref[2:3, at] * g1 + cw_ref[1:2, at] * g2 + cw_ref[0:1, at] * g3
        gx_ref[:, at] = gx.astype(bf16)
        gcb_ref[:, at] += fold_rows(g0)
        gcw_ref[24:32, at] += fold_rows(g0 * x)
        gcw_ref[16:24, at] += fold_rows(g1 * x)
        gcw_ref[8:16, at] += fold_rows(g2 * x)
        gcw_ref[0:8, at] += fold_rows(g3 * x)
        yield
    gx_ref[:, channels:] = g_dt.astype(bf16)


def state_backward(seg, xbc, dt, s, sin, gm, cw, head, seqs):
    rows, channels = xbc.shape
    inner = gm.shape[1]
    blocks = rows // seqs // Q
    at = lambda b: (0, blocks - 1 - b, 0)
    tiled = lambda v: v.reshape(seqs, rows // seqs, v.shape[1])
    out = pl.pallas_call(
        bwd_kernel,
        grid=(blocks,),
        in_specs=[
            fixed(seg.shape),
            pl.BlockSpec((seqs, Q, channels), at),
            pl.BlockSpec((seqs, Q, LANES), at),
            pl.BlockSpec((seqs, Q, channels), at),
            pl.BlockSpec((seqs, None, LANES, inner), lambda b: (0, blocks - 1 - b, 0, 0)),
            pl.BlockSpec((seqs, Q, inner), at),
        ]
        + [fixed(v.shape) for v in (cw, head)],
        out_specs=[
            pl.BlockSpec((seqs, Q, channels + LANES), at),
            fixed((32, channels)), fixed((8, channels)), fixed((8, inner)), fixed((8, LANES)), fixed((8, LANES)),
        ],
        out_shape=[
            jax.ShapeDtypeStruct((seqs, rows // seqs, channels + LANES), bf16),
            jax.ShapeDtypeStruct((32, channels), f32),
            jax.ShapeDtypeStruct((8, channels), f32),
            jax.ShapeDtypeStruct((8, inner), f32),
            jax.ShapeDtypeStruct((8, LANES), f32),
            jax.ShapeDtypeStruct((8, LANES), f32),
        ],
        scratch_shapes=[
            pltpu.VMEM((seqs, LANES, inner), f32),
            pltpu.VMEM((seqs, Q + 8, channels), f32),
            pltpu.VMEM((seqs, LANES, LANES), f32),
            pltpu.VMEM((seqs, 3 * Q, LANES), f32),
            pltpu.VMEM((seqs, Q, LANES), f32),
            pltpu.VMEM((seqs, Q, LANES), f32),
            pltpu.VMEM((seqs, 8, inner), f32),
            pltpu.VMEM((2 * LANES, inner), bf16),
            pltpu.VMEM((Q, Q), bf16),
            pltpu.VMEM((1, inner), f32),
            pltpu.VMEM((inner, LANES), bf16),
            pltpu.VMEM((Q, 4 * Q), bf16),
            pltpu.VMEM((2 * Q, 2 * Q), bf16),
        ],
        compiler_params=params(60 << 20),
        name="state_backward",
    )(
        seg, tiled(xbc), tiled(dt), tiled(s), sin.reshape(seqs, blocks, LANES, inner), tiled(gm), cw, head
    )
    return out[0].reshape(rows, channels + LANES), *out[1:]


def token_kernel(tok_ref, cot_ref, gz_ref, gx_ref, wa_ref, wb_ref, wx_ref, gain_ref, out_ref, ggain_ref):
    half = gz_ref.shape[1] // 2
    g = dot(gz_ref[:, :half], flat(wa_ref), NT) + dot(gz_ref[:, half:], flat(wb_ref), NT)
    g += dot(gx_ref[...], wx_ref[...], NT)
    u = tok_ref[...].astype(f32)
    r = lax.rsqrt(jnp.mean(u * u, axis=-1, keepdims=True) + EPS)
    unit = u * r

    @pl.when(pl.program_id(0) == 0)
    def _():
        ggain_ref[...] = jnp.zeros_like(ggain_ref)

    ggain_ref[...] += fold_rows(unit * g)
    q = g * gain_ref[...]
    mean = jnp.mean(unit * q, axis=-1, keepdims=True)
    out_ref[...] = (cot_ref[...].astype(f32) + r * (q - unit * mean)).astype(bf16)


def token_grad(tok, cot, gz, gx, weights, wx, gain, tile=256):
    rows, width = tok.shape
    at = lambda i: (i, 0)
    return pl.pallas_call(
        token_kernel,
        grid=(rows // tile,),
        in_specs=[
            pl.BlockSpec((tile, width), at),
            pl.BlockSpec((tile, width), at),
            pl.BlockSpec((tile, gz.shape[1]), at),
            pl.BlockSpec((tile, gx.shape[1]), at),
            *[spec for _, spec in weights], fixed(wx.shape), fixed(gain.shape),
        ],
        out_specs=[pl.BlockSpec((tile, width), at), fixed((8, width))],
        out_shape=[jax.ShapeDtypeStruct((rows, width), bf16), jax.ShapeDtypeStruct((8, width), f32)],
        compiler_params=params(60 << 20),
        name="token_grad",
    )(tok, cot, gz, gx, *[v for v, _ in weights], wx, gain)


MESH = pl.DeviceIdType.MESH


def place(line):
    me = lax.axis_index("dp")
    index = lambda l, x, c: (l * 2 + x) * 2 + c
    return me // 4, (me // 2) % 2, me % 2, index, lax.axis_index("seq")


def meet(devices):
    barrier = pltpu.get_barrier_semaphore()
    for device in devices:
        pl.semaphore_signal(barrier, inc=1, device_id=device, device_id_type=MESH)
    pl.semaphore_wait(barrier, len(devices))


def remote(src, dst, send, recv, device):
    return pltpu.make_async_remote_copy(
        src_ref=src, dst_ref=dst, send_sem=send, recv_sem=recv, device_id=device, device_id_type=MESH
    )


def gather_kernel(line, own_ref, out_ref, line_send, x_send, y_send, core_send, recv, local):
    l, x, c, index, y = place(line)
    others = [{"dp": index((l + k) % line, x, c)} for k in range(1, line)]
    beside, sibling, across = {"dp": index(l, 1 - x, c)}, {"dp": index(l, x, 1 - c)}, {"seq": 1 - y}
    meet(others + [beside, sibling, across])
    started = []

    def send(src, at, sem, device):
        copy = remote(src, out_ref.at[at], sem, recv.at[at], device)
        copy.start()
        started.append(copy)

    def arrived(at):
        remote(out_ref.at[at], out_ref.at[at], local.at[1], recv.at[at], sibling).wait_recv()

    mine = pltpu.make_async_copy(own_ref, out_ref.at[l, x, c], local.at[0])
    mine.start()
    send(own_ref.at[y], (l, x, c, y), x_send.at[0], beside)
    for k in range(1, line):
        send(own_ref.at[y], (l, x, c, y), line_send.at[k, 0], others[k - 1])
    for k in range(1, line):
        send(own_ref.at[1 - y], (l, x, c, 1 - y), line_send.at[k, 1], others[k - 1])
    for h in range(2):
        send(own_ref.at[h], (l, x, c, h), core_send.at[0, h], sibling)
    for k in range(1, line):
        at = ((l + k) % line, x, c, y)
        arrived(at)
        send(out_ref.at[at], at, x_send.at[k], beside)
        send(out_ref.at[at], at, core_send.at[k, 0], sibling)
    for k in range(line):
        at = ((l + k) % line, 1 - x, c, y)
        arrived(at)
        send(out_ref.at[at], at, y_send.at[k], across)
        send(out_ref.at[at], at, core_send.at[line + k, 0], sibling)
    for k in range(1, line):
        at = ((l + k) % line, x, c, 1 - y)
        arrived(at)
        send(out_ref.at[at], at, core_send.at[k, 1], sibling)
    for k in range(line):
        at = ((l + k) % line, 1 - x, c, 1 - y)
        arrived(at)
        send(out_ref.at[at], at, core_send.at[line + k, 1], sibling)
    for k in range(line):
        for side in range(2):
            for h in range(2):
                arrived(((l + k) % line, side, 1 - c, h))
    for copy in started:
        copy.wait_send()
    mine.wait()


def gather(local, owners):
    own, columns = local.shape
    line = owners // 4
    vmem = pl.BlockSpec(memory_space=pltpu.VMEM)
    dma = pltpu.SemaphoreType.DMA
    out = pl.pallas_call(
        functools.partial(gather_kernel, line),
        in_specs=[vmem],
        out_specs=vmem,
        out_shape=jax.ShapeDtypeStruct((line, 2, 2, 2, own // 2, columns), local.dtype),
        scratch_shapes=[
            dma((line, 2)), dma((line,)), dma((line,)), dma((2 * line, 2)), dma((line, 2, 2, 2)), dma((2,)),
        ],
        compiler_params=params(48 << 20, collective_id=1, has_side_effects=True),
        name="gather",
    )(local.reshape(2, own // 2, columns))
    return out.reshape(owners * own, columns)


def pack_small(acc, cw_ref, cb_ref, ggain_ref, skip_ref, ngain_ref, alog_ref, dtb_ref):
    inner, width = ggain_ref.shape[1], ngain_ref.shape[1]
    total = lambda v: jnp.sum(v, axis=0, keepdims=True)
    acc[...] = jnp.zeros(acc.shape, f32)
    for k in range(4):
        acc[k : k + 1, :] = total(cw_ref[8 * k : 8 * k + 8, :])
    acc[4:5, :] = total(cb_ref[...])
    acc[5:6, :inner] = total(ggain_ref[...])
    acc[6:7, :width] = total(ngain_ref[...])
    acc[6:7, width : width + LANES] = total(alog_ref[...])
    acc[6:7, width + LANES : width + 2 * LANES] = total(dtb_ref[...])
    skip = jnp.concatenate(split(skip_ref[...], 3), axis=0)
    by_head = ones_where(iota((inner, LANES), 0) // HEAD == iota((inner, LANES), 1))
    acc[6:7, width + 2 * LANES : width + 3 * LANES] = total(dot(skip, by_head))


def finish_kernel(
    line, bits, cw_ref, cb_ref, ggain_ref, skip_ref, ngain_ref, alog_ref, dtb_ref, zo_ref, zo_got_ref, d_ref, from_x_ref, from_y_ref,
    small_ref, din_ref, dout_ref,
    acc, got, one, two_got, two, three_got, three, line_got, last, last_got,
    small_send, small_recv, two_send, two_recv, three_send, three_recv,
    line_send, line_recv, last_sem,
):
    l, x, c, index, y = place(line)
    me = lax.axis_index("dp")
    doubling = [{"dp": me + bit - 2 * bit * ((me // bit) % 2)} for bit in bits]
    others = [{"dp": index((l + k) % line, x, c)} for k in range(1, line)]
    beside, sibling, across = {"dp": index(l, 1 - x, c)}, {"dp": index(l, x, 1 - c)}, {"seq": 1 - y}
    meet(doubling + others + [beside, sibling, across])
    def plus(a, b):
        return a.astype(f32) + b.astype(f32)

    def launch(*args):
        copy = remote(*args)
        copy.start()
        return copy

    second, third = [], []
    for i in range(line):
        for j in range(2):
            for n in range(2):
                if i % 2 == 0:
                    one[i, j, n] = plus(d_ref[i, x, j, n], from_x_ref[i // 2, j, n]).astype(bf16)
                else:
                    one[i, n, j] = plus(d_ref[i, j, n, y], from_y_ref[i // 2, j, n]).astype(bf16)
        second.append(launch(one.at[i, 1 - c], two_got.at[i], two_send.at[i], two_recv.at[i], sibling))
    pack_small(acc.at[0], cw_ref, cb_ref, ggain_ref, skip_ref, ngain_ref, alog_ref, dtb_ref)
    smalls = doubling + [across]

    def small_start(k):
        return launch(acc.at[k], got.at[k], small_send.at[k], small_recv.at[k], smalls[k])

    small = small_start(0)
    for i in range(line):
        second[i].wait()
        for j in range(2):
            two[i, j] = plus(one[i, c, j], two_got[i, j]).astype(bf16)
        src, device = (two.at[i, 1 - y], across) if i % 2 == 0 else (two.at[i, 1 - x], beside)
        third.append(launch(src, three_got.at[i], three_send.at[i], three_recv.at[i], device))
    for i in range(line):
        third[i].wait()
        kept = two[i, y] if i % 2 == 0 else two[i, x]
        three[i] = plus(kept, three_got[i]).astype(bf16)

    def to_owner(k):
        target = (l + k) % line
        return remote(three.at[target], line_got.at[l], line_send.at[k], line_recv.at[l], others[k - 1])

    for k in range(1, line):
        to_owner(k).start()
    for k in range(len(smalls)):
        small.wait()
        acc[k + 1] = acc[k] + got[k]
        if k + 1 < len(smalls):
            small = small_start(k + 1)

    small_ref[...] = acc[len(smalls)]
    own, half = din_ref.shape[0], zo_ref.shape[1]
    zo = plus(zo_ref[...], zo_got_ref[...])
    din_ref[:, :half] = zo[:own]
    din_ref[:, half : 2 * half] = zo[own : 2 * own]
    dout_ref[...] = zo[2 * own :]

    total = three[l].astype(f32)
    for k in range(1, line):
        at_k = (l + k) % line
        remote(three.at[0], line_got.at[at_k], last_sem.at[2], line_recv.at[at_k], sibling).wait_recv()
        total += line_got[at_k].astype(f32)
    last[...] = total.astype(bf16)
    final = launch(last, last_got, last_sem.at[0], last_sem.at[1], across)
    for k in range(1, line):
        to_owner(k).wait_send()
    final.wait()
    left = din_ref.shape[1] - 2 * half
    kept, came = last[...].astype(f32), last_got[...].astype(f32)
    lower = (y == 0).astype(f32)
    din_ref[: own // 2, 2 * half :] = (kept * lower + came * (1.0 - lower))[:, :left]
    din_ref[own // 2 :, 2 * half :] = (came * lower + kept * (1.0 - lower))[:, :left]


def finish(smalls, d_zo, zo_got, parts, from_x, from_y, own, proj):
    line, columns, half = parts.shape[0], parts.shape[-1], d_zo.shape[1]
    owners = 4 * line
    bits = [1 << i for i in range(owners.bit_length() - 1)]
    channels = smalls[1].shape[1]
    vmem = pl.BlockSpec(memory_space=pltpu.VMEM)
    dma = pltpu.SemaphoreType.DMA
    piece = (own // 2, columns)
    steps = len(bits) + 1
    low = lambda *dims: pltpu.VMEM(dims + piece, bf16)
    return pl.pallas_call(
        functools.partial(finish_kernel, line, bits),
        in_specs=[vmem] * 12,
        out_specs=[vmem] * 3,
        out_shape=[
            jax.ShapeDtypeStruct((8, channels), f32),
            jax.ShapeDtypeStruct((own, proj), f32),
            jax.ShapeDtypeStruct((2 * own, half), f32),
        ],
        scratch_shapes=[
            pltpu.VMEM((steps + 1, 8, channels), f32),
            pltpu.VMEM((steps, 8, channels), f32),
            low(line, 2, 2), low(line, 2), low(line, 2), low(line), low(line), low(line), low(), low(),
            dma((steps,)), dma((steps,)),
        ]
        + [dma((line,))] * 6
        + [dma((3,))],
        compiler_params=params(48 << 20, collective_id=0, has_side_effects=True),
        name="finish",
    )(*smalls, d_zo, zo_got, parts, from_x, from_y)


def finish_plain(smalls, d_zo, d_x, own, proj):
    cw, cb, ggain, skip, ngain, alog, dtb = (v.reshape(-1, 8, v.shape[1]).sum(1) for v in smalls)
    skip = jnp.pad(skip.reshape(1, -1, HEAD).sum(2), ((0, 0), (0, LANES - skip.shape[1] // HEAD)))
    tail = jnp.concatenate([ngain, alog, dtb, skip], axis=1)
    wide = lambda v: jnp.pad(v, ((0, 0), (0, cb.shape[1] - v.shape[1])))
    small = lax.psum(jnp.concatenate([cw, cb, wide(ggain), wide(tail)], axis=0), ("dp", "seq"))
    d_x = lax.psum_scatter(d_x, "dp", scatter_dimension=0, tiled=True)
    d_zo, d_x = lax.psum((d_zo.astype(f32), d_x.astype(f32)), "seq")
    d_in = jnp.concatenate([d_zo[:own], d_zo[own : 2 * own], d_x], axis=1)[:, :proj]
    return small, d_in, d_zo[2 * own :]


def per_device(
    sizes, tokens, segments, cotangent, norm_gain, weight_in, conv_weight, conv_bias, dt_bias, a_log, skip_d,
    gate_gain, weight_out,
):
    seqs, length, width = tokens.shape
    rows = seqs * length
    inner = gate_gain.shape[0]
    channels = conv_bias.shape[0]
    heads = dt_bias.shape[0]
    own = weight_in.shape[0]
    owners = width // own
    tok = tokens.reshape(rows, width)
    cot = cotangent.reshape(rows, width)
    pad = LANES - heads

    local_x = jnp.pad(weight_in[:, inner:], ((0, 0), (0, pad)))
    owned = sizes["dp"] % 4 == 0 and sizes["seq"] == 2
    wx = gather(local_x, owners) if owned else lax.all_gather(local_x, "dp", axis=0, tiled=True)
    local_zo = jnp.concatenate([weight_in[:, :width], weight_in[:, width:inner], weight_out], axis=0)
    wx, local_zo = lax.optimization_barrier((wx, local_zo))
    slab = lax.all_gather(local_zo, "dp", axis=0, tiled=True).reshape(owners, 4 * own, width)
    weights = slab_views(slab, own)

    head = jnp.pad(jnp.stack([dt_bias, -jnp.exp(a_log), skip_d]), ((0, 5), (0, pad)))
    seg = segments.astype(f32).reshape(rows // Q, Q)
    cb = conv_bias.reshape(1, channels)
    ngain = norm_gain.reshape(1, width)
    ggain = gate_gain.reshape(1, inner)

    normed, xbc, dt = project(tok, ngain, wx, channels)
    y, s, sin = state_forward(seg, xbc, dt, conv_weight, cb, head, inner, seqs)
    gn, out, gz, gm, p_ggain = gate(tok, normed, y, cot, weights, ggain)
    d_z = dot(normed, gz, TN).astype(bf16)
    d_out = dot(gn, cot, TN).astype(bf16)
    d_zo = jnp.concatenate(
        [
            d_z[:, :width].reshape(owners, own, width),
            d_z[:, width:].reshape(owners, own, width),
            d_out.reshape(owners, 2 * own, width),
        ],
        axis=1,
    ).reshape(owners * 4 * own, width)
    d_zo, gm = lax.optimization_barrier((d_zo, gm))
    d_zo = lax.psum_scatter(d_zo, "dp", scatter_dimension=0, tiled=True)
    gx, p_cw, p_cb, p_skip, p_alog, p_dtb = state_backward(seg, xbc, dt, s, sin, gm, conv_weight, head, seqs)
    d_x = dot(normed, gx, TN).astype(bf16)
    if owned:
        line = owners // 4
        parts = d_x.reshape(line, 2, 2, 2, own // 2, d_x.shape[1])
        beside, across = 1 - (lax.axis_index("dp") // 2) % 2, 1 - lax.axis_index("seq")
        to_x = lax.dynamic_index_in_dim(parts[0::2], beside, 1, keepdims=False)
        to_y = lax.dynamic_index_in_dim(parts[1::2], across, 3, keepdims=False)
        from_x = lax.ppermute(to_x, "dp", [(i, i + 2 - 4 * ((i // 2) % 2)) for i in range(owners)])
        from_y = lax.ppermute(to_y, "seq", [(0, 1), (1, 0)])
    g_tok, p_ngain = token_grad(tok, cot, gz, gx, weights[:2], wx, ngain)
    smalls = (p_cw, p_cb, p_ggain, p_skip, p_ngain, p_alog, p_dtb)
    if owned:
        zo_got = lax.ppermute(d_zo, "seq", [(0, 1), (1, 0)])
        small, d_in, d_out = finish(smalls, d_zo, zo_got, parts, from_x, from_y, own, weight_in.shape[1])
    else:
        small, d_in, d_out = finish_plain(smalls, d_zo, d_x, own, weight_in.shape[1])
    return (
        out.reshape(tokens.shape),
        g_tok.reshape(tokens.shape),
        small[6, :width],
        d_in,
        small[:4],
        small[4],
        small[6, width + LANES : width + LANES + heads],
        small[6, width : width + heads],
        small[6, width + 2 * LANES : width + 2 * LANES + heads],
        small[5, :inner],
        d_out,
    )


def solution(mesh):
    data = P(("dp", "seq"), None, None)
    owned = P("dp", None)
    placed = (data, P(("dp", "seq"), None), data, P(), owned, P(), P(), P(), P(), P(), P(), owned)
    return jax.shard_map(
        functools.partial(per_device, dict(mesh.shape)),
        mesh=mesh,
        in_specs=placed,
        out_specs=(data, data, P(), owned, P(), P(), P(), P(), P(), P(), owned),
        check_vma=False,
    )
```
